32 devices in a mesh: xy: 16 (over z, y, core), gz: 2 (over x).
Axes of the slice: x: 2, y: 2, z: 4, core: 2. Of those that a mesh axis runs over, the one named last changes fastest.
Arguments:
- positions: float32 [3, 32, 2, 16, 128], P(None, None, 'gz', 'xy'), may hold values from 0 to 2
- velocities: float32 [3, 32, 2, 16, 128], P(None, None, 'gz', 'xy'), may hold values from -6 to 6
- forces_prev: float32 [3, 32, 2, 16, 128], P(None, None, 'gz', 'xy'), may hold values from -48 to 48
- seeds: int32 [32, 2, 16, 128], P(None, 'gz', 'xy'), may hold values from 0 to 16383
- counts: int32 [2, 16, 128], P('gz', 'xy'), may hold values from 12 to 32, as said below
- offsets: int32 [2], replicated, may hold values from 0 to 127
Outputs:
- forces: float32 [3, 32, 2, 16, 128], P(None, None, 'gz', 'xy')
- velocities_out: float32 [3, 32, 2, 16, 128], P(None, None, 'gz', 'xy')
- stress: float32 [6, 2, 16, 128], P(None, 'gz', 'xy')
The draws below stay inside these ranges and needn't reach their ends.
Inputs may be any that keep to these rules, and one draw needn't show every extreme that they name: `counts`: each cell holds 12 to 32 beads; every row of 128 cells along x has a full cell.
All inputs are finite; a program needn't handle non-finite values.
Results may differ from the reference program's by a relative error of at most 0.0003.
Values sent between devices are 32-bit elements; how exact they have to be, the bound alone decides.
No kernel may reach another device: no remote copies, remote signals or barrier semaphores. Data moves between devices by JAX's collectives and lax.ppermute only.
A program may use at most 128 MiB of HBM per device.

```python
import math
import jax
import jax.numpy as jnp
from jax import lax

SLOTS = 32
NX = 128
NY = 16
NZ = 2


def draw_counts(key, part):
    first_key = jax.random.fold_in(key, 11)
    second_key = jax.random.fold_in(key, 23)
    base = jax.random.randint(first_key, (NZ, NY, NX), 3 * SLOTS // 8, SLOTS + 1, dtype=jnp.int32)
    spot = jax.random.randint(second_key, (NZ, NY, 1), 0, NX, dtype=jnp.int32)
    full = jnp.arange(NX, dtype=jnp.int32)[None, None, :] == spot
    return jnp.where(full, SLOTS, base).astype(jnp.int32)


def place_ends(drawn, own_key, smallest, top_value):
    shape = drawn.shape
    place = [jax.random.randint(jax.random.fold_in(own_key, axis), (), 0, shape[axis]) for axis in range(len(shape))]
    drawn = drawn.at[tuple(place)].set(smallest)
    longest = shape.index(max(shape))
    place[longest] = (place[longest] + 1) % shape[longest]
    return drawn.at[tuple(place)].set(top_value)


def block_levels(key, dims, split, least, top_value):
    level, own = 1.0, jax.random.fold_in(key, 6)
    for axis_at, blocks in split:
        steps = jnp.exp(jax.random.uniform(jax.random.fold_in(own, axis_at), (blocks,), jnp.float32, least / len(split), top_value / len(split)))
        level = level * jnp.repeat(steps, dims[axis_at] // blocks).reshape([-1 if axis == axis_at else 1 for axis in range(len(dims))])
    return level


def normal_values(key, dims, scale, limit, split=(), held_as=jnp.bfloat16):
    values = jax.random.normal(key, dims, jnp.float32) * scale
    if len(split) > 0:
        values = block_levels(key, dims, split, -0.22, 0.18) * values
    return jnp.clip(values, min=-limit, max=limit).astype(held_as)


def setup_inputs(seed: int = 0) -> dict:
    arg_keys = jax.random.split(jax.random.key(seed), 7)
    return {
        "positions": jnp.clip(2.0 * jax.random.uniform(arg_keys[0], (3, SLOTS, NZ, NY, NX), jnp.float32) ** block_levels(arg_keys[0], (3, SLOTS, NZ, NY, NX), ((2, 2), (3, 16)), -0.2, 0.2), 0.0, 2.0),
        "velocities": normal_values(arg_keys[1], (3, SLOTS, NZ, NY, NX), 1.0, 6.0, ((2, 2), (3, 16)), jnp.float32),
        "forces_prev": normal_values(arg_keys[2], (3, SLOTS, NZ, NY, NX), 8.0, 48.0, ((2, 2), (3, 16)), jnp.float32),
        "seeds": place_ends(jax.random.randint(arg_keys[3], (SLOTS, NZ, NY, NX), 0, 16384), jax.random.fold_in(arg_keys[3], 1), 0, 16383).astype(jnp.int32),
        "counts": draw_counts(jax.random.fold_in(arg_keys[6], 71), 0),
        "offsets": jax.random.randint(arg_keys[5], (2,), 0, NX).astype(jnp.int32),
    }


CONSERVATIVE = 25.0
FRICTION = 4.5
NOISE_LEVEL = 3.0
TIME_STEP = 0.04
SHEAR_SPEED = 1.0
CELL_VOLUME = 8.0
FLOOR_SQUARED = 0.0025
COMPONENT_PAIRS = [(0, 0), (1, 1), (2, 2), (0, 1), (0, 2), (1, 2)]
NEIGHBOURS = [(dz, dy, dx) for dz in (-1, 0, 1) for dy in (-1, 0, 1) for dx in (-1, 0, 1)]

def pair_terms(home_beads, near_beads, offset, same_cell, step):
    slots = home_beads.shape[1]
    shift = jnp.asarray([offset[0], offset[1], offset[2]], jnp.float32)[:, None, None, None]
    separation = home_beads[0:3, :, None, :] - near_beads[0:3, None, :, :] - 2.0 * shift
    velocity_gap = home_beads[3:6, :, None, :] - near_beads[3:6, None, :, :]
    squared = lax.optimization_barrier(jnp.sum(separation * separation, axis=0))
    distance = jnp.sqrt(jnp.maximum(squared, FLOOR_SQUARED))
    occupied = home_beads[7][:, None, :] * near_beads[7][None, :, :]
    if same_cell:
        occupied = occupied * (1.0 - jnp.eye(slots, dtype=jnp.float32))[:, :, None]
    weight = jnp.maximum(1.0 - distance, 0.0) * occupied
    seed_sum = home_beads[6].astype(jnp.int32)[:, None, :] + near_beads[6].astype(jnp.int32)[None, :, :] + (7919 * step + 1)
    hashed = seed_sum * (seed_sum + 1) % 65521
    noise = (hashed.astype(jnp.float32) / 65521.0 - 0.5) * math.sqrt(12.0)
    approach = lax.optimization_barrier(jnp.sum(separation * velocity_gap, axis=0)) / distance
    magnitude = (CONSERVATIVE * weight - FRICTION * weight * weight * approach + NOISE_LEVEL * weight * noise / math.sqrt(TIME_STEP)) / distance
    pair_force = magnitude[None] * separation
    home_force = lax.optimization_barrier(jnp.sum(pair_force, axis=2))
    near_force = -lax.optimization_barrier(jnp.sum(pair_force, axis=1))
    virial = jnp.stack([lax.optimization_barrier(jnp.sum(separation[first] * pair_force[second], axis=(0, 1))) for first, second in COMPONENT_PAIRS]) * (0.5 / CELL_VOLUME)
    return (home_force, near_force, virial)

def build_ghosts(state, offset_now):
    shear = jnp.asarray([0.0, 0.0, 0.0, SHEAR_SPEED, 0.0, 0.0, 0.0, 0.0], jnp.float32)[:, None, None, None, None]
    lower = jnp.roll(state[:, :, :, -1:, :], -offset_now, axis=-1) - shear
    upper = jnp.roll(state[:, :, :, :1, :], offset_now, axis=-1) + shear
    return jnp.concatenate([lower, state, upper], axis=3)

def evaluate(state, offset_now, step):
    extended = build_ghosts(state, offset_now)
    slots = state.shape[1]
    depth = state.shape[2]
    rows = state.shape[3]
    width = state.shape[4]

    def plane(level):
        home = lax.dynamic_index_in_dim(state, level, 2, keepdims=False).reshape(8, slots, -1)
        total_force = jnp.zeros((3, slots, rows * width), jnp.float32)
        total_virial = jnp.zeros((6, rows * width), jnp.float32)
        for dz, dy, dx in NEIGHBOURS:
            near_plane = lax.dynamic_index_in_dim(extended, (level + dz) % depth, 2, keepdims=False)
            near = jnp.roll(near_plane[:, :, 1 + dy:1 + dy + rows, :], -dx, axis=-1).reshape(8, slots, -1)
            same = (dz, dy, dx) == (0, 0, 0)
            home_force, near_force, virial = pair_terms(home, near, (dx, dy, dz), same, step)
            total_force = total_force + home_force
            total_virial = total_virial + virial
        return (total_force.reshape(3, slots, rows, width), total_virial.reshape(6, rows, width))
    planes_force, planes_virial = lax.map(plane, jnp.arange(depth, dtype=jnp.int32))
    return (jnp.moveaxis(planes_force, 0, 2), jnp.moveaxis(planes_virial, 0, 1))

def reference(positions, velocities, forces_prev, seeds, counts, offsets):
    present = (lax.broadcasted_iota(jnp.int32, seeds.shape, 0) < counts[None]).astype(jnp.float32)
    fixed_part = jnp.stack([seeds.astype(jnp.float32), present])
    position_now = positions
    velocity_now = velocities
    force_now = forces_prev
    stress = None
    for step in range(2):
        half_speed = velocity_now + 0.5 * TIME_STEP * force_now
        position_now = position_now + TIME_STEP * half_speed
        state = jnp.concatenate([position_now, half_speed, fixed_part], axis=0)
        force_now, stress = evaluate(state, offsets[step], step)
        velocity_now = half_speed + 0.5 * TIME_STEP * force_now
    return (force_now, velocity_now * present[None], stress)
```

```python
import functools
import math

import jax
import jax.numpy as jnp
from jax import lax
from jax.experimental import pallas as pl
from jax.experimental.pallas import tpu as pltpu
from jax.sharding import PartitionSpec as P

CONSERVATIVE = 25.0
FRICTION = 4.5
NOISE_LEVEL = 3.0
TIME_STEP = 0.04
SHEAR_SPEED = 1.0
CELL_VOLUME = 8.0
FLOOR_SQUARED = 0.0025
EDGE = 2.0
MODULUS = 65521
COMPONENT_PAIRS = [(0, 0), (1, 1), (2, 2), (0, 1), (0, 2), (1, 2)]

NOISE_UNIT = NOISE_LEVEL * math.sqrt(12.0) / math.sqrt(TIME_STEP)
SHIFT = CONSERVATIVE / NOISE_UNIT - 0.5 - 0.5 / MODULUS
VELOCITY_SCALE = FRICTION / NOISE_UNIT
INVERSE = 1.0 / MODULUS
FAR = 1.0e15
REACH = 1.001
SEED_MIDDLE = 8192
F32 = jnp.float32
SUB = 8


def take_rows(values, index):
    dims = lax.GatherDimensionNumbers(
        offset_dims=(),
        collapsed_slice_dims=(0,),
        start_index_map=(0,),
        operand_batching_dims=(1,),
        start_indices_batching_dims=(1,),
    )
    return lax.gather(
        values,
        index[..., None],
        dims,
        slice_sizes=(1, 1),
        mode=lax.GatherScatterMode.PROMISE_IN_BOUNDS,
    )


def centred(value):
    turns = jnp.round(value.astype(F32) * F32(INVERSE)).astype(jnp.int32)
    return (value - turns * MODULUS).astype(F32)


def home_noise(seed, step):
    a = seed.astype(jnp.int32) + (7919 * step + 1 + SEED_MIDDLE)
    return (
        centred(256 * a),
        centred(2 * a),
        centred(a * (a + 1)) + 0.5,
    )


def near_noise(seed):
    b = seed - SEED_MIDDLE
    high = jnp.floor((b + 64.0) * (1.0 / 128.0))
    low = b - 128.0 * high
    whole = b.astype(jnp.int32)
    return high, low, centred(whole * (whole + 1))


def pair_kernel(
    *refs, slots, lanes, sources, rows, own, step, first, last, virial, has_fixed
):
    refs = list(refs)
    take = lambda n: [refs.pop(0) for _ in range(n)]
    turn_ref, shear_ref, home_ref, home_fixed_ref = take(4)
    near_refs = take(sources)
    fixed_refs = take(sources) if has_fixed else near_refs
    force_in = None if first else take(1)[0]
    virial_in = take(1)[0] if (virial and not first) else None
    if last and virial:
        force_out, velocity_out, virial_out = take(3)
    elif virial:
        force_out, virial_out = take(2)
    else:
        (force_out,) = take(1)
    home, near, box, rank, pick, liste, part, total, tally, sizes = take(10)
    groups = slots // SUB
    capacity = liste.shape[0] // 9
    iota = lax.broadcasted_iota(jnp.int32, (SUB, lanes), 0)
    iota_f = iota.astype(F32)
    fixed_at = 6 * slots

    def block(ref, base, group):
        return ref[base + group * SUB : base + (group + 1) * SUB, :]

    def spread(row):
        return jnp.broadcast_to(row, (SUB, lanes))

    home_count = spread(home_fixed_ref[fixed_at + slots : fixed_at + slots + 1, :])
    low = [jnp.full((SUB, lanes), FAR, F32) for _ in range(3)]
    high = [jnp.full((SUB, lanes), -FAR, F32) for _ in range(3)]
    home_there = []
    for g in range(groups):
        there = iota_f + F32(g * SUB) < home_count
        home_there.append(there)
        for a in range(3):
            p = block(home_ref, a * slots, g)
            low[a] = jnp.minimum(low[a], jnp.where(there, p, FAR))
            high[a] = jnp.maximum(high[a], jnp.where(there, p, -FAR))
            home[(a * slots + g * SUB) : (a * slots + (g + 1) * SUB), :] = (
                jnp.where(there, p, -FAR) if a == 0 else p
            )
            home[((3 + a) * slots + g * SUB) : ((3 + a) * slots + (g + 1) * SUB), :] = (
                block(home_ref, (3 + a) * slots, g) * F32(VELOCITY_SCALE)
            )
        for a, value in enumerate(home_noise(block(home_fixed_ref, fixed_at, g), step)):
            at = (6 + a) * slots + g * SUB
            home[at : at + SUB, :] = value
    home_low = [spread(jnp.min(v, axis=0, keepdims=True)) - REACH for v in low]
    home_high = [spread(jnp.max(v, axis=0, keepdims=True)) + REACH for v in high]

    for r, (source, offset, dz, dy) in enumerate(rows):
        data, fixed = near_refs[source], fixed_refs[source]
        base = r * 7 * slots
        amount = turn_ref[0 if dy < 0 else 1] if dy else None
        turned = (lambda v: pltpu.roll(v, amount, 1)) if dy else (lambda v: v)
        count = turned(spread(fixed[offset[1] + fixed_at + slots : offset[1] + fixed_at + slots + 1, :]))
        for g in range(groups):
            there = iota_f + F32(g * SUB) < count
            for c in range(7):
                ref, at = (fixed, offset[1]) if c == 6 else (data, offset[0])
                v = turned(block(ref, at + c * slots, g))
                if c == 0:
                    v = jnp.where(there, v, FAR)
                if c == 1 and dy:
                    v = v + F32(EDGE * dy)
                if c == 2 and dz:
                    v = v + F32(EDGE * dz)
                if c == 3 and dy:
                    v = v + shear_ref[0 if dy < 0 else 1]
                if 3 <= c < 6:
                    v = v * F32(VELOCITY_SCALE)
                near[base + c * slots + g * SUB : base + c * slots + (g + 1) * SUB, :] = v

    def ranked(slot, marks):
        before = jnp.zeros((SUB, lanes), F32)
        for g in range(groups):
            run = jnp.where(marks[g], 1.0, 0.0)
            for d in (1, 2, 4):
                run = run + jnp.where(iota >= d, pltpu.roll(run, d, 0), 0.0)
            place = jnp.where(marks[g], run + (before - 1.0), -1.0)
            rank[(slot * slots + g * SUB) : (slot * slots + (g + 1) * SUB), :] = place
            before = before + spread(run[SUB - 1 : SUB, :])
        sizes[slot] = jnp.max(before).astype(jnp.int32)

    for r, (source, offset, dz, dy) in enumerate(rows):
        base = r * 7 * slots
        near_low = [jnp.full((SUB, lanes), FAR, F32) for _ in range(2)]
        near_high = [jnp.full((SUB, lanes), -FAR, F32) for _ in range(2)]
        for d, dx in enumerate((0, -1, 1)):
            marks = []
            for g in range(groups):
                pos = [
                    near[base + a * slots + g * SUB : base + a * slots + (g + 1) * SUB, :]
                    for a in range(3)
                ]
                if dx:
                    pos = [pltpu.roll(v, (-dx) % lanes, 1) for v in pos]
                    pos[0] = pos[0] + F32(EDGE * dx)
                mark = (pos[0] > home_low[0]) & (pos[0] < home_high[0])
                for a in (1, 2):
                    mark = mark & (pos[a] > home_low[a]) & (pos[a] < home_high[a])
                marks.append(mark)
                if not own:
                    for a in (1, 2):
                        near_low[a - 1] = jnp.minimum(near_low[a - 1], jnp.where(mark, pos[a], FAR))
                        near_high[a - 1] = jnp.maximum(near_high[a - 1], jnp.where(mark, pos[a], -FAR))
            ranked(4 * r + d, marks)
        if not own:
            bounds = [
                (
                    spread(jnp.min(near_low[a], axis=0, keepdims=True)) - REACH,
                    spread(jnp.max(near_high[a], axis=0, keepdims=True)) + REACH,
                )
                for a in range(2)
            ]
            marks = []
            for g in range(groups):
                mark = home_there[g]
                for a in range(2):
                    p = home[(a + 1) * slots + g * SUB : (a + 1) * slots + (g + 1) * SUB, :]
                    mark = mark & (p > bounds[a][0]) & (p < bounds[a][1])
                marks.append(mark)
            ranked(4 * r + 3, marks)

    def choose(slot, k):
        target = iota_f + (k * SUB).astype(F32)
        index = jnp.full((SUB, lanes), -1, jnp.int32)
        for s in range(slots):
            index = jnp.where(rank[pl.ds(slot * slots + s, SUB, stride=0), :] == target, s, index)
        return index

    def gathered(ref, base, index):
        within = index & (SUB - 1)
        result = take_rows(ref[pl.ds(base, SUB), :], within)
        for g in range(1, groups):
            result = jnp.where(
                index >= g * SUB, take_rows(ref[pl.ds(base + g * SUB, SUB), :], within), result
            )
        return result

    def aligned(value):
        return pl.multiple_of(value, SUB)

    def run_pairs(count, where_home, blocks):
        def one(j, carry):
            carry = list(carry)
            n = [liste[pl.ds(c * capacity + j, SUB, stride=0), :] for c in range(9)]
            tot = [None] * 3
            for b in range(blocks):
                h = [where_home[c * slots + b * SUB : c * slots + (b + 1) * SUB, :] for c in range(9)]
                rx, ry, rz = h[0] - n[0], h[1] - n[1], h[2] - n[2]
                squared = jnp.maximum(rx * rx + ry * ry + rz * rz, FLOOR_SQUARED)
                inverse = lax.rsqrt(squared)
                weight = jnp.maximum(1.0 - squared * inverse, 0.0)
                u = weight * inverse
                rv = rx * (h[3] - n[3]) + ry * (h[4] - n[4]) + rz * (h[5] - n[5])
                t = ((h[6] * n[6] + h[7] * n[7]) + (h[8] + n[8])) * F32(INVERSE)
                y = (t - jnp.floor(t)) + F32(SHIFT)
                magnitude = u * (y - u * rv)
                f = [magnitude * rx, magnitude * ry, magnitude * rz]
                for a in range(3):
                    carry[3 * b + a] = carry[3 * b + a] + f[a]
                    tot[a] = f[a] if tot[a] is None else tot[a] + f[a]
            if virial:
                for i, (a, b) in enumerate(COMPONENT_PAIRS):
                    carry[3 * blocks + i] = carry[3 * blocks + i] - n[a] * tot[b]
            return tuple(carry)

        def two(i, carry):
            return one(2 * i + 1, one(2 * i, carry))

        zero = jnp.zeros((SUB, lanes), F32)
        start = (zero,) * (3 * blocks + (6 if virial else 0))
        done = lax.fori_loop(0, (count + 1) // 2, two, start)
        for b in range(blocks):
            for a in range(3):
                part[a * slots + b * SUB : a * slots + (b + 1) * SUB, :] = done[3 * b + a]
        if virial:
            for i, (a, b) in enumerate(COMPONENT_PAIRS):
                value = tally[i * SUB : (i + 1) * SUB, :] + done[3 * blocks + i]
                for g in range(blocks):
                    value = value + (
                        where_home[a * slots + g * SUB : a * slots + (g + 1) * SUB, :] * done[3 * g + b]
                    )
                tally[i * SUB : (i + 1) * SUB, :] = value

    for c in range(3):
        for g in range(groups):
            at = c * slots + g * SUB
            total[at : at + SUB, :] = (
                jnp.zeros((SUB, lanes), F32) if first else force_in[at : at + SUB, :]
            )
    if virial:
        for i in range(6):
            tally[i * SUB : (i + 1) * SUB, :] = (
                jnp.zeros((SUB, lanes), F32) if first else virial_in[i * SUB : (i + 1) * SUB, :]
            )

    def direction(r, _):
        base = r * (7 * slots)
        filled = jnp.int32(0)
        for d, dx in enumerate((0, -1, 1)):
            slot = 4 * r + d
            size = sizes[slot]

            def fill(k, _, slot=slot, dx=dx, filled=filled):
                index = choose(slot, k)
                valid = index >= 0
                values = [
                    gathered_near(base + c * slots, index, dx) for c in range(7)
                ]
                values[0] = jnp.where(valid, values[0] + F32(EDGE * dx), FAR)
                values = values[:6] + list(near_noise(values[6]))
                for c in range(9):
                    liste[pl.ds(c * capacity + filled + k * SUB, SUB), :] = values[c]
                return 0

            def gathered_near(at, index, dx):
                within = index & (SUB - 1)
                result = None
                for g in range(groups):
                    v = near[pl.ds(aligned(at + g * SUB), SUB), :]
                    if dx:
                        v = pltpu.roll(v, (-dx) % lanes, 1)
                    v = take_rows(v, within)
                    result = v if g == 0 else jnp.where(index >= g * SUB, v, result)
                return result

            lax.fori_loop(0, (size + SUB - 1) // SUB, fill, 0)
            filled = filled + size
        liste[pl.ds(filled, SUB), :] = jnp.full((SUB, lanes), FAR, F32)
        for c in range(1, 9):
            liste[pl.ds(c * capacity + filled, SUB), :] = jnp.zeros((SUB, lanes), F32)
        if own:
            run_pairs(filled, home, groups)
            for c in range(3):
                for g in range(groups):
                    at = c * slots + g * SUB
                    total[at : at + SUB, :] = total[at : at + SUB, :] + part[at : at + SUB, :]
            return 0
        slot = 4 * r + 3
        needed = (sizes[slot] + SUB - 1) // SUB

        def fill_home(k, _):
            index = choose(slot, k)
            for c in range(9):
                v = gathered(home, c * slots, index)
                if c == 0:
                    v = jnp.where(index >= 0, v, -FAR)
                pick[pl.ds(aligned(c * slots + k * SUB), SUB), :] = v
            return 0

        lax.fori_loop(0, needed, fill_home, 0)
        for blocks in range(1, groups + 1):
            pl.when(needed == blocks)(functools.partial(run_pairs, filled, pick, blocks))

        def back(k, _):
            for g in range(groups):
                place = rank[pl.ds(aligned(slot * slots + g * SUB), SUB), :].astype(jnp.int32)
                mine = (place >= k * SUB) & (place < (k + 1) * SUB)
                within = place & (SUB - 1)
                for c in range(3):
                    at = c * slots + g * SUB
                    v = take_rows(part[pl.ds(aligned(c * slots + k * SUB), SUB), :], within)
                    total[at : at + SUB, :] = total[at : at + SUB, :] + jnp.where(mine, v, 0.0)
            return 0

        lax.fori_loop(0, needed, back, 0)
        return 0

    if len(rows) == 1:
        direction(jnp.int32(0), 0)
    else:
        lax.fori_loop(0, len(rows), direction, 0)

    half = F32(0.5 * TIME_STEP)
    for c in range(3):
        for g in range(groups):
            at = c * slots + g * SUB
            f = total[at : at + SUB, :]
            if not last:
                force_out[at : at + SUB, :] = f
                continue
            f = f * F32(NOISE_UNIT)
            v = block(home_ref, (3 + c) * slots, g) + half * f
            if virial:
                force_out[at : at + SUB, :] = f
                velocity_out[at : at + SUB, :] = jnp.where(home_there[g], v, 0.0)
            else:
                v = v + half * f
                force_out[at : at + SUB, :] = block(home_ref, c * slots, g) + F32(TIME_STEP) * v
                force_out[3 * slots + at : 3 * slots + at + SUB, :] = v
    if virial:
        for i in range(6):
            v = tally[i * SUB : (i + 1) * SUB, :]
            if last:
                virial_out[i : i + 1, :] = jnp.sum(v, axis=0, keepdims=True) * F32(
                    NOISE_UNIT * 0.5 / CELL_VOLUME
                )
            else:
                virial_out[i * SUB : (i + 1) * SUB, :] = v


def pairs(turn, shear, home, home_fixed, nears, fixed, carried, rows, step, last, virial, slots, cost):
    lanes = home.shape[-1]
    own = len(rows) == 1
    first = carried is None
    operands = [turn, shear, home, home_fixed, *nears]
    if fixed is not None:
        operands += list(fixed)
    if not first:
        operands += list(carried)
    shape = lambda n: jax.ShapeDtypeStruct((n, lanes), F32)
    if last and virial:
        outs = (shape(3 * slots), shape(3 * slots), shape(6))
    elif virial:
        outs = (shape(3 * slots), shape(6 * SUB))
    elif last:
        outs = (shape(6 * slots),)
    else:
        outs = (shape(3 * slots),)
    vmem = pl.BlockSpec(memory_space=pltpu.VMEM)
    smem = pl.BlockSpec(memory_space=pltpu.SMEM)
    capacity = 3 * slots + 2 * SUB
    count = len(rows)
    return pl.pallas_call(
        functools.partial(
            pair_kernel,
            slots=slots,
            lanes=lanes,
            sources=len(nears),
            rows=rows,
            own=own,
            step=step,
            first=first,
            last=last,
            virial=virial,
            has_fixed=fixed is not None,
        ),
        out_shape=outs,
        in_specs=[smem, smem] + [vmem] * (len(operands) - 2),
        out_specs=tuple(vmem for _ in outs),
        scratch_shapes=[
            pltpu.VMEM((9 * slots, lanes), F32),
            pltpu.VMEM((count * 7 * slots, lanes), F32),
            pltpu.VMEM((SUB, lanes), F32),
            pltpu.VMEM((count * 4 * slots, lanes), F32),
            pltpu.VMEM((9 * slots, lanes), F32),
            pltpu.VMEM((9 * capacity, lanes), F32),
            pltpu.VMEM((3 * slots, lanes), F32),
            pltpu.VMEM((3 * slots, lanes), F32),
            pltpu.VMEM((6 * SUB, lanes), F32),
            pltpu.SMEM((4 * count,), jnp.int32),
        ],
        cost_estimate=pl.CostEstimate(flops=cost, bytes_accessed=1, transcendentals=0),
        name=f"pairs_{count}_{step}",
    )(*operands)


def kick_kernel(position, velocity, force, seed, count, out, *, slots, lanes):
    for c in range(3):
        for g in range(slots // SUB):
            at = c * slots + g * SUB
            rows = slice(at, at + SUB)
            v = velocity[rows, :] + F32(0.5 * TIME_STEP) * force[rows, :]
            out[rows, :] = position[rows, :] + F32(TIME_STEP) * v
            out[3 * slots + at : 3 * slots + at + SUB, :] = v
    out[6 * slots : 7 * slots, :] = seed[...].astype(F32)
    out[7 * slots : 7 * slots + SUB, :] = jnp.broadcast_to(count[...], (SUB, lanes)).astype(F32)


def ring(count, by):
    return [(i, (i + by) % count) for i in range(count)]


def shards(positions, velocities, forces_prev, seeds, counts, offsets):
    slots, depth, width, lanes = seeds.shape
    assert depth == 1 and width == 1
    gz, xy = lax.axis_size("gz"), lax.axis_size("xy")
    index = lax.axis_index("xy")
    flat = lambda a: a.reshape(-1, lanes)
    tall = 7 * slots + SUB
    state = pl.pallas_call(
        functools.partial(kick_kernel, slots=slots, lanes=lanes),
        out_shape=jax.ShapeDtypeStruct((tall, lanes), F32),
        in_specs=[pl.BlockSpec(memory_space=pltpu.VMEM)] * 5,
        out_specs=pl.BlockSpec(memory_space=pltpu.VMEM),
        name="kick",
    )(flat(positions), flat(velocities), flat(forces_prev), flat(seeds), flat(counts))
    first_lower, first_upper = index == 0, index == xy - 1
    shear = jnp.stack(
        [jnp.where(first_lower, -SHEAR_SPEED, 0.0), jnp.where(first_upper, SHEAR_SPEED, 0.0)]
    ).astype(F32)
    home_fixed = state
    kept = None
    for step in range(2):
        offset = offsets[step]
        turn = jnp.stack(
            [
                jnp.where(first_lower, (lanes - offset) % lanes, 0),
                jnp.where(first_upper, offset % lanes, 0),
            ]
        ).astype(jnp.int32)
        final = step == 1
        high = state.shape[0]
        planes = [lax.ppermute(state, "gz", ring(gz, -1))]
        if gz > 2:
            planes.append(lax.ppermute(state, "gz", ring(gz, 1)))
        up, down = 0, len(planes) - 1
        stacked = jnp.concatenate([state, *planes], axis=0)
        lower = lax.ppermute(stacked, "xy", ring(xy, 1))
        upper = lax.ppermute(stacked, "xy", ring(xy, -1))
        if not final:
            kept = (planes, lower, upper)
            fixed = [None] * 3
        else:
            fixed = [[home_fixed], kept[0], [kept[1], kept[2]]]
        call = functools.partial(
            pairs, turn, shear, state, home_fixed, step=step, virial=final, slots=slots
        )
        here = (0, 0)
        carried = call(
            [state], fixed[0], None, rows=((0, here, 0, 0),), last=False, cost=4_000_000
        )
        carried = call(
            planes,
            fixed[1],
            carried,
            rows=((down, here, -1, 0), (up, here, 1, 0)),
            last=False,
            cost=4_000_000,
        )
        rows = []
        for source, dy in ((0, -1), (1, 1)):
            for dz, place in ((0, 0), (-1, 1 + down), (1, 1 + up)):
                rows.append((source, (place * high, place * tall), dz, dy))
        outs = call(
            [lower, upper], fixed[2], carried, rows=tuple(rows), last=True, cost=8_000_000
        )
        if not final:
            state = outs[0]
    force, velocity, stress = outs
    return (
        force.reshape(positions.shape),
        velocity.reshape(positions.shape),
        stress.reshape(6, depth, width, lanes),
    )


def solution(mesh):
    beads = P(None, None, "gz", "xy", None)
    return jax.shard_map(
        shards,
        mesh=mesh,
        in_specs=(beads, beads, beads, P(None, "gz", "xy", None), P("gz", "xy", None), P()),
        out_specs=(beads, beads, P(None, "gz", "xy", None)),
        check_vma=False,
    )
```

```python
import functools
import math

import jax
import jax.numpy as jnp
from jax import lax
from jax.experimental import pallas as pl
from jax.experimental.pallas import tpu as pltpu
from jax.sharding import PartitionSpec as P

CONSERVATIVE = 25.0
FRICTION = 4.5
NOISE_LEVEL = 3.0
TIME_STEP = 0.04
SHEAR_SPEED = 1.0
CELL_VOLUME = 8.0
FLOOR_SQUARED = 0.0025
EDGE = 2.0
MODULUS = 65521
COMPONENT_PAIRS = [(0, 0), (1, 1), (2, 2), (0, 1), (0, 2), (1, 2)]

NOISE_UNIT = NOISE_LEVEL * math.sqrt(12.0) / math.sqrt(TIME_STEP)
SHIFT = CONSERVATIVE / NOISE_UNIT - 0.5 - 0.5 / MODULUS
VELOCITY_SCALE = FRICTION / NOISE_UNIT
INVERSE = 1.0 / MODULUS
FAR = 1.0e15
REACH = 1.001
SEED_MIDDLE = 8192
F32 = jnp.float32
SUB = 8
VMEM_LIMIT = 6 * 2**20
KICK_LIMIT = 67043328 - 160 * 1024


def take_rows(values, index):
    dims = lax.GatherDimensionNumbers(
        offset_dims=(),
        collapsed_slice_dims=(0,),
        start_index_map=(0,),
        operand_batching_dims=(1,),
        start_indices_batching_dims=(1,),
    )
    return lax.gather(
        values,
        index[..., None],
        dims,
        slice_sizes=(1, 1),
        mode=lax.GatherScatterMode.PROMISE_IN_BOUNDS,
    )


def centred(value):
    turns = jnp.round(value.astype(F32) * F32(INVERSE)).astype(jnp.int32)
    return (value - turns * MODULUS).astype(F32)


def home_noise(seed, step):
    a = seed.astype(jnp.int32) + (7919 * step + 1 + SEED_MIDDLE)
    return (
        centred(256 * a),
        centred(2 * a),
        centred(a * (a + 1)) + 0.5,
    )


def near_noise(seed):
    b = seed - SEED_MIDDLE
    high = jnp.floor((b + 64.0) * (1.0 / 128.0))
    low = b - 128.0 * high
    whole = b.astype(jnp.int32)
    return high, low, centred(whole * (whole + 1))


def pair_kernel(
    *refs, slots, lanes, sources, rows, own, step, first, last, virial, has_fixed
):
    refs = list(refs)
    take = lambda n: [refs.pop(0) for _ in range(n)]
    offset_ref, home_ref, home_fixed_ref = take(3)
    near_refs = take(sources)
    fixed_refs = take(sources) if has_fixed else near_refs
    force_in = None if first else take(1)[0]
    virial_in = take(1)[0] if (virial and not first) else None
    if last and virial:
        force_out, velocity_out, virial_out = take(3)
    elif virial:
        force_out, virial_out = take(2)
    else:
        (force_out,) = take(1)
    home, near, box, rank, pick, liste, part, total, tally, sizes = take(10)
    groups = slots // SUB
    capacity = liste.shape[0] // 9
    iota = lax.broadcasted_iota(jnp.int32, (SUB, lanes), 0)
    iota_f = iota.astype(F32)
    fixed_at = 6 * slots
    turns = shears = None
    if any(dy for _, _, _, dy in rows):
        index, count = lax.axis_index("xy"), lax.axis_size("xy")
        amount = offset_ref[step]
        turns = (
            jnp.where((index == 0) & (amount > 0), lanes - amount, 0),
            jnp.where(index == count - 1, amount, 0),
        )
        shears = (
            jnp.where(index == 0, F32(-SHEAR_SPEED), F32(0.0)),
            jnp.where(index == count - 1, F32(SHEAR_SPEED), F32(0.0)),
        )

    def block(ref, base, group):
        return ref[base + group * SUB : base + (group + 1) * SUB, :]

    def spread(row):
        return jnp.broadcast_to(row, (SUB, lanes))

    home_count = spread(home_fixed_ref[fixed_at + slots : fixed_at + slots + 1, :])
    low = [jnp.full((SUB, lanes), FAR, F32) for _ in range(3)]
    high = [jnp.full((SUB, lanes), -FAR, F32) for _ in range(3)]
    home_there = []
    for g in range(groups):
        there = iota_f + F32(g * SUB) < home_count
        home_there.append(there)
        for a in range(3):
            p = block(home_ref, a * slots, g)
            low[a] = jnp.minimum(low[a], jnp.where(there, p, FAR))
            high[a] = jnp.maximum(high[a], jnp.where(there, p, -FAR))
            home[(a * slots + g * SUB) : (a * slots + (g + 1) * SUB), :] = (
                jnp.where(there, p, -FAR) if a == 0 else p
            )
            home[((3 + a) * slots + g * SUB) : ((3 + a) * slots + (g + 1) * SUB), :] = (
                block(home_ref, (3 + a) * slots, g) * F32(VELOCITY_SCALE)
            )
        for a, value in enumerate(home_noise(block(home_fixed_ref, fixed_at, g), step)):
            at = (6 + a) * slots + g * SUB
            home[at : at + SUB, :] = value
    home_low = [spread(jnp.min(v, axis=0, keepdims=True)) - REACH for v in low]
    home_high = [spread(jnp.max(v, axis=0, keepdims=True)) + REACH for v in high]

    for r, (source, offset, dz, dy) in enumerate(rows):
        data, fixed = near_refs[source], fixed_refs[source]
        base = r * 7 * slots
        amount = turns[0 if dy < 0 else 1] if dy else None
        turned = (lambda v: pltpu.roll(v, amount, 1)) if dy else (lambda v: v)
        count = turned(spread(fixed[offset[1] + fixed_at + slots : offset[1] + fixed_at + slots + 1, :]))
        for g in range(groups):
            there = iota_f + F32(g * SUB) < count
            for c in range(7):
                ref, at = (fixed, offset[1]) if c == 6 else (data, offset[0])
                v = turned(block(ref, at + c * slots, g))
                if c == 0:
                    v = jnp.where(there, v, FAR)
                if c == 1 and dy:
                    v = v + F32(EDGE * dy)
                if c == 2 and dz:
                    v = v + F32(EDGE * dz)
                if c == 3 and dy:
                    v = v + shears[0 if dy < 0 else 1]
                if 3 <= c < 6:
                    v = v * F32(VELOCITY_SCALE)
                near[base + c * slots + g * SUB : base + c * slots + (g + 1) * SUB, :] = v

    def ranked(slot, marks):
        before = jnp.zeros((SUB, lanes), F32)
        for g in range(groups):
            run = jnp.where(marks[g], 1.0, 0.0)
            for d in (1, 2, 4):
                run = run + jnp.where(iota >= d, pltpu.roll(run, d, 0), 0.0)
            place = jnp.where(marks[g], run + (before - 1.0), -1.0)
            rank[(slot * slots + g * SUB) : (slot * slots + (g + 1) * SUB), :] = place
            before = before + spread(run[SUB - 1 : SUB, :])
        sizes[slot] = jnp.max(before).astype(jnp.int32)

    for r, (source, offset, dz, dy) in enumerate(rows):
        base = r * 7 * slots
        near_low = [jnp.full((SUB, lanes), FAR, F32) for _ in range(2)]
        near_high = [jnp.full((SUB, lanes), -FAR, F32) for _ in range(2)]
        for d, dx in enumerate((0, -1, 1)):
            marks = []
            for g in range(groups):
                pos = [
                    near[base + a * slots + g * SUB : base + a * slots + (g + 1) * SUB, :]
                    for a in range(3)
                ]
                if dx:
                    pos = [pltpu.roll(v, (-dx) % lanes, 1) for v in pos]
                    pos[0] = pos[0] + F32(EDGE * dx)
                mark = (pos[0] > home_low[0]) & (pos[0] < home_high[0])
                for a in (1, 2):
                    mark = mark & (pos[a] > home_low[a]) & (pos[a] < home_high[a])
                marks.append(mark)
                if not own:
                    for a in (1, 2):
                        near_low[a - 1] = jnp.minimum(near_low[a - 1], jnp.where(mark, pos[a], FAR))
                        near_high[a - 1] = jnp.maximum(near_high[a - 1], jnp.where(mark, pos[a], -FAR))
            ranked(4 * r + d, marks)
        if not own:
            bounds = [
                (
                    spread(jnp.min(near_low[a], axis=0, keepdims=True)) - REACH,
                    spread(jnp.max(near_high[a], axis=0, keepdims=True)) + REACH,
                )
                for a in range(2)
            ]
            marks = []
            for g in range(groups):
                mark = home_there[g]
                for a in range(2):
                    p = home[(a + 1) * slots + g * SUB : (a + 1) * slots + (g + 1) * SUB, :]
                    mark = mark & (p > bounds[a][0]) & (p < bounds[a][1])
                marks.append(mark)
            ranked(4 * r + 3, marks)

    def choose(slot, k):
        target = iota_f + (k * SUB).astype(F32)
        index = jnp.full((SUB, lanes), -1, jnp.int32)
        for s in range(slots):
            index = jnp.where(rank[pl.ds(slot * slots + s, SUB, stride=0), :] == target, s, index)
        return index

    def gathered(ref, base, index):
        within = index & (SUB - 1)
        result = take_rows(ref[pl.ds(base, SUB), :], within)
        for g in range(1, groups):
            result = jnp.where(
                index >= g * SUB, take_rows(ref[pl.ds(base + g * SUB, SUB), :], within), result
            )
        return result

    def aligned(value):
        return pl.multiple_of(value, SUB)

    def run_pairs(count, where_home, blocks):
        def one(j, carry):
            carry = list(carry)
            n = [liste[pl.ds(c * capacity + j, SUB, stride=0), :] for c in range(9)]
            tot = [None] * 3
            for b in range(blocks):
                h = [where_home[c * slots + b * SUB : c * slots + (b + 1) * SUB, :] for c in range(9)]
                rx, ry, rz = h[0] - n[0], h[1] - n[1], h[2] - n[2]
                squared = jnp.maximum(rx * rx + ry * ry + rz * rz, FLOOR_SQUARED)
                inverse = lax.rsqrt(squared)
                u = jnp.maximum(inverse - 1.0, 0.0)
                rv = rx * (h[3] - n[3]) + ry * (h[4] - n[4]) + rz * (h[5] - n[5])
                t = ((h[6] * n[6] + h[7] * n[7]) + (h[8] + n[8])) * F32(INVERSE)
                y = (t - jnp.floor(t)) + F32(SHIFT)
                magnitude = u * (y - u * rv)
                f = [magnitude * rx, magnitude * ry, magnitude * rz]
                for a in range(3):
                    carry[3 * b + a] = carry[3 * b + a] + f[a]
                    tot[a] = f[a] if tot[a] is None else tot[a] + f[a]
            if virial:
                for i, (a, b) in enumerate(COMPONENT_PAIRS):
                    carry[3 * blocks + i] = carry[3 * blocks + i] - n[a] * tot[b]
            return tuple(carry)

        def two(i, carry):
            return one(2 * i + 1, one(2 * i, carry))

        zero = jnp.zeros((SUB, lanes), F32)
        start = (zero,) * (3 * blocks + (6 if virial else 0))
        done = lax.fori_loop(0, (count + 1) // 2, two, start)
        for b in range(blocks):
            for a in range(3):
                part[a * slots + b * SUB : a * slots + (b + 1) * SUB, :] = done[3 * b + a]
        if virial:
            for i, (a, b) in enumerate(COMPONENT_PAIRS):
                value = tally[i * SUB : (i + 1) * SUB, :] + done[3 * blocks + i]
                for g in range(blocks):
                    value = value + (
                        where_home[a * slots + g * SUB : a * slots + (g + 1) * SUB, :] * done[3 * g + b]
                    )
                tally[i * SUB : (i + 1) * SUB, :] = value

    for c in range(3):
        for g in range(groups):
            at = c * slots + g * SUB
            total[at : at + SUB, :] = (
                jnp.zeros((SUB, lanes), F32) if first else force_in[at : at + SUB, :]
            )
    if virial:
        for i in range(6):
            tally[i * SUB : (i + 1) * SUB, :] = (
                jnp.zeros((SUB, lanes), F32) if first else virial_in[i * SUB : (i + 1) * SUB, :]
            )

    def direction(r, _):
        base = r * (7 * slots)
        filled = jnp.int32(0)
        for d, dx in enumerate((0, -1, 1)):
            slot = 4 * r + d
            size = sizes[slot]

            def fill(k, _, slot=slot, dx=dx, filled=filled):
                index = choose(slot, k)
                valid = index >= 0
                values = [
                    gathered_near(base + c * slots, index, dx) for c in range(7)
                ]
                values[0] = jnp.where(valid, values[0] + F32(EDGE * dx), FAR)
                values = values[:6] + list(near_noise(values[6]))
                for c in range(9):
                    liste[pl.ds(c * capacity + filled + k * SUB, SUB), :] = values[c]
                return 0

            def gathered_near(at, index, dx):
                within = index & (SUB - 1)
                result = None
                for g in range(groups):
                    v = near[pl.ds(aligned(at + g * SUB), SUB), :]
                    if dx:
                        v = pltpu.roll(v, (-dx) % lanes, 1)
                    v = take_rows(v, within)
                    result = v if g == 0 else jnp.where(index >= g * SUB, v, result)
                return result

            lax.fori_loop(0, (size + SUB - 1) // SUB, fill, 0)
            filled = filled + size
        liste[pl.ds(filled, SUB), :] = jnp.full((SUB, lanes), FAR, F32)
        for c in range(1, 9):
            liste[pl.ds(c * capacity + filled, SUB), :] = jnp.zeros((SUB, lanes), F32)
        if own:
            run_pairs(filled, home, groups)
            for c in range(3):
                for g in range(groups):
                    at = c * slots + g * SUB
                    total[at : at + SUB, :] = total[at : at + SUB, :] + part[at : at + SUB, :]
            return 0
        slot = 4 * r + 3
        needed = (sizes[slot] + SUB - 1) // SUB

        def fill_home(k, _):
            index = choose(slot, k)
            for c in range(9):
                v = gathered(home, c * slots, index)
                if c == 0:
                    v = jnp.where(index >= 0, v, -FAR)
                pick[pl.ds(aligned(c * slots + k * SUB), SUB), :] = v
            return 0

        lax.fori_loop(0, needed, fill_home, 0)
        for blocks in range(1, groups + 1):
            pl.when(needed == blocks)(functools.partial(run_pairs, filled, pick, blocks))

        def back(k, _):
            for g in range(groups):
                place = rank[pl.ds(aligned(slot * slots + g * SUB), SUB), :].astype(jnp.int32)
                mine = (place >= k * SUB) & (place < (k + 1) * SUB)
                within = place & (SUB - 1)
                for c in range(3):
                    at = c * slots + g * SUB
                    v = take_rows(part[pl.ds(aligned(c * slots + k * SUB), SUB), :], within)
                    total[at : at + SUB, :] = total[at : at + SUB, :] + jnp.where(mine, v, 0.0)
            return 0

        lax.fori_loop(0, needed, back, 0)
        return 0

    if len(rows) == 1:
        direction(jnp.int32(0), 0)
    else:
        lax.fori_loop(0, len(rows), direction, 0)

    half = F32(0.5 * TIME_STEP)
    for c in range(3):
        for g in range(groups):
            at = c * slots + g * SUB
            f = total[at : at + SUB, :]
            if not last:
                force_out[at : at + SUB, :] = f
                continue
            f = f * F32(NOISE_UNIT)
            v = block(home_ref, (3 + c) * slots, g) + half * f
            if virial:
                force_out[at : at + SUB, :] = f
                velocity_out[at : at + SUB, :] = jnp.where(home_there[g], v, 0.0)
            else:
                v = v + half * f
                force_out[at : at + SUB, :] = block(home_ref, c * slots, g) + F32(TIME_STEP) * v
                force_out[3 * slots + at : 3 * slots + at + SUB, :] = v
    if virial:
        for i in range(6):
            v = tally[i * SUB : (i + 1) * SUB, :]
            if last:
                virial_out[i] = jnp.sum(v, axis=0, keepdims=True) * F32(
                    NOISE_UNIT * 0.5 / CELL_VOLUME
                )
            else:
                virial_out[i * SUB : (i + 1) * SUB, :] = v


def pairs(offsets, home, home_fixed, nears, fixed, carried, rows, step, last, virial, slots, cost):
    lanes = home.shape[-1]
    own = len(rows) == 1
    first = carried is None
    operands = [offsets, home, home_fixed, *nears]
    if fixed is not None:
        operands += list(fixed)
    if not first:
        operands += list(carried)
    shape = lambda n: jax.ShapeDtypeStruct((n, lanes), F32)
    if last and virial:
        outs = (shape(3 * slots), shape(3 * slots), jax.ShapeDtypeStruct((6, 1, lanes), F32))
    elif virial:
        outs = (shape(3 * slots), shape(6 * SUB))
    elif last:
        outs = (shape(6 * slots),)
    else:
        outs = (shape(3 * slots),)
    vmem = pl.BlockSpec(memory_space=pltpu.VMEM)
    smem = pl.BlockSpec(memory_space=pltpu.SMEM)
    capacity = 3 * slots + 2 * SUB
    count = len(rows)
    return pl.pallas_call(
        functools.partial(
            pair_kernel,
            slots=slots,
            lanes=lanes,
            sources=len(nears),
            rows=rows,
            own=own,
            step=step,
            first=first,
            last=last,
            virial=virial,
            has_fixed=fixed is not None,
        ),
        out_shape=outs,
        in_specs=[smem] + [vmem] * (len(operands) - 1),
        out_specs=tuple(vmem for _ in outs),
        scratch_shapes=[
            pltpu.VMEM((9 * slots, lanes), F32),
            pltpu.VMEM((count * 7 * slots, lanes), F32),
            pltpu.VMEM((SUB, lanes), F32),
            pltpu.VMEM((count * 4 * slots, lanes), F32),
            pltpu.VMEM((9 * slots, lanes), F32),
            pltpu.VMEM((9 * capacity, lanes), F32),
            pltpu.VMEM((3 * slots, lanes), F32),
            pltpu.VMEM((3 * slots, lanes), F32),
            pltpu.VMEM((6 * SUB, lanes), F32),
            pltpu.SMEM((4 * count,), jnp.int32),
        ],
        compiler_params=pltpu.CompilerParams(vmem_limit_bytes=VMEM_LIMIT),
        cost_estimate=pl.CostEstimate(flops=cost, bytes_accessed=1, transcendentals=0),
        name=f"pairs_{count}_{step}",
    )(*operands)


def kick_kernel(*refs, slots, lanes):
    sources, out, held, done = refs[:5], refs[5], refs[6:11], refs[11]
    copies = [
        pltpu.make_async_copy(source, target, done.at[i])
        for i, (source, target) in enumerate(zip(sources, held))
    ]
    for copy in copies:
        copy.start()
    for copy in copies:
        copy.wait()
    position, velocity, force, seed, count = held
    for c in range(3):
        for g in range(slots // SUB):
            at = c * slots + g * SUB
            rows = slice(at, at + SUB)
            v = velocity[rows, :] + F32(0.5 * TIME_STEP) * force[rows, :]
            out[rows, :] = position[rows, :] + F32(TIME_STEP) * v
            out[3 * slots + at : 3 * slots + at + SUB, :] = v
    out[6 * slots : 7 * slots, :] = seed[...].astype(F32)
    out[7 * slots : 7 * slots + SUB, :] = jnp.broadcast_to(count[...], (SUB, lanes)).astype(F32)


def ring(count, by):
    return [(i, (i + by) % count) for i in range(count)]


def shards(positions, velocities, forces_prev, seeds, counts, offsets):
    slots, depth, width, lanes = seeds.shape
    assert depth == 1 and width == 1
    gz, xy = lax.axis_size("gz"), lax.axis_size("xy")
    flat = lambda a: a.reshape(-1, lanes)
    tall = 7 * slots + SUB
    inputs = [flat(a) for a in (positions, velocities, forces_prev, seeds, counts)]
    state = pl.pallas_call(
        functools.partial(kick_kernel, slots=slots, lanes=lanes),
        out_shape=jax.ShapeDtypeStruct((tall, lanes), F32),
        in_specs=[pl.BlockSpec(memory_space=pltpu.HBM)] * 5,
        out_specs=pl.BlockSpec(memory_space=pltpu.VMEM),
        scratch_shapes=[pltpu.VMEM(a.shape, a.dtype) for a in inputs]
        + [pltpu.SemaphoreType.DMA((5,))],
        compiler_params=pltpu.CompilerParams(vmem_limit_bytes=KICK_LIMIT),
        name="kick",
    )(*inputs)
    home_fixed = state
    kept = None
    for step in range(2):
        final = step == 1
        high = state.shape[0]
        planes = [lax.ppermute(state, "gz", ring(gz, -1))]
        if gz > 2:
            planes.append(lax.ppermute(state, "gz", ring(gz, 1)))
        up, down = 0, len(planes) - 1
        near_fixed = lambda at: None if not final else kept[at]
        call = functools.partial(
            pairs, offsets, state, home_fixed, step=step, virial=final, slots=slots
        )
        here = (0, 0)
        carried = call(
            [state],
            [home_fixed] if final else None,
            None,
            rows=((0, here, 0, 0),),
            last=False,
            cost=100_000_000,
        )
        planes, carried = lax.optimization_barrier((planes, carried))
        stacked = jnp.concatenate([state, *planes], axis=0)
        lower = lax.ppermute(stacked, "xy", ring(xy, 1))
        upper = lax.ppermute(stacked, "xy", ring(xy, -1))
        carried = call(
            planes,
            near_fixed(0),
            carried,
            rows=((down, here, -1, 0), (up, here, 1, 0)),
            last=False,
            cost=100_000_000,
        )
        rows = []
        for source, dy in ((0, -1), (1, 1)):
            for dz, place in ((0, 0), (-1, 1 + down), (1, 1 + up)):
                rows.append((source, (place * high, place * tall), dz, dy))
        outs = call(
            [lower, upper], near_fixed(1), carried, rows=tuple(rows), last=True, cost=200_000_000
        )
        if not final:
            kept = (planes, [lower, upper])
            state = outs[0]
    force, velocity, stress = outs
    return (
        force.reshape(positions.shape),
        velocity.reshape(positions.shape),
        stress.reshape(6, depth, width, lanes),
    )


def solution(mesh):
    beads = P(None, None, "gz", "xy", None)
    return jax.shard_map(
        shards,
        mesh=mesh,
        in_specs=(beads, beads, beads, P(None, "gz", "xy", None), P("gz", "xy", None), P()),
        out_specs=(beads, beads, P(None, "gz", "xy", None)),
        check_vma=False,
    )
```

```python
import functools
import math

import jax
import jax.numpy as jnp
from jax import lax
from jax.experimental import pallas as pl
from jax.experimental.pallas import tpu as pltpu
from jax.sharding import PartitionSpec as P

CONSERVATIVE = 25.0
FRICTION = 4.5
NOISE_LEVEL = 3.0
TIME_STEP = 0.04
SHEAR_SPEED = 1.0
CELL_VOLUME = 8.0
FLOOR_SQUARED = 0.0025
EDGE = 2.0
MODULUS = 65521
COMPONENT_PAIRS = [(0, 0), (1, 1), (2, 2), (0, 1), (0, 2), (1, 2)]

NOISE_UNIT = NOISE_LEVEL * math.sqrt(12.0) / math.sqrt(TIME_STEP)
SHIFT = CONSERVATIVE / NOISE_UNIT - 0.5 - 0.5 / MODULUS
VELOCITY_SCALE = FRICTION / NOISE_UNIT
INVERSE = 1.0 / MODULUS
FAR = 1.0e15
REACH = 1.001
SEED_MIDDLE = 8192
NEAR_SIDE, FAR_SIDE = 1, 2
F32 = jnp.float32
SUB = 8
UNROLL = 4
VMEM_LIMIT = 6 * 2**20
KICK_LIMIT = 67043328 - 160 * 1024


def take_rows(values, index):
    dims = lax.GatherDimensionNumbers(
        offset_dims=(),
        collapsed_slice_dims=(0,),
        start_index_map=(0,),
        operand_batching_dims=(1,),
        start_indices_batching_dims=(1,),
    )
    return lax.gather(
        values,
        index[..., None],
        dims,
        slice_sizes=(1, 1),
        mode=lax.GatherScatterMode.PROMISE_IN_BOUNDS,
    )


def centred(value):
    turns = jnp.round(value.astype(F32) * F32(INVERSE)).astype(jnp.int32)
    return (value - turns * MODULUS).astype(F32)


def home_noise(seed, step):
    a = seed.astype(jnp.int32) + (7919 * step + 1 + SEED_MIDDLE)
    return (
        centred(256 * a),
        centred(2 * a),
        centred(a * (a + 1)) + 0.5,
    )


def near_noise(seed):
    b = seed - SEED_MIDDLE
    high = jnp.floor((b + 64.0) * (1.0 / 128.0))
    low = b - 128.0 * high
    whole = b.astype(jnp.int32)
    return high, low, centred(whole * (whole + 1))


def pair_kernel(
    *refs, slots, lanes, sources, rows, own, step, first, last, virial, has_fixed, side
):
    refs = list(refs)
    take = lambda n: [refs.pop(0) for _ in range(n)]
    offset_ref, home_ref, home_fixed_ref = take(3)
    near_refs = take(sources)
    fixed_refs = take(sources) if has_fixed else near_refs
    force_in = None if first else take(1)[0]
    virial_in = take(1)[0] if (virial and not first) else None
    if last and virial:
        force_out, velocity_out, virial_out = take(3)
    elif virial:
        force_out, virial_out = take(2)
    else:
        (force_out,) = take(1)
    home, near, answer, rank, pick, liste, part, total, tally, sizes = take(10)
    groups = slots // SUB
    pitch = slots + SUB
    capacity = liste.shape[0] // 9
    iota = lax.broadcasted_iota(jnp.int32, (SUB, lanes), 0)
    iota_f = iota.astype(F32)
    fixed_at = 6 * slots
    if side:
        index, count = lax.axis_index("xy"), lax.axis_size("xy")
        upper = (lax.rem(index, 2) == 0) == (side == NEAR_SIDE)
        across = jnp.where(upper, F32(1.0), F32(-1.0))
        wraps = jnp.where(upper, index == count - 1, index == 0)
        amount = offset_ref[step]
        turn = jnp.where(upper, amount, lax.rem(lanes - amount, lanes))
        turn = jnp.where(wraps, turn, 0)
        shear = jnp.where(wraps, across * F32(SHEAR_SPEED), F32(0.0))
        turning = side != NEAR_SIDE
    else:
        turning = False

    def block(ref, base, group):
        return ref[base + group * SUB : base + (group + 1) * SUB, :]

    def spread(row):
        return jnp.broadcast_to(row, (SUB, lanes))

    home_count = spread(home_fixed_ref[fixed_at + slots : fixed_at + slots + 1, :])
    low = [jnp.full((SUB, lanes), FAR, F32) for _ in range(3)]
    high = [jnp.full((SUB, lanes), -FAR, F32) for _ in range(3)]
    home_there = []
    for g in range(groups):
        there = iota_f + F32(g * SUB) < home_count
        home_there.append(there)
        for a in range(3):
            p = block(home_ref, a * slots, g)
            low[a] = jnp.minimum(low[a], jnp.where(there, p, FAR))
            high[a] = jnp.maximum(high[a], jnp.where(there, p, -FAR))
            home[(a * pitch + g * SUB) : (a * pitch + (g + 1) * SUB), :] = (
                jnp.where(there, p, -FAR) if a == 0 else p
            )
            home[((3 + a) * pitch + g * SUB) : ((3 + a) * pitch + (g + 1) * SUB), :] = (
                block(home_ref, (3 + a) * slots, g) * F32(VELOCITY_SCALE)
            )
        for a, value in enumerate(home_noise(block(home_fixed_ref, fixed_at, g), step)):
            at = (6 + a) * pitch + g * SUB
            home[at : at + SUB, :] = value
    home_low = [spread(jnp.min(v, axis=0, keepdims=True)) - REACH for v in low]
    home_high = [spread(jnp.max(v, axis=0, keepdims=True)) + REACH for v in high]

    reach = {}
    for r, (source, offset, dz) in enumerate(rows):
        data, fixed = near_refs[source], fixed_refs[source]
        base = r * 7 * pitch
        turned = (lambda v: pltpu.roll(v, turn, 1)) if turning else (lambda v: v)
        count = turned(spread(fixed[offset[1] + fixed_at + slots : offset[1] + fixed_at + slots + 1, :]))
        reach_low = [jnp.full((SUB, lanes), FAR, F32) for _ in range(2)]
        reach_high = [jnp.full((SUB, lanes), -FAR, F32) for _ in range(2)]
        for g in range(groups):
            there = iota_f + F32(g * SUB) < count
            for c in range(7):
                ref, at = (fixed, offset[1]) if c == 6 else (data, offset[0])
                v = turned(block(ref, at + c * slots, g))
                if c == 0:
                    v = jnp.where(there, v, FAR)
                if c == 1 and side:
                    v = v + F32(EDGE) * across
                if c == 2 and dz:
                    v = v + F32(EDGE * dz)
                if c == 3 and turning:
                    v = v + shear
                if 3 <= c < 6:
                    v = v * F32(VELOCITY_SCALE)
                if c in (1, 2) and not own:
                    a = c - 1
                    reach_low[a] = jnp.minimum(reach_low[a], jnp.where(there, v, FAR))
                    reach_high[a] = jnp.maximum(reach_high[a], jnp.where(there, v, -FAR))
                near[base + c * pitch + g * SUB : base + c * pitch + (g + 1) * SUB, :] = v
        if not own:
            for a in range(2):
                least = jnp.min(reach_low[a], axis=0, keepdims=True)
                most = jnp.max(reach_high[a], axis=0, keepdims=True)
                least, most = spread(least), spread(most)
                least = jnp.minimum(least, jnp.minimum(pltpu.roll(least, 1, 1), pltpu.roll(least, lanes - 1, 1)))
                most = jnp.maximum(most, jnp.maximum(pltpu.roll(most, 1, 1), pltpu.roll(most, lanes - 1, 1)))
                reach[(r, a)] = (least - REACH, most + REACH)

    below = lax.broadcasted_iota(jnp.int32, (slots, slots), 0) >= lax.broadcasted_iota(
        jnp.int32, (slots, slots), 1
    )
    triangle = jnp.where(below, 1.0, 0.0).astype(jnp.bfloat16)

    def ranked(slot, marks):
        ones = jnp.concatenate([jnp.where(m, 1.0, 0.0) for m in marks], axis=0)
        upto = jnp.dot(triangle, ones.astype(jnp.bfloat16), preferred_element_type=F32)
        for g in range(groups):
            rows_of = slice(g * SUB, (g + 1) * SUB)
            place = jnp.where(marks[g], upto[rows_of, :] - 1.0, -1.0)
            rank[(slot * slots + g * SUB) : (slot * slots + (g + 1) * SUB), :] = place
        sizes[slot] = jnp.max(upto[slots - 1 : slots, :]).astype(jnp.int32)

    for r, (source, offset, dz) in enumerate(rows):
        base = r * 7 * pitch
        for d, dx in enumerate((0, -1, 1)):
            if own and d < 2:
                continue
            marks = []
            for g in range(groups):
                pos = [
                    near[base + a * pitch + g * SUB : base + a * pitch + (g + 1) * SUB, :]
                    for a in range(3)
                ]
                if dx:
                    pos = [pltpu.roll(v, (-dx) % lanes, 1) for v in pos]
                    pos[0] = pos[0] + F32(EDGE * dx)
                mark = (pos[0] > home_low[0]) & (pos[0] < home_high[0])
                for a in (1, 2):
                    mark = mark & (pos[a] > home_low[a]) & (pos[a] < home_high[a])
                marks.append(mark)
            ranked(4 * r + d, marks)
        if not own:
            marks = []
            for g in range(groups):
                mark = home_there[g]
                for a in range(2):
                    p = home[(a + 1) * pitch + g * SUB : (a + 1) * pitch + (g + 1) * SUB, :]
                    mark = mark & (p > reach[(r, a)][0]) & (p < reach[(r, a)][1])
                marks.append(mark)
            ranked(4 * r + 3, marks)

    def choose(slot, k):
        target = iota_f + (k * (2 * SUB)).astype(F32)
        index = [jnp.full((SUB, lanes), -1, jnp.int32) for _ in range(2)]
        for s in range(slots):
            place = rank[pl.ds(slot * slots + s, SUB, stride=0), :]
            for i in range(2):
                index[i] = jnp.where(place == target + F32(i * SUB), s, index[i])
        return index

    def gathered(ref, base, index):
        within = index & (SUB - 1)
        result = take_rows(ref[pl.ds(base, SUB), :], within)
        for g in range(1, groups):
            result = jnp.where(
                index >= g * SUB, take_rows(ref[pl.ds(base + g * SUB, SUB), :], within), result
            )
        return result

    def aligned(value):
        return pl.multiple_of(value, SUB)

    def run_pairs(count, where_home, blocks, start=0, react=False):
        def one(j, carry):
            carry = list(carry)
            n = [liste[pl.ds(c * capacity + start + j, SUB, stride=0), :] for c in range(9)]
            tot = [None] * 3
            for b in range(blocks):
                h = [where_home[c * pitch + b * SUB : c * pitch + (b + 1) * SUB, :] for c in range(9)]
                rx, ry, rz = h[0] - n[0], h[1] - n[1], h[2] - n[2]
                squared = jnp.maximum(rx * rx + ry * ry + rz * rz, FLOOR_SQUARED)
                u = jnp.maximum(lax.rsqrt(squared) - 1.0, 0.0)
                rv = rx * (h[3] - n[3]) + ry * (h[4] - n[4]) + rz * (h[5] - n[5])
                t = ((h[6] * n[6] + h[7] * n[7]) + (h[8] + n[8])) * F32(INVERSE)
                y = (t - jnp.floor(t)) + F32(SHIFT)
                magnitude = u * (y - u * rv)
                f = [magnitude * rx, magnitude * ry, magnitude * rz]
                for a in range(3):
                    carry[3 * b + a] = carry[3 * b + a] + f[a]
                    tot[a] = f[a] if tot[a] is None else tot[a] + f[a]
            if virial:
                for i, (a, b) in enumerate(COMPONENT_PAIRS):
                    carry[3 * blocks + i] = carry[3 * blocks + i] - n[a] * tot[b]
            if react:
                for a in range(3):
                    answer[pl.ds(a * slots + j, 1), :] = jnp.sum(tot[a], axis=0, keepdims=True)
            return tuple(carry)

        def several(i, carry):
            for k in range(UNROLL):
                carry = one(UNROLL * i + k, carry)
            return carry

        zero = jnp.zeros((SUB, lanes), F32)
        begin = (zero,) * (3 * blocks + (6 if virial else 0))
        done = lax.fori_loop(0, (count + UNROLL - 1) // UNROLL, several, begin)
        for b in range(blocks):
            for a in range(3):
                part[a * slots + b * SUB : a * slots + (b + 1) * SUB, :] = done[3 * b + a]
        if virial:
            for i, (a, b) in enumerate(COMPONENT_PAIRS):
                value = done[3 * blocks + i]
                for g in range(blocks):
                    value = value + (
                        where_home[a * pitch + g * SUB : a * pitch + (g + 1) * SUB, :] * done[3 * g + b]
                    )
                if react:
                    value = value + pltpu.roll(value, 1, 1)
                tally[i * SUB : (i + 1) * SUB, :] = tally[i * SUB : (i + 1) * SUB, :] + value

    for c in range(3):
        for g in range(groups):
            at = c * slots + g * SUB
            total[at : at + SUB, :] = (
                jnp.zeros((SUB, lanes), F32) if first else force_in[at : at + SUB, :]
            )
    if virial:
        for i in range(6):
            tally[i * SUB : (i + 1) * SUB, :] = (
                jnp.zeros((SUB, lanes), F32) if first else virial_in[i * SUB : (i + 1) * SUB, :]
            )

    def gather_near(at, index, dx):
        v = gathered(near, at, index)
        return pltpu.roll(v, (-dx) % lanes, 1) if dx else v

    def fill_near(base, slot, dx, filled):
        def fill(k, _):
            for i, index in enumerate(choose(slot, k)):
                valid = index >= 0
                if dx:
                    index = pltpu.roll(index, dx % lanes, 1)
                values = [gather_near(base + c * pitch, index, dx) for c in range(7)]
                values[0] = jnp.where(valid, values[0] + F32(EDGE * dx), FAR)
                values = values[:6] + list(near_noise(values[6]))
                for c in range(9):
                    at = c * capacity + filled + k * (2 * SUB) + i * SUB
                    liste[pl.ds(at, SUB), :] = values[c]
            return 0

        size = sizes[slot]
        lax.fori_loop(0, (size + 2 * SUB - 1) // (2 * SUB), fill, 0)
        return filled + size

    def close(filled):
        liste[pl.ds(filled, SUB), :] = jnp.full((SUB, lanes), FAR, F32)
        for c in range(1, 9):
            liste[pl.ds(c * capacity + filled, SUB), :] = jnp.zeros((SUB, lanes), F32)

    def collect():
        for c in range(3):
            for g in range(groups):
                at = c * slots + g * SUB
                total[at : at + SUB, :] = total[at : at + SUB, :] + part[at : at + SUB, :]

    def own_row():
        for g in range(groups):
            values = [near[c * pitch + g * SUB : c * pitch + (g + 1) * SUB, :] for c in range(7)]
            values = values[:6] + list(near_noise(values[6]))
            for c in range(9):
                at = c * capacity + g * SUB
                liste[at : at + SUB, :] = values[c]
        close(fill_near(0, 2, 1, slots))
        run_pairs(slots, home, groups)
        collect()
        size = sizes[2]
        run_pairs(size, home, groups, start=slots, react=True)
        collect()

        def back(k, _):
            forces = [
                pltpu.roll(answer[pl.ds(aligned(c * slots + k * SUB), SUB), :], 1, 1) for c in range(3)
            ]
            for g in range(groups):
                place = rank[(2 * slots + g * SUB) : (2 * slots + (g + 1) * SUB), :]
                place = pltpu.roll(place, 1, 1).astype(jnp.int32)
                mine = (place >= k * SUB) & (place < (k + 1) * SUB)
                within = place & (SUB - 1)
                for c in range(3):
                    at = c * slots + g * SUB
                    v = take_rows(forces[c], within)
                    total[at : at + SUB, :] = total[at : at + SUB, :] - jnp.where(mine, v, 0.0)
            return 0

        lax.fori_loop(0, (size + SUB - 1) // SUB, back, 0)

    def direction(r, _):
        base = r * (7 * pitch)
        filled = jnp.int32(0)
        for d, dx in enumerate((0, -1, 1)):
            filled = fill_near(base, 4 * r + d, dx, filled)
        close(filled)
        slot = 4 * r + 3
        needed = (sizes[slot] + SUB - 1) // SUB

        def fill_home(k, _):
            for i, index in enumerate(choose(slot, k)):
                for c in range(9):
                    v = gathered(home, c * pitch, index)
                    if c == 0:
                        v = jnp.where(index >= 0, v, -FAR)
                    pick[pl.ds(aligned(c * pitch + k * (2 * SUB) + i * SUB), SUB), :] = v
            return 0

        lax.fori_loop(0, (needed + 1) // 2, fill_home, 0)
        for blocks in range(1, groups + 1):
            pl.when(needed == blocks)(functools.partial(run_pairs, filled, pick, blocks))

        def back(k, _):
            for g in range(groups):
                place = rank[pl.ds(aligned(slot * slots + g * SUB), SUB), :].astype(jnp.int32)
                mine = (place >= k * SUB) & (place < (k + 1) * SUB)
                within = place & (SUB - 1)
                for c in range(3):
                    at = c * slots + g * SUB
                    v = take_rows(part[pl.ds(aligned(c * slots + k * SUB), SUB), :], within)
                    total[at : at + SUB, :] = total[at : at + SUB, :] + jnp.where(mine, v, 0.0)
            return 0

        lax.fori_loop(0, needed, back, 0)
        return 0

    if own:
        own_row()
    else:
        lax.fori_loop(0, len(rows), direction, 0)

    half = F32(0.5 * TIME_STEP)
    for c in range(3):
        for g in range(groups):
            at = c * slots + g * SUB
            f = total[at : at + SUB, :]
            if not last:
                force_out[at : at + SUB, :] = f
                continue
            f = f * F32(NOISE_UNIT)
            v = block(home_ref, (3 + c) * slots, g) + half * f
            if virial:
                force_out[at : at + SUB, :] = f
                velocity_out[at : at + SUB, :] = jnp.where(home_there[g], v, 0.0)
            else:
                v = v + half * f
                force_out[at : at + SUB, :] = block(home_ref, c * slots, g) + F32(TIME_STEP) * v
                force_out[3 * slots + at : 3 * slots + at + SUB, :] = v
    if virial:
        for i in range(6):
            v = tally[i * SUB : (i + 1) * SUB, :]
            if last:
                virial_out[i] = jnp.sum(v, axis=0, keepdims=True) * F32(
                    NOISE_UNIT * 0.5 / CELL_VOLUME
                )
            else:
                virial_out[i * SUB : (i + 1) * SUB, :] = v


def pairs(offsets, home, home_fixed, nears, fixed, carried, rows, step, last, virial, slots, cost, side=0):
    lanes = home.shape[-1]
    own = len(rows) == 1
    first = carried is None
    operands = [offsets, home, home_fixed, *nears]
    if fixed is not None:
        operands += list(fixed)
    if not first:
        operands += list(carried)
    shape = lambda n: jax.ShapeDtypeStruct((n, lanes), F32)
    if last and virial:
        outs = (shape(3 * slots), shape(3 * slots), jax.ShapeDtypeStruct((6, 1, lanes), F32))
    elif virial:
        outs = (shape(3 * slots), shape(6 * SUB))
    elif last:
        outs = (shape(6 * slots),)
    else:
        outs = (shape(3 * slots),)
    vmem = pl.BlockSpec(memory_space=pltpu.VMEM)
    smem = pl.BlockSpec(memory_space=pltpu.SMEM)
    pitch = slots + SUB
    capacity = 3 * slots + 2 * SUB + 1
    count = len(rows)
    return pl.pallas_call(
        functools.partial(
            pair_kernel,
            slots=slots,
            lanes=lanes,
            sources=len(nears),
            rows=rows,
            own=own,
            step=step,
            first=first,
            last=last,
            virial=virial,
            has_fixed=fixed is not None,
            side=side,
        ),
        out_shape=outs,
        in_specs=[smem] + [vmem] * (len(operands) - 1),
        out_specs=tuple(vmem for _ in outs),
        scratch_shapes=[
            pltpu.VMEM((9 * pitch, lanes), F32),
            pltpu.VMEM((count * 7 * pitch, lanes), F32),
            pltpu.VMEM((4 * slots, lanes), F32),
            pltpu.VMEM((count * 4 * slots, lanes), F32),
            pltpu.VMEM((9 * pitch, lanes), F32),
            pltpu.VMEM((9 * capacity, lanes), F32),
            pltpu.VMEM((3 * slots, lanes), F32),
            pltpu.VMEM((3 * slots, lanes), F32),
            pltpu.VMEM((6 * SUB, lanes), F32),
            pltpu.SMEM((4 * count,), jnp.int32),
        ],
        compiler_params=pltpu.CompilerParams(vmem_limit_bytes=VMEM_LIMIT),
        cost_estimate=pl.CostEstimate(flops=cost, bytes_accessed=1, transcendentals=0),
        name=f"pairs_{side}_{step}",
    )(*operands)


def kick_kernel(*refs, slots, lanes):
    sources, out, held, done = refs[:5], refs[5], refs[6:11], refs[11]
    copies = [
        pltpu.make_async_copy(source, target, done.at[i])
        for i, (source, target) in enumerate(zip(sources, held))
    ]
    for copy in copies:
        copy.start()
    for copy in copies:
        copy.wait()
    position, velocity, force, seed, count = held
    for c in range(3):
        for g in range(slots // SUB):
            at = c * slots + g * SUB
            rows = slice(at, at + SUB)
            v = velocity[rows, :] + F32(0.5 * TIME_STEP) * force[rows, :]
            out[rows, :] = position[rows, :] + F32(TIME_STEP) * v
            out[3 * slots + at : 3 * slots + at + SUB, :] = v
    out[6 * slots : 7 * slots, :] = seed[...].astype(F32)
    out[7 * slots : 7 * slots + SUB, :] = jnp.broadcast_to(count[...], (SUB, lanes)).astype(F32)


def ring(count, by):
    return [(i, (i + by) % count) for i in range(count)]


def swap(count, first):
    assert count % 2 == 0
    pairs_of = [((first + i) % count, (first + i + 1) % count) for i in range(0, count, 2)]
    return pairs_of + [(b, a) for a, b in pairs_of]


def shards(positions, velocities, forces_prev, seeds, counts, offsets):
    slots, depth, width, lanes = seeds.shape
    assert depth == 1 and width == 1
    gz, xy = lax.axis_size("gz"), lax.axis_size("xy")
    flat = lambda a: a.reshape(-1, lanes)
    tall = 7 * slots + SUB
    inputs = [flat(a) for a in (positions, velocities, forces_prev, seeds, counts)]
    state = pl.pallas_call(
        functools.partial(kick_kernel, slots=slots, lanes=lanes),
        out_shape=jax.ShapeDtypeStruct((tall, lanes), F32),
        in_specs=[pl.BlockSpec(memory_space=pltpu.HBM)] * 5,
        out_specs=pl.BlockSpec(memory_space=pltpu.VMEM),
        scratch_shapes=[pltpu.VMEM(a.shape, a.dtype) for a in inputs]
        + [pltpu.SemaphoreType.DMA((5,))],
        compiler_params=pltpu.CompilerParams(vmem_limit_bytes=KICK_LIMIT),
        name="kick",
    )(*inputs)
    home_fixed = state
    kept = None
    for step in range(2):
        final = step == 1
        high = state.shape[0]
        planes = [lax.ppermute(state, "gz", ring(gz, -1))]
        if gz > 2:
            planes.append(lax.ppermute(state, "gz", ring(gz, 1)))
        up, down = 0, len(planes) - 1
        call = functools.partial(
            pairs, offsets, state, home_fixed, step=step, virial=final, slots=slots
        )
        here = (0, 0)
        carried = call(
            [state],
            [home_fixed] if final else None,
            None,
            rows=((0, here, 0),),
            last=False,
            cost=100_000_000,
        )
        planes, carried = lax.optimization_barrier((planes, carried))
        stacked = jnp.concatenate([state, *planes], axis=0)
        far = lax.ppermute(stacked, "xy", swap(xy, 1))
        near = lax.ppermute(stacked, "xy", swap(xy, 0))
        arrived = (planes, [near], [far])
        if not final:
            kept = arrived
        carried = call(
            planes,
            kept[0] if final else None,
            carried,
            rows=((down, here, -1), (up, here, 1)),
            last=False,
            cost=100_000_000,
        )
        beside = tuple(
            (0, (place * high, place * tall), dz) for dz, place in ((0, 0), (-1, 1 + down), (1, 1 + up))
        )
        for side in (NEAR_SIDE, FAR_SIDE):
            carried = call(
                arrived[side],
                kept[side] if final else None,
                carried,
                rows=beside,
                last=side == FAR_SIDE,
                cost=100_000_000,
                side=side,
            )
        outs = carried
        if not final:
            state = outs[0]
    force, velocity, stress = outs
    return (
        force.reshape(positions.shape),
        velocity.reshape(positions.shape),
        stress.reshape(6, depth, width, lanes),
    )


def solution(mesh):
    beads = P(None, None, "gz", "xy", None)
    return jax.shard_map(
        shards,
        mesh=mesh,
        in_specs=(beads, beads, beads, P(None, "gz", "xy", None), P("gz", "xy", None), P()),
        out_specs=(beads, beads, P(None, "gz", "xy", None)),
        check_vma=False,
    )
```

```python
import functools
import math

import jax
import jax.numpy as jnp
from jax import lax
from jax.experimental import pallas as pl
from jax.experimental.pallas import tpu as pltpu
from jax.sharding import PartitionSpec as P

CONSERVATIVE = 25.0
FRICTION = 4.5
NOISE_LEVEL = 3.0
TIME_STEP = 0.04
SHEAR_SPEED = 1.0
CELL_VOLUME = 8.0
FLOOR_SQUARED = 0.0025
EDGE = 2.0
MODULUS = 65521
COMPONENT_PAIRS = [(0, 0), (1, 1), (2, 2), (0, 1), (0, 2), (1, 2)]

NOISE_UNIT = NOISE_LEVEL * math.sqrt(12.0) / math.sqrt(TIME_STEP)
SHIFT = CONSERVATIVE / NOISE_UNIT - 0.5 - 0.5 / MODULUS
VELOCITY_SCALE = FRICTION / NOISE_UNIT
INVERSE = 1.0 / MODULUS
FAR = 1.0e15
REACH = 1.001
SEED_MIDDLE = 8192
NEAR_SIDE, FAR_SIDE = 1, 2
F32 = jnp.float32
SUB = 8
UNROLL = 4
VMEM_LIMIT = 6 * 2**20
KICK_LIMIT = 67043328 - 160 * 1024


def take_rows(values, index):
    dims = lax.GatherDimensionNumbers(
        offset_dims=(),
        collapsed_slice_dims=(0,),
        start_index_map=(0,),
        operand_batching_dims=(1,),
        start_indices_batching_dims=(1,),
    )
    return lax.gather(
        values,
        index[..., None],
        dims,
        slice_sizes=(1, 1),
        mode=lax.GatherScatterMode.PROMISE_IN_BOUNDS,
    )


def centred(value):
    turns = jnp.round(value.astype(F32) * F32(INVERSE)).astype(jnp.int32)
    return (value - turns * MODULUS).astype(F32)


def home_noise(seed, step):
    a = seed.astype(jnp.int32) + (7919 * step + 1 + SEED_MIDDLE)
    return (
        centred(256 * a),
        centred(2 * a),
        centred(a * (a + 1)) + 0.5,
    )


def near_noise(seed):
    b = seed - SEED_MIDDLE
    high = jnp.floor((b + 64.0) * (1.0 / 128.0))
    low = b - 128.0 * high
    whole = b.astype(jnp.int32)
    return high, low, centred(whole * (whole + 1))


def pair_kernel(
    *refs, slots, lanes, sources, rows, own, step, first, last, virial, has_fixed, side
):
    refs = list(refs)
    take = lambda n: [refs.pop(0) for _ in range(n)]
    turning = side == FAR_SIDE
    home_ref, home_fixed_ref = take(2)
    home = None if own else take(1)[0]
    near_refs = take(sources)
    fixed_refs = take(sources) if has_fixed else near_refs
    force_in = None if first else take(1)[0]
    virial_in = take(1)[0] if (virial and not first) else None
    if last and virial:
        force_out, velocity_out, virial_out = take(3)
    elif virial:
        force_out, virial_out = take(2)
    else:
        (force_out,) = take(1)
    if own:
        (home,) = take(1)
    near, answer, rank, pick, liste, part, total, tally, sizes = take(9)
    groups = slots // SUB
    pitch = slots + SUB
    capacity = liste.shape[0] // 9
    iota = lax.broadcasted_iota(jnp.int32, (SUB, lanes), 0)
    iota_f = iota.astype(F32)
    fixed_at = 6 * slots
    if side:
        index, count = lax.axis_index("xy"), lax.axis_size("xy")
        upper = (lax.rem(index, 2) == 0) == (side == NEAR_SIDE)
        across = jnp.where(upper, F32(1.0), F32(-1.0))
    if turning:
        wraps = jnp.where(upper, index == count - 1, index == 0)
        strain_at = fixed_at + slots + 1 + step
        amount = jnp.max(home_fixed_ref[strain_at : strain_at + 1, :]).astype(jnp.int32)
        turn = jnp.where(upper, amount, lax.rem(lanes - amount, lanes))
        turn = jnp.where(wraps, turn, 0)
        shear = jnp.where(wraps, across * F32(SHEAR_SPEED), F32(0.0))

    def block(ref, base, group):
        return ref[base + group * SUB : base + (group + 1) * SUB, :]

    def spread(row):
        return jnp.broadcast_to(row, (SUB, lanes))

    box_at = 9 * pitch
    if own:
        home_count = spread(home_fixed_ref[fixed_at + slots : fixed_at + slots + 1, :])
        low = [jnp.full((SUB, lanes), FAR, F32) for _ in range(3)]
        high = [jnp.full((SUB, lanes), -FAR, F32) for _ in range(3)]
        for g in range(groups):
            there = iota_f + F32(g * SUB) < home_count
            for a in range(3):
                p = block(home_ref, a * slots, g)
                low[a] = jnp.minimum(low[a], jnp.where(there, p, FAR))
                high[a] = jnp.maximum(high[a], jnp.where(there, p, -FAR))
                at = a * pitch + g * SUB
                home[at : at + SUB, :] = jnp.where(there, p, -FAR) if a == 0 else p
                at = (3 + a) * pitch + g * SUB
                home[at : at + SUB, :] = block(home_ref, (3 + a) * slots, g) * F32(VELOCITY_SCALE)
            for a, value in enumerate(home_noise(block(home_fixed_ref, fixed_at, g), step)):
                at = (6 + a) * pitch + g * SUB
                home[at : at + SUB, :] = value
        home_low = [spread(jnp.min(v, axis=0, keepdims=True)) - REACH for v in low]
        home_high = [spread(jnp.max(v, axis=0, keepdims=True)) + REACH for v in high]
        for i, v in enumerate(home_low + home_high):
            home[box_at + i * SUB : box_at + (i + 1) * SUB, :] = v
    else:
        walls = [home[box_at + i * SUB : box_at + (i + 1) * SUB, :] for i in range(6)]
        home_low, home_high = walls[:3], walls[3:]
        home_there = [home[g * SUB : (g + 1) * SUB, :] > F32(-0.5 * FAR) for g in range(groups)]

    reach = {}
    for r, (source, offset, dz) in enumerate(rows):
        data, fixed = near_refs[source], fixed_refs[source]
        base = r * 7 * pitch
        turned = (lambda v: pltpu.roll(v, turn, 1)) if turning else (lambda v: v)
        count = turned(spread(fixed[offset[1] + fixed_at + slots : offset[1] + fixed_at + slots + 1, :]))
        reach_low = [jnp.full((SUB, lanes), FAR, F32) for _ in range(2)]
        reach_high = [jnp.full((SUB, lanes), -FAR, F32) for _ in range(2)]
        for g in range(groups):
            there = iota_f + F32(g * SUB) < count
            for c in range(7):
                ref, at = (fixed, offset[1]) if c == 6 else (data, offset[0])
                v = turned(block(ref, at + c * slots, g))
                if c == 0:
                    v = jnp.where(there, v, FAR)
                if c == 1 and side:
                    v = v + F32(EDGE) * across
                if c == 2 and dz:
                    v = v + F32(EDGE * dz)
                if c == 3 and turning:
                    v = v + shear
                if 3 <= c < 6:
                    v = v * F32(VELOCITY_SCALE)
                if c in (1, 2) and not own:
                    a = c - 1
                    reach_low[a] = jnp.minimum(reach_low[a], jnp.where(there, v, FAR))
                    reach_high[a] = jnp.maximum(reach_high[a], jnp.where(there, v, -FAR))
                near[base + c * pitch + g * SUB : base + c * pitch + (g + 1) * SUB, :] = v
        if not own:
            for a in range(2):
                least = jnp.min(reach_low[a], axis=0, keepdims=True)
                most = jnp.max(reach_high[a], axis=0, keepdims=True)
                least, most = spread(least), spread(most)
                least = jnp.minimum(least, jnp.minimum(pltpu.roll(least, 1, 1), pltpu.roll(least, lanes - 1, 1)))
                most = jnp.maximum(most, jnp.maximum(pltpu.roll(most, 1, 1), pltpu.roll(most, lanes - 1, 1)))
                reach[(r, a)] = (least - REACH, most + REACH)

    below = lax.broadcasted_iota(jnp.int32, (slots, slots), 0) >= lax.broadcasted_iota(
        jnp.int32, (slots, slots), 1
    )
    triangle = jnp.where(below, 1.0, 0.0).astype(jnp.bfloat16)

    def ranked(slot, marks):
        ones = jnp.concatenate([jnp.where(m, 1.0, 0.0) for m in marks], axis=0)
        upto = jnp.dot(triangle, ones.astype(jnp.bfloat16), preferred_element_type=F32)
        for g in range(groups):
            rows_of = slice(g * SUB, (g + 1) * SUB)
            place = jnp.where(marks[g], upto[rows_of, :] - 1.0, -1.0)
            rank[(slot * slots + g * SUB) : (slot * slots + (g + 1) * SUB), :] = place
        sizes[slot] = jnp.max(upto[slots - 1 : slots, :]).astype(jnp.int32)

    for r, (source, offset, dz) in enumerate(rows):
        base = r * 7 * pitch
        for d, dx in enumerate((0, -1, 1)):
            if own and d < 2:
                continue
            marks = []
            for g in range(groups):
                pos = [
                    near[base + a * pitch + g * SUB : base + a * pitch + (g + 1) * SUB, :]
                    for a in range(3)
                ]
                if dx:
                    pos = [pltpu.roll(v, (-dx) % lanes, 1) for v in pos]
                    pos[0] = pos[0] + F32(EDGE * dx)
                mark = (pos[0] > home_low[0]) & (pos[0] < home_high[0])
                for a in (1, 2):
                    mark = mark & (pos[a] > home_low[a]) & (pos[a] < home_high[a])
                marks.append(mark)
            ranked(4 * r + d, marks)
        if not own:
            marks = []
            for g in range(groups):
                mark = home_there[g]
                for a in range(2):
                    p = home[(a + 1) * pitch + g * SUB : (a + 1) * pitch + (g + 1) * SUB, :]
                    mark = mark & (p > reach[(r, a)][0]) & (p < reach[(r, a)][1])
                marks.append(mark)
            ranked(4 * r + 3, marks)

    def choose(slot, k):
        target = iota_f + (k * (2 * SUB)).astype(F32)
        index = [jnp.full((SUB, lanes), -1, jnp.int32) for _ in range(2)]
        for s in range(slots):
            place = rank[pl.ds(slot * slots + s, SUB, stride=0), :]
            for i in range(2):
                index[i] = jnp.where(place == target + F32(i * SUB), s, index[i])
        return index

    def gathered(ref, base, index):
        within = index & (SUB - 1)
        result = take_rows(ref[pl.ds(base, SUB), :], within)
        for g in range(1, groups):
            result = jnp.where(
                index >= g * SUB, take_rows(ref[pl.ds(base + g * SUB, SUB), :], within), result
            )
        return result

    def aligned(value):
        return pl.multiple_of(value, SUB)

    def run_pairs(count, where_home, blocks, start=0, react=False):
        def one(j, carry):
            carry = list(carry)
            n = [liste[pl.ds(c * capacity + start + j, SUB, stride=0), :] for c in range(9)]
            tot = [None] * 3
            for b in range(blocks):
                h = [where_home[c * pitch + b * SUB : c * pitch + (b + 1) * SUB, :] for c in range(9)]
                rx, ry, rz = h[0] - n[0], h[1] - n[1], h[2] - n[2]
                squared = jnp.maximum(rx * rx + ry * ry + rz * rz, FLOOR_SQUARED)
                u = jnp.maximum(lax.rsqrt(squared) - 1.0, 0.0)
                rv = rx * (h[3] - n[3]) + ry * (h[4] - n[4]) + rz * (h[5] - n[5])
                t = ((h[6] * n[6] + h[7] * n[7]) + (h[8] + n[8])) * F32(INVERSE)
                y = (t - jnp.floor(t)) + F32(SHIFT)
                magnitude = u * (y - u * rv)
                f = [magnitude * rx, magnitude * ry, magnitude * rz]
                for a in range(3):
                    carry[3 * b + a] = carry[3 * b + a] + f[a]
                    tot[a] = f[a] if tot[a] is None else tot[a] + f[a]
            if virial:
                for i, (a, b) in enumerate(COMPONENT_PAIRS):
                    carry[3 * blocks + i] = carry[3 * blocks + i] - n[a] * tot[b]
            if react:
                for a in range(3):
                    answer[pl.ds(a * slots + j, 1), :] = jnp.sum(tot[a], axis=0, keepdims=True)
            return tuple(carry)

        def several(i, carry):
            for k in range(UNROLL):
                carry = one(UNROLL * i + k, carry)
            return carry

        zero = jnp.zeros((SUB, lanes), F32)
        begin = (zero,) * (3 * blocks + (6 if virial else 0))
        done = lax.fori_loop(0, (count + UNROLL - 1) // UNROLL, several, begin)
        for b in range(blocks):
            for a in range(3):
                part[a * slots + b * SUB : a * slots + (b + 1) * SUB, :] = done[3 * b + a]
        if virial:
            for i, (a, b) in enumerate(COMPONENT_PAIRS):
                value = done[3 * blocks + i]
                for g in range(blocks):
                    value = value + (
                        where_home[a * pitch + g * SUB : a * pitch + (g + 1) * SUB, :] * done[3 * g + b]
                    )
                if react:
                    value = value + pltpu.roll(value, 1, 1)
                tally[i * SUB : (i + 1) * SUB, :] = tally[i * SUB : (i + 1) * SUB, :] + value

    for c in range(3):
        for g in range(groups):
            at = c * slots + g * SUB
            total[at : at + SUB, :] = (
                jnp.zeros((SUB, lanes), F32) if first else force_in[at : at + SUB, :]
            )
    if virial:
        for i in range(6):
            tally[i * SUB : (i + 1) * SUB, :] = (
                jnp.zeros((SUB, lanes), F32) if first else virial_in[i * SUB : (i + 1) * SUB, :]
            )

    def gather_near(at, index, dx):
        v = gathered(near, at, index)
        return pltpu.roll(v, (-dx) % lanes, 1) if dx else v

    def fill_near(base, slot, dx, filled):
        def fill(k, _):
            for i, index in enumerate(choose(slot, k)):
                valid = index >= 0
                if dx:
                    index = pltpu.roll(index, dx % lanes, 1)
                values = [gather_near(base + c * pitch, index, dx) for c in range(7)]
                values[0] = jnp.where(valid, values[0] + F32(EDGE * dx), FAR)
                values = values[:6] + list(near_noise(values[6]))
                for c in range(9):
                    at = c * capacity + filled + k * (2 * SUB) + i * SUB
                    liste[pl.ds(at, SUB), :] = values[c]
            return 0

        size = sizes[slot]
        lax.fori_loop(0, (size + 2 * SUB - 1) // (2 * SUB), fill, 0)
        return filled + size

    def close(filled):
        liste[pl.ds(filled, SUB), :] = jnp.full((SUB, lanes), FAR, F32)
        for c in range(1, 9):
            liste[pl.ds(c * capacity + filled, SUB), :] = jnp.zeros((SUB, lanes), F32)

    def collect():
        for c in range(3):
            for g in range(groups):
                at = c * slots + g * SUB
                total[at : at + SUB, :] = total[at : at + SUB, :] + part[at : at + SUB, :]

    def own_row():
        for g in range(groups):
            values = [near[c * pitch + g * SUB : c * pitch + (g + 1) * SUB, :] for c in range(7)]
            values = values[:6] + list(near_noise(values[6]))
            for c in range(9):
                at = c * capacity + g * SUB
                liste[at : at + SUB, :] = values[c]
        close(fill_near(0, 2, 1, slots))
        run_pairs(slots, home, groups)
        collect()
        size = sizes[2]
        run_pairs(size, home, groups, start=slots, react=True)
        collect()

        def back(k, _):
            forces = [
                pltpu.roll(answer[pl.ds(aligned(c * slots + k * SUB), SUB), :], 1, 1) for c in range(3)
            ]
            for g in range(groups):
                place = rank[(2 * slots + g * SUB) : (2 * slots + (g + 1) * SUB), :]
                place = pltpu.roll(place, 1, 1).astype(jnp.int32)
                mine = (place >= k * SUB) & (place < (k + 1) * SUB)
                within = place & (SUB - 1)
                for c in range(3):
                    at = c * slots + g * SUB
                    v = take_rows(forces[c], within)
                    total[at : at + SUB, :] = total[at : at + SUB, :] - jnp.where(mine, v, 0.0)
            return 0

        lax.fori_loop(0, (size + SUB - 1) // SUB, back, 0)

    def direction(r, _):
        base = r * (7 * pitch)
        filled = jnp.int32(0)
        for d, dx in enumerate((0, -1, 1)):
            filled = fill_near(base, 4 * r + d, dx, filled)
        close(filled)
        slot = 4 * r + 3
        needed = (sizes[slot] + SUB - 1) // SUB

        def fill_home(k, _):
            for i, index in enumerate(choose(slot, k)):
                for c in range(9):
                    v = gathered(home, c * pitch, index)
                    if c == 0:
                        v = jnp.where(index >= 0, v, -FAR)
                    pick[pl.ds(aligned(c * pitch + k * (2 * SUB) + i * SUB), SUB), :] = v
            return 0

        lax.fori_loop(0, (needed + 1) // 2, fill_home, 0)
        for blocks in range(1, groups + 1):
            pl.when(needed == blocks)(functools.partial(run_pairs, filled, pick, blocks))

        def back(k, _):
            for g in range(groups):
                place = rank[pl.ds(aligned(slot * slots + g * SUB), SUB), :].astype(jnp.int32)
                mine = (place >= k * SUB) & (place < (k + 1) * SUB)
                within = place & (SUB - 1)
                for c in range(3):
                    at = c * slots + g * SUB
                    v = take_rows(part[pl.ds(aligned(c * slots + k * SUB), SUB), :], within)
                    total[at : at + SUB, :] = total[at : at + SUB, :] + jnp.where(mine, v, 0.0)
            return 0

        lax.fori_loop(0, needed, back, 0)
        return 0

    if own:
        own_row()
    else:
        lax.fori_loop(0, len(rows), direction, 0)

    half = F32(0.5 * TIME_STEP)
    for c in range(3):
        for g in range(groups):
            at = c * slots + g * SUB
            f = total[at : at + SUB, :]
            if not last:
                force_out[at : at + SUB, :] = f
                continue
            f = f * F32(NOISE_UNIT)
            v = block(home_ref, (3 + c) * slots, g) + half * f
            if virial:
                force_out[at : at + SUB, :] = f
                velocity_out[at : at + SUB, :] = jnp.where(home_there[g], v, 0.0)
            else:
                v = v + half * f
                force_out[at : at + SUB, :] = block(home_ref, c * slots, g) + F32(TIME_STEP) * v
                force_out[3 * slots + at : 3 * slots + at + SUB, :] = v
    if virial:
        for i in range(6):
            v = tally[i * SUB : (i + 1) * SUB, :]
            if last:
                virial_out[i] = jnp.sum(v, axis=0, keepdims=True) * F32(
                    NOISE_UNIT * 0.5 / CELL_VOLUME
                )
            else:
                virial_out[i * SUB : (i + 1) * SUB, :] = v


def pairs(home, home_fixed, beads, nears, fixed, carried, rows, step, last, virial, slots, cost, side=0):
    lanes = home.shape[-1]
    own = len(rows) == 1
    first = carried is None
    operands = [home, home_fixed, *beads, *nears]
    if fixed is not None:
        operands += list(fixed)
    if not first:
        operands += list(carried)
    shape = lambda n: jax.ShapeDtypeStruct((n, lanes), F32)
    if last and virial:
        outs = (shape(3 * slots), shape(3 * slots), jax.ShapeDtypeStruct((6, 1, lanes), F32))
    elif virial:
        outs = (shape(3 * slots), shape(6 * SUB))
    elif last:
        outs = (shape(6 * slots),)
    else:
        outs = (shape(3 * slots),)
    pitch = slots + SUB
    if own:
        outs += (shape(9 * pitch + 6 * SUB),)
    vmem = pl.BlockSpec(memory_space=pltpu.VMEM)
    capacity = 3 * slots + 2 * SUB + 1
    count = len(rows)
    return pl.pallas_call(
        functools.partial(
            pair_kernel,
            slots=slots,
            lanes=lanes,
            sources=len(nears),
            rows=rows,
            own=own,
            step=step,
            first=first,
            last=last,
            virial=virial,
            has_fixed=fixed is not None,
            side=side,
        ),
        out_shape=outs,
        in_specs=[vmem] * len(operands),
        out_specs=tuple(vmem for _ in outs),
        scratch_shapes=[
            pltpu.VMEM((count * 7 * pitch, lanes), F32),
            pltpu.VMEM((4 * slots, lanes), F32),
            pltpu.VMEM((count * 4 * slots, lanes), F32),
            pltpu.VMEM((9 * pitch, lanes), F32),
            pltpu.VMEM((9 * capacity, lanes), F32),
            pltpu.VMEM((3 * slots, lanes), F32),
            pltpu.VMEM((3 * slots, lanes), F32),
            pltpu.VMEM((6 * SUB, lanes), F32),
            pltpu.SMEM((4 * count,), jnp.int32),
        ],
        compiler_params=pltpu.CompilerParams(vmem_limit_bytes=VMEM_LIMIT),
        cost_estimate=pl.CostEstimate(flops=cost, bytes_accessed=1, transcendentals=0),
        name=f"pairs_{side}_{step}",
    )(*operands)


def kick_kernel(*refs, slots, lanes):
    sources, out, held, done = refs[:6], refs[6], refs[7:13], refs[13]
    copies = [
        pltpu.make_async_copy(source, target, done.at[i])
        for i, (source, target) in enumerate(zip(sources, held))
    ]
    for copy in copies:
        copy.start()
    for copy in copies:
        copy.wait()
    position, velocity, force, seed, count, strain = held
    for c in range(3):
        for g in range(slots // SUB):
            at = c * slots + g * SUB
            rows = slice(at, at + SUB)
            v = velocity[rows, :] + F32(0.5 * TIME_STEP) * force[rows, :]
            out[rows, :] = position[rows, :] + F32(TIME_STEP) * v
            out[3 * slots + at : 3 * slots + at + SUB, :] = v
    out[6 * slots : 7 * slots, :] = seed[...].astype(F32)
    aside = jnp.broadcast_to(count[...], (SUB, lanes)).astype(F32)
    row = lax.broadcasted_iota(jnp.int32, (SUB, lanes), 0)
    for step in range(strain.shape[1]):
        aside = jnp.where(row == 1 + step, strain[:, step : step + 1].astype(F32), aside)
    out[7 * slots : 7 * slots + SUB, :] = aside


def ring(count, by):
    return [(i, (i + by) % count) for i in range(count)]


def swap(count, first):
    assert count % 2 == 0
    pairs_of = [((first + i) % count, (first + i + 1) % count) for i in range(0, count, 2)]
    return pairs_of + [(b, a) for a, b in pairs_of]


def shards(positions, velocities, forces_prev, seeds, counts, offsets):
    slots, depth, width, lanes = seeds.shape
    assert depth == 1 and width == 1
    gz, xy = lax.axis_size("gz"), lax.axis_size("xy")
    flat = lambda a: a.reshape(-1, lanes)
    tall = 7 * slots + SUB
    inputs = [flat(a) for a in (positions, velocities, forces_prev, seeds, counts)]
    inputs.append(offsets.reshape(1, -1))
    state = pl.pallas_call(
        functools.partial(kick_kernel, slots=slots, lanes=lanes),
        out_shape=jax.ShapeDtypeStruct((tall, lanes), F32),
        in_specs=[pl.BlockSpec(memory_space=pltpu.HBM)] * len(inputs),
        out_specs=pl.BlockSpec(memory_space=pltpu.VMEM),
        scratch_shapes=[pltpu.VMEM(a.shape, a.dtype) for a in inputs]
        + [pltpu.SemaphoreType.DMA((len(inputs),))],
        compiler_params=pltpu.CompilerParams(vmem_limit_bytes=KICK_LIMIT),
        name="kick",
    )(*inputs)
    home_fixed = state
    kept = None
    for step in range(2):
        final = step == 1
        high = state.shape[0]
        planes = [lax.ppermute(state, "gz", ring(gz, -1))]
        if gz > 2:
            planes.append(lax.ppermute(state, "gz", ring(gz, 1)))
        up, down = 0, len(planes) - 1
        call = functools.partial(
            pairs, state, home_fixed, step=step, virial=final, slots=slots
        )
        here = (0, 0)
        *carried, beads = call(
            [],
            [state],
            [home_fixed] if final else None,
            None,
            rows=((0, here, 0),),
            last=False,
            cost=100_000_000,
        )
        planes, carried, beads = lax.optimization_barrier((planes, carried, beads))
        stacked = jnp.concatenate([state, *planes], axis=0)
        far = lax.ppermute(stacked, "xy", swap(xy, 1))
        near = lax.ppermute(stacked, "xy", swap(xy, 0))
        arrived = (planes, [near], [far])
        if not final:
            kept = arrived
        carried = call(
            [beads],
            planes,
            kept[0] if final else None,
            carried,
            rows=((down, here, -1), (up, here, 1)),
            last=False,
            cost=100_000_000,
        )
        beside = tuple(
            (0, (place * high, place * tall), dz) for dz, place in ((0, 0), (-1, 1 + down), (1, 1 + up))
        )
        for side in (NEAR_SIDE, FAR_SIDE):
            carried = call(
                [beads],
                arrived[side],
                kept[side] if final else None,
                carried,
                rows=beside,
                last=side == FAR_SIDE,
                cost=100_000_000,
                side=side,
            )
        outs = carried
        if not final:
            state = outs[0]
    force, velocity, stress = outs
    return (
        force.reshape(positions.shape),
        velocity.reshape(positions.shape),
        stress.reshape(6, depth, width, lanes),
    )


def solution(mesh):
    beads = P(None, None, "gz", "xy", None)
    return jax.shard_map(
        shards,
        mesh=mesh,
        in_specs=(beads, beads, beads, P(None, "gz", "xy", None), P("gz", "xy", None), P()),
        out_specs=(beads, beads, P(None, "gz", "xy", None)),
        check_vma=False,
    )
```

```python
import functools
import math

import jax
import jax.numpy as jnp
from jax import lax
from jax.experimental import pallas as pl
from jax.experimental.pallas import tpu as pltpu
from jax.sharding import PartitionSpec as P

CONSERVATIVE = 25.0
FRICTION = 4.5
NOISE_LEVEL = 3.0
TIME_STEP = 0.04
SHEAR_SPEED = 1.0
CELL_VOLUME = 8.0
FLOOR_SQUARED = 0.0025
EDGE = 2.0
MODULUS = 65521
COMPONENT_PAIRS = [(0, 0), (1, 1), (2, 2), (0, 1), (0, 2), (1, 2)]

NOISE_UNIT = NOISE_LEVEL * math.sqrt(12.0) / math.sqrt(TIME_STEP)
SHIFT = CONSERVATIVE / NOISE_UNIT - 0.5 - 0.5 / MODULUS
VELOCITY_SCALE = FRICTION / NOISE_UNIT
INVERSE = 1.0 / MODULUS
FAR = 1.0e15
REACH = 1.001
SEED_MIDDLE = 8192
NEAR_SIDE, FAR_SIDE = 1, 2
F32 = jnp.float32
SUB = 8
UNROLL = 4
VMEM_LIMIT = 6 * 2**20
KICK_LIMIT = 67043328 - 160 * 1024


def take_rows(values, index):
    dims = lax.GatherDimensionNumbers(
        offset_dims=(),
        collapsed_slice_dims=(0,),
        start_index_map=(0,),
        operand_batching_dims=(1,),
        start_indices_batching_dims=(1,),
    )
    return lax.gather(
        values,
        index[..., None],
        dims,
        slice_sizes=(1, 1),
        mode=lax.GatherScatterMode.PROMISE_IN_BOUNDS,
    )


def centred(value):
    turns = jnp.round(value.astype(F32) * F32(INVERSE)).astype(jnp.int32)
    return (value - turns * MODULUS).astype(F32)


def home_noise(seed, step):
    a = seed.astype(jnp.int32) + (7919 * step + 1 + SEED_MIDDLE)
    return (
        centred(256 * a),
        centred(2 * a),
        centred(a * (a + 1)) + 0.5,
    )


def near_noise(seed):
    b = seed - SEED_MIDDLE
    high = jnp.floor((b + 64.0) * (1.0 / 128.0))
    low = b - 128.0 * high
    whole = b.astype(jnp.int32)
    return high, low, centred(whole * (whole + 1))


def pair_kernel(
    *refs, slots, lanes, sources, rows, own, step, first, last, virial, has_fixed, side
):
    refs = list(refs)
    take = lambda n: [refs.pop(0) for _ in range(n)]
    turning = side == FAR_SIDE
    home_ref, home_fixed_ref = take(2)
    home = None if own else take(1)[0]
    near_refs = take(sources)
    fixed_refs = take(sources) if has_fixed else near_refs
    force_in = None if first else take(1)[0]
    virial_in = take(1)[0] if (virial and not first) else None
    if last and virial:
        force_out, velocity_out, virial_out = take(3)
    elif virial:
        force_out, virial_out = take(2)
    else:
        (force_out,) = take(1)
    if own:
        (home,) = take(1)
    near, answer, rank, pick, liste, part, total, tally, sizes = take(9)
    groups = slots // SUB
    pitch = slots + SUB
    capacity = liste.shape[0] // 9
    iota = lax.broadcasted_iota(jnp.int32, (SUB, lanes), 0)
    iota_f = iota.astype(F32)
    fixed_at = 6 * slots
    if side:
        index, count = lax.axis_index("xy"), lax.axis_size("xy")
        upper = (lax.rem(index, 2) == 0) == (side == NEAR_SIDE)
        across = jnp.where(upper, F32(1.0), F32(-1.0))
    if turning:
        wraps = jnp.where(upper, index == count - 1, index == 0)
        strain_at = fixed_at + slots + 1 + step
        amount = jnp.max(home_fixed_ref[strain_at : strain_at + 1, :]).astype(jnp.int32)
        turn = jnp.where(upper, amount, lax.rem(lanes - amount, lanes))
        turn = jnp.where(wraps, turn, 0)
        shear = jnp.where(wraps, across * F32(SHEAR_SPEED), F32(0.0))

    def block(ref, base, group):
        return ref[base + group * SUB : base + (group + 1) * SUB, :]

    def spread(row):
        return jnp.broadcast_to(row, (SUB, lanes))

    box_at = 9 * pitch
    if own:
        home_count = spread(home_fixed_ref[fixed_at + slots : fixed_at + slots + 1, :])
        low = [jnp.full((SUB, lanes), FAR, F32) for _ in range(3)]
        high = [jnp.full((SUB, lanes), -FAR, F32) for _ in range(3)]
        for g in range(groups):
            there = iota_f + F32(g * SUB) < home_count
            for a in range(3):
                p = block(home_ref, a * slots, g)
                low[a] = jnp.minimum(low[a], jnp.where(there, p, FAR))
                high[a] = jnp.maximum(high[a], jnp.where(there, p, -FAR))
                at = a * pitch + g * SUB
                home[at : at + SUB, :] = jnp.where(there, p, -FAR) if a == 0 else p
                at = (3 + a) * pitch + g * SUB
                home[at : at + SUB, :] = block(home_ref, (3 + a) * slots, g) * F32(VELOCITY_SCALE)
            for a, value in enumerate(home_noise(block(home_fixed_ref, fixed_at, g), step)):
                at = (6 + a) * pitch + g * SUB
                home[at : at + SUB, :] = value
        home_low = [spread(jnp.min(v, axis=0, keepdims=True)) - REACH for v in low]
        home_high = [spread(jnp.max(v, axis=0, keepdims=True)) + REACH for v in high]
        for i, v in enumerate(home_low + home_high):
            home[box_at + i * SUB : box_at + (i + 1) * SUB, :] = v
    else:
        walls = [home[box_at + i * SUB : box_at + (i + 1) * SUB, :] for i in range(6)]
        home_low, home_high = walls[:3], walls[3:]
        home_there = [home[g * SUB : (g + 1) * SUB, :] > F32(-0.5 * FAR) for g in range(groups)]

    reach = {}
    for r, (source, offset, dz) in enumerate(rows):
        data, fixed = near_refs[source], fixed_refs[source]
        base = r * 7 * pitch
        turned = (lambda v: pltpu.roll(v, turn, 1)) if turning else (lambda v: v)
        count = turned(spread(fixed[offset[1] + fixed_at + slots : offset[1] + fixed_at + slots + 1, :]))
        reach_low = [jnp.full((SUB, lanes), FAR, F32) for _ in range(2)]
        reach_high = [jnp.full((SUB, lanes), -FAR, F32) for _ in range(2)]
        for g in range(groups):
            there = iota_f + F32(g * SUB) < count
            for c in range(7):
                ref, at = (fixed, offset[1]) if c == 6 else (data, offset[0])
                v = turned(block(ref, at + c * slots, g))
                if c == 0:
                    v = jnp.where(there, v, FAR)
                if c == 1 and side:
                    v = v + F32(EDGE) * across
                if c == 2 and dz:
                    v = v + F32(EDGE * dz)
                if c == 3 and turning:
                    v = v + shear
                if 3 <= c < 6:
                    v = v * F32(VELOCITY_SCALE)
                if c in (1, 2) and not own:
                    a = c - 1
                    reach_low[a] = jnp.minimum(reach_low[a], jnp.where(there, v, FAR))
                    reach_high[a] = jnp.maximum(reach_high[a], jnp.where(there, v, -FAR))
                near[base + c * pitch + g * SUB : base + c * pitch + (g + 1) * SUB, :] = v
        if not own:
            for a in range(2):
                least = jnp.min(reach_low[a], axis=0, keepdims=True)
                most = jnp.max(reach_high[a], axis=0, keepdims=True)
                least, most = spread(least), spread(most)
                least = jnp.minimum(least, jnp.minimum(pltpu.roll(least, 1, 1), pltpu.roll(least, lanes - 1, 1)))
                most = jnp.maximum(most, jnp.maximum(pltpu.roll(most, 1, 1), pltpu.roll(most, lanes - 1, 1)))
                reach[(r, a)] = (least - REACH, most + REACH)

    below = lax.broadcasted_iota(jnp.int32, (slots, slots), 0) >= lax.broadcasted_iota(
        jnp.int32, (slots, slots), 1
    )
    triangle = jnp.where(below, 1.0, 0.0).astype(jnp.bfloat16)

    def ranked(slot, marks):
        ones = jnp.concatenate([jnp.where(m, 1.0, 0.0) for m in marks], axis=0)
        upto = jnp.dot(triangle, ones.astype(jnp.bfloat16), preferred_element_type=F32)
        for g in range(groups):
            rows_of = slice(g * SUB, (g + 1) * SUB)
            place = jnp.where(marks[g], upto[rows_of, :] - 1.0, -1.0)
            rank[(slot * slots + g * SUB) : (slot * slots + (g + 1) * SUB), :] = place
        sizes[slot] = jnp.max(upto[slots - 1 : slots, :]).astype(jnp.int32)

    for r, (source, offset, dz) in enumerate(rows):
        base = r * 7 * pitch
        for d, dx in enumerate((0, -1, 1)):
            if own and d < 2:
                continue
            marks = []
            for g in range(groups):
                pos = [
                    near[base + a * pitch + g * SUB : base + a * pitch + (g + 1) * SUB, :]
                    for a in range(3)
                ]
                if dx:
                    pos = [pltpu.roll(v, (-dx) % lanes, 1) for v in pos]
                    pos[0] = pos[0] + F32(EDGE * dx)
                mark = (pos[0] > home_low[0]) & (pos[0] < home_high[0])
                for a in (1, 2):
                    mark = mark & (pos[a] > home_low[a]) & (pos[a] < home_high[a])
                marks.append(mark)
            ranked(4 * r + d, marks)
        if not own:
            marks = []
            for g in range(groups):
                mark = home_there[g]
                for a in range(2):
                    p = home[(a + 1) * pitch + g * SUB : (a + 1) * pitch + (g + 1) * SUB, :]
                    mark = mark & (p > reach[(r, a)][0]) & (p < reach[(r, a)][1])
                marks.append(mark)
            ranked(4 * r + 3, marks)

    def choose(slot, k):
        target = iota_f + (k * (2 * SUB)).astype(F32)
        index = [jnp.full((SUB, lanes), -1, jnp.int32) for _ in range(2)]
        for s in range(slots):
            place = rank[pl.ds(slot * slots + s, SUB, stride=0), :]
            for i in range(2):
                index[i] = jnp.where(place == target + F32(i * SUB), s, index[i])
        return index

    def gathered(ref, base, index):
        within = index & (SUB - 1)
        result = take_rows(ref[pl.ds(base, SUB), :], within)
        for g in range(1, groups):
            result = jnp.where(
                index >= g * SUB, take_rows(ref[pl.ds(base + g * SUB, SUB), :], within), result
            )
        return result

    def aligned(value):
        return pl.multiple_of(value, SUB)

    def run_pairs(count, where_home, blocks, start=0, react=False):
        def one(j, carry):
            carry = list(carry)
            n = [liste[pl.ds(c * capacity + start + j, SUB, stride=0), :] for c in range(9)]
            tot = [None] * 3
            for b in range(blocks):
                h = [where_home[c * pitch + b * SUB : c * pitch + (b + 1) * SUB, :] for c in range(9)]
                rx, ry, rz = h[0] - n[0], h[1] - n[1], h[2] - n[2]
                squared = jnp.maximum(rx * rx + ry * ry + rz * rz, FLOOR_SQUARED)
                u = jnp.maximum(lax.rsqrt(squared) - 1.0, 0.0)
                rv = rx * (h[3] - n[3]) + ry * (h[4] - n[4]) + rz * (h[5] - n[5])
                t = ((h[6] * n[6] + h[7] * n[7]) + (h[8] + n[8])) * F32(INVERSE)
                y = (t - jnp.floor(t)) + F32(SHIFT)
                magnitude = u * (y - u * rv)
                f = [magnitude * rx, magnitude * ry, magnitude * rz]
                for a in range(3):
                    carry[3 * b + a] = carry[3 * b + a] + f[a]
                    tot[a] = f[a] if tot[a] is None else tot[a] + f[a]
            if virial:
                for i, (a, b) in enumerate(COMPONENT_PAIRS):
                    carry[3 * blocks + i] = carry[3 * blocks + i] - n[a] * tot[b]
            if react:
                for a in range(3):
                    answer[pl.ds(a * slots + j, 1), :] = jnp.sum(tot[a], axis=0, keepdims=True)
            return tuple(carry)

        def several(i, carry):
            for k in range(UNROLL):
                carry = one(UNROLL * i + k, carry)
            return carry

        zero = jnp.zeros((SUB, lanes), F32)
        begin = (zero,) * (3 * blocks + (6 if virial else 0))
        done = lax.fori_loop(0, (count + UNROLL - 1) // UNROLL, several, begin)
        for b in range(blocks):
            for a in range(3):
                part[a * slots + b * SUB : a * slots + (b + 1) * SUB, :] = done[3 * b + a]
        if virial:
            for i, (a, b) in enumerate(COMPONENT_PAIRS):
                value = done[3 * blocks + i]
                for g in range(blocks):
                    value = value + (
                        where_home[a * pitch + g * SUB : a * pitch + (g + 1) * SUB, :] * done[3 * g + b]
                    )
                if react:
                    value = value + pltpu.roll(value, 1, 1)
                tally[i * SUB : (i + 1) * SUB, :] = tally[i * SUB : (i + 1) * SUB, :] + value

    for c in range(3):
        for g in range(groups):
            at = c * slots + g * SUB
            total[at : at + SUB, :] = (
                jnp.zeros((SUB, lanes), F32) if first else force_in[at : at + SUB, :]
            )
    if virial:
        for i in range(6):
            tally[i * SUB : (i + 1) * SUB, :] = (
                jnp.zeros((SUB, lanes), F32) if first else virial_in[i * SUB : (i + 1) * SUB, :]
            )

    def gather_near(at, index, dx):
        v = gathered(near, at, index)
        return pltpu.roll(v, (-dx) % lanes, 1) if dx else v

    def fill_near(base, slot, dx, filled, k):
        for i, index in enumerate(choose(slot, k)):
            valid = index >= 0
            if dx:
                index = pltpu.roll(index, dx % lanes, 1)
            values = [gather_near(base + c * pitch, index, dx) for c in range(7)]
            values[0] = jnp.where(valid, values[0] + F32(EDGE * dx), FAR)
            values = values[:6] + list(near_noise(values[6]))
            for c in range(9):
                at = c * capacity + filled + k * (2 * SUB) + i * SUB
                liste[pl.ds(at, SUB), :] = values[c]

    def fill_home(slot, k):
        for i, index in enumerate(choose(slot, k)):
            for c in range(9):
                v = gathered(home, c * pitch, index)
                if c == 0:
                    v = jnp.where(index >= 0, v, -FAR)
                pick[pl.ds(aligned(c * pitch + k * (2 * SUB) + i * SUB), SUB), :] = v

    def steps(size):
        return (size + 2 * SUB - 1) // (2 * SUB)

    def each(first, size, fill):
        def body(k, _):
            fill(k)
            return 0

        lax.fori_loop(first, steps(size), body, 0)

    def close(filled):
        liste[pl.ds(filled, SUB), :] = jnp.full((SUB, lanes), FAR, F32)
        for c in range(1, 9):
            liste[pl.ds(c * capacity + filled, SUB), :] = jnp.zeros((SUB, lanes), F32)

    def collect():
        for c in range(3):
            for g in range(groups):
                at = c * slots + g * SUB
                total[at : at + SUB, :] = total[at : at + SUB, :] + part[at : at + SUB, :]

    def own_row():
        for g in range(groups):
            values = [near[c * pitch + g * SUB : c * pitch + (g + 1) * SUB, :] for c in range(7)]
            values = values[:6] + list(near_noise(values[6]))
            for c in range(9):
                at = c * capacity + g * SUB
                liste[at : at + SUB, :] = values[c]
        size = sizes[2]
        each(0, size, functools.partial(fill_near, 0, 2, 1, slots))
        close(slots + size)
        run_pairs(slots, home, groups)
        collect()
        run_pairs(size, home, groups, start=slots, react=True)
        collect()

        def back(k, _):
            forces = [
                pltpu.roll(answer[pl.ds(aligned(c * slots + k * SUB), SUB), :], 1, 1) for c in range(3)
            ]
            for g in range(groups):
                place = rank[(2 * slots + g * SUB) : (2 * slots + (g + 1) * SUB), :]
                place = pltpu.roll(place, 1, 1).astype(jnp.int32)
                mine = (place >= k * SUB) & (place < (k + 1) * SUB)
                within = place & (SUB - 1)
                for c in range(3):
                    at = c * slots + g * SUB
                    v = take_rows(forces[c], within)
                    total[at : at + SUB, :] = total[at : at + SUB, :] - jnp.where(mine, v, 0.0)
            return 0

        lax.fori_loop(0, (size + SUB - 1) // SUB, back, 0)

    def direction(r, _):
        base = r * (7 * pitch)
        slot = 4 * r + 3
        needed = (sizes[slot] + SUB - 1) // SUB
        parts, filled, longest = [], jnp.int32(0), sizes[slot]
        for d, dx in enumerate((0, -1, 1)):
            size = sizes[4 * r + d]
            parts.append((size, functools.partial(fill_near, base, 4 * r + d, dx, filled)))
            filled = filled + size
            longest = jnp.maximum(longest, size)

        @pl.when(longest > 2 * SUB)
        def _():
            for size, fill in parts:
                each(1, size, fill)
            each(1, sizes[slot], functools.partial(fill_home, slot))

        for _, fill in parts:
            fill(jnp.int32(0))
        fill_home(slot, jnp.int32(0))
        close(filled)
        for blocks in range(1, groups + 1):
            pl.when(needed == blocks)(functools.partial(run_pairs, filled, pick, blocks))

        def back(k, _):
            for g in range(groups):
                place = rank[pl.ds(aligned(slot * slots + g * SUB), SUB), :].astype(jnp.int32)
                mine = (place >= k * SUB) & (place < (k + 1) * SUB)
                within = place & (SUB - 1)
                for c in range(3):
                    at = c * slots + g * SUB
                    v = take_rows(part[pl.ds(aligned(c * slots + k * SUB), SUB), :], within)
                    total[at : at + SUB, :] = total[at : at + SUB, :] + jnp.where(mine, v, 0.0)
            return 0

        lax.fori_loop(0, needed, back, 0)
        return 0

    if own:
        own_row()
    else:
        lax.fori_loop(0, len(rows), direction, 0)

    half = F32(0.5 * TIME_STEP)
    for c in range(3):
        for g in range(groups):
            at = c * slots + g * SUB
            f = total[at : at + SUB, :]
            if not last:
                force_out[at : at + SUB, :] = f
                continue
            f = f * F32(NOISE_UNIT)
            v = block(home_ref, (3 + c) * slots, g) + half * f
            if virial:
                force_out[at : at + SUB, :] = f
                velocity_out[at : at + SUB, :] = jnp.where(home_there[g], v, 0.0)
            else:
                v = v + half * f
                force_out[at : at + SUB, :] = block(home_ref, c * slots, g) + F32(TIME_STEP) * v
                force_out[3 * slots + at : 3 * slots + at + SUB, :] = v
    if virial:
        for i in range(6):
            v = tally[i * SUB : (i + 1) * SUB, :]
            if last:
                virial_out[i] = jnp.sum(v, axis=0, keepdims=True) * F32(
                    NOISE_UNIT * 0.5 / CELL_VOLUME
                )
            else:
                virial_out[i * SUB : (i + 1) * SUB, :] = v


def pairs(home, home_fixed, beads, nears, fixed, carried, rows, step, last, virial, slots, cost, side=0):
    lanes = home.shape[-1]
    own = len(rows) == 1
    first = carried is None
    operands = [home, home_fixed, *beads, *nears]
    if fixed is not None:
        operands += list(fixed)
    if not first:
        operands += list(carried)
    shape = lambda n: jax.ShapeDtypeStruct((n, lanes), F32)
    if last and virial:
        outs = (shape(3 * slots), shape(3 * slots), jax.ShapeDtypeStruct((6, 1, lanes), F32))
    elif virial:
        outs = (shape(3 * slots), shape(6 * SUB))
    elif last:
        outs = (shape(6 * slots),)
    else:
        outs = (shape(3 * slots),)
    pitch = slots + SUB
    if own:
        outs += (shape(9 * pitch + 6 * SUB),)
    vmem = pl.BlockSpec(memory_space=pltpu.VMEM)
    capacity = 3 * slots + 2 * SUB + 1
    count = len(rows)
    return pl.pallas_call(
        functools.partial(
            pair_kernel,
            slots=slots,
            lanes=lanes,
            sources=len(nears),
            rows=rows,
            own=own,
            step=step,
            first=first,
            last=last,
            virial=virial,
            has_fixed=fixed is not None,
            side=side,
        ),
        out_shape=outs,
        in_specs=[vmem] * len(operands),
        out_specs=tuple(vmem for _ in outs),
        scratch_shapes=[
            pltpu.VMEM((count * 7 * pitch, lanes), F32),
            pltpu.VMEM((4 * slots, lanes), F32),
            pltpu.VMEM((count * 4 * slots, lanes), F32),
            pltpu.VMEM((9 * pitch, lanes), F32),
            pltpu.VMEM((9 * capacity, lanes), F32),
            pltpu.VMEM((3 * slots, lanes), F32),
            pltpu.VMEM((3 * slots, lanes), F32),
            pltpu.VMEM((6 * SUB, lanes), F32),
            pltpu.SMEM((4 * count,), jnp.int32),
        ],
        compiler_params=pltpu.CompilerParams(vmem_limit_bytes=VMEM_LIMIT),
        cost_estimate=pl.CostEstimate(flops=cost, bytes_accessed=1, transcendentals=0),
        name=f"pairs_{side}_{step}",
    )(*operands)


def kick_kernel(*refs, slots, lanes):
    sources, out, held, done = refs[:6], refs[6], refs[7:13], refs[13]
    copies = [
        pltpu.make_async_copy(source, target, done.at[i])
        for i, (source, target) in enumerate(zip(sources, held))
    ]
    for copy in copies:
        copy.start()
    for copy in copies:
        copy.wait()
    position, velocity, force, seed, count, strain = held
    for c in range(3):
        for g in range(slots // SUB):
            at = c * slots + g * SUB
            rows = slice(at, at + SUB)
            v = velocity[rows, :] + F32(0.5 * TIME_STEP) * force[rows, :]
            out[rows, :] = position[rows, :] + F32(TIME_STEP) * v
            out[3 * slots + at : 3 * slots + at + SUB, :] = v
    out[6 * slots : 7 * slots, :] = seed[...].astype(F32)
    aside = jnp.broadcast_to(count[...], (SUB, lanes)).astype(F32)
    row = lax.broadcasted_iota(jnp.int32, (SUB, lanes), 0)
    for step in range(strain.shape[1]):
        aside = jnp.where(row == 1 + step, strain[:, step : step + 1].astype(F32), aside)
    out[7 * slots : 7 * slots + SUB, :] = aside


def ring(count, by):
    return [(i, (i + by) % count) for i in range(count)]


def swap(count, first):
    assert count % 2 == 0
    pairs_of = [((first + i) % count, (first + i + 1) % count) for i in range(0, count, 2)]
    return pairs_of + [(b, a) for a, b in pairs_of]


def shards(positions, velocities, forces_prev, seeds, counts, offsets):
    slots, depth, width, lanes = seeds.shape
    assert depth == 1 and width == 1
    gz, xy = lax.axis_size("gz"), lax.axis_size("xy")
    flat = lambda a: a.reshape(-1, lanes)
    tall = 7 * slots + SUB
    inputs = [flat(a) for a in (positions, velocities, forces_prev, seeds, counts)]
    inputs.append(offsets.reshape(1, -1))
    state = pl.pallas_call(
        functools.partial(kick_kernel, slots=slots, lanes=lanes),
        out_shape=jax.ShapeDtypeStruct((tall, lanes), F32),
        in_specs=[pl.BlockSpec(memory_space=pltpu.HBM)] * len(inputs),
        out_specs=pl.BlockSpec(memory_space=pltpu.VMEM),
        scratch_shapes=[pltpu.VMEM(a.shape, a.dtype) for a in inputs]
        + [pltpu.SemaphoreType.DMA((len(inputs),))],
        compiler_params=pltpu.CompilerParams(vmem_limit_bytes=KICK_LIMIT),
        name="kick",
    )(*inputs)
    home_fixed = state
    kept = None
    for step in range(2):
        final = step == 1
        high = state.shape[0]
        planes = [lax.ppermute(state, "gz", ring(gz, -1))]
        if gz > 2:
            planes.append(lax.ppermute(state, "gz", ring(gz, 1)))
        up, down = 0, len(planes) - 1
        call = functools.partial(
            pairs, state, home_fixed, step=step, virial=final, slots=slots
        )
        here = (0, 0)
        *carried, beads = call(
            [],
            [state],
            [home_fixed] if final else None,
            None,
            rows=((0, here, 0),),
            last=False,
            cost=100_000_000,
        )
        planes, carried, beads = lax.optimization_barrier((planes, carried, beads))
        stacked = jnp.concatenate([state, *planes], axis=0)
        far = lax.ppermute(stacked, "xy", swap(xy, 1))
        near = lax.ppermute(stacked, "xy", swap(xy, 0))
        arrived = (planes, [near], [far])
        if not final:
            kept = arrived
        carried = call(
            [beads],
            planes,
            kept[0] if final else None,
            carried,
            rows=((down, here, -1), (up, here, 1)),
            last=False,
            cost=100_000_000,
        )
        beside = tuple(
            (0, (place * high, place * tall), dz) for dz, place in ((0, 0), (-1, 1 + down), (1, 1 + up))
        )
        for side in (NEAR_SIDE, FAR_SIDE):
            carried = call(
                [beads],
                arrived[side],
                kept[side] if final else None,
                carried,
                rows=beside,
                last=side == FAR_SIDE,
                cost=100_000_000,
                side=side,
            )
        outs = carried
        if not final:
            state = outs[0]
    force, velocity, stress = outs
    return (
        force.reshape(positions.shape),
        velocity.reshape(positions.shape),
        stress.reshape(6, depth, width, lanes),
    )


def solution(mesh):
    beads = P(None, None, "gz", "xy", None)
    return jax.shard_map(
        shards,
        mesh=mesh,
        in_specs=(beads, beads, beads, P(None, "gz", "xy", None), P("gz", "xy", None), P()),
        out_specs=(beads, beads, P(None, "gz", "xy", None)),
        check_vma=False,
    )
```

```python
import functools
import math

import jax
import jax.numpy as jnp
from jax import lax
from jax.experimental import pallas as pl
from jax.experimental.pallas import tpu as pltpu
from jax.sharding import PartitionSpec as P

CONSERVATIVE = 25.0
FRICTION = 4.5
NOISE_LEVEL = 3.0
TIME_STEP = 0.04
SHEAR_SPEED = 1.0
CELL_VOLUME = 8.0
FLOOR_SQUARED = 0.0025
EDGE = 2.0
MODULUS = 65521
COMPONENT_PAIRS = [(0, 0), (1, 1), (2, 2), (0, 1), (0, 2), (1, 2)]

NOISE_UNIT = NOISE_LEVEL * math.sqrt(12.0) / math.sqrt(TIME_STEP)
SHIFT = CONSERVATIVE / NOISE_UNIT - 0.5 - 0.5 / MODULUS
VELOCITY_SCALE = FRICTION / NOISE_UNIT
INVERSE = 1.0 / MODULUS
FAR = 1.0e15
REACH = 1.001
SEED_MIDDLE = 8192
NEAR_SIDE, FAR_SIDE = 1, 2
F32 = jnp.float32
SUB = 8
UNROLL = 4
VMEM_LIMIT = 6 * 2**20
KICK_LIMIT = 67043328 - 160 * 1024


def take_rows(values, index):
    dims = lax.GatherDimensionNumbers(
        offset_dims=(),
        collapsed_slice_dims=(0,),
        start_index_map=(0,),
        operand_batching_dims=(1,),
        start_indices_batching_dims=(1,),
    )
    return lax.gather(
        values,
        index[..., None],
        dims,
        slice_sizes=(1, 1),
        mode=lax.GatherScatterMode.PROMISE_IN_BOUNDS,
    )


def centred(value):
    turns = jnp.round(value.astype(F32) * F32(INVERSE)).astype(jnp.int32)
    return (value - turns * MODULUS).astype(F32)


def home_noise(seed, step):
    a = seed.astype(jnp.int32) + (7919 * step + 1 + SEED_MIDDLE)
    return (
        centred(256 * a),
        centred(2 * a),
        centred(a * (a + 1)) + 0.5,
    )


def near_noise(seed):
    b = seed - SEED_MIDDLE
    high = jnp.floor((b + 64.0) * (1.0 / 128.0))
    low = b - 128.0 * high
    whole = b.astype(jnp.int32)
    return high, low, centred(whole * (whole + 1))


def pair_kernel(
    *refs, slots, lanes, sources, rows, own, step, first, last, virial, has_fixed, side
):
    refs = list(refs)
    take = lambda n: [refs.pop(0) for _ in range(n)]
    turning = side == FAR_SIDE
    home_ref, home_fixed_ref = take(2)
    home = None if own else take(1)[0]
    near_refs = take(sources)
    fixed_refs = take(sources) if has_fixed else near_refs
    force_in = None if first else take(1)[0]
    virial_in = take(1)[0] if (virial and not first) else None
    if last and virial:
        force_out, velocity_out, virial_out = take(3)
    elif virial:
        force_out, virial_out = take(2)
    else:
        (force_out,) = take(1)
    if own:
        (home,) = take(1)
    near, answer, rank, upto, pick, liste, part, total, tally, sizes = take(10)
    groups = slots // SUB
    pitch = slots + SUB
    capacity = liste.shape[0] // 9
    iota = lax.broadcasted_iota(jnp.int32, (SUB, lanes), 0)
    iota_f = iota.astype(F32)
    fixed_at = 6 * slots
    if side:
        index, count = lax.axis_index("xy"), lax.axis_size("xy")
        upper = (lax.rem(index, 2) == 0) == (side == NEAR_SIDE)
        across = jnp.where(upper, F32(1.0), F32(-1.0))
    if turning:
        wraps = jnp.where(upper, index == count - 1, index == 0)
        strain_at = fixed_at + slots + 1 + step
        amount = jnp.max(home_fixed_ref[strain_at : strain_at + 1, :]).astype(jnp.int32)
        turn = jnp.where(upper, amount, lax.rem(lanes - amount, lanes))
        turn = jnp.where(wraps, turn, 0)
        shear = jnp.where(wraps, across * F32(SHEAR_SPEED), F32(0.0))

    def block(ref, base, group):
        return ref[base + group * SUB : base + (group + 1) * SUB, :]

    def spread(row):
        return jnp.broadcast_to(row, (SUB, lanes))

    box_at = 9 * pitch
    if own:
        home_count = spread(home_fixed_ref[fixed_at + slots : fixed_at + slots + 1, :])
        low = [jnp.full((SUB, lanes), FAR, F32) for _ in range(3)]
        high = [jnp.full((SUB, lanes), -FAR, F32) for _ in range(3)]
        for g in range(groups):
            there = iota_f + F32(g * SUB) < home_count
            for a in range(3):
                p = block(home_ref, a * slots, g)
                low[a] = jnp.minimum(low[a], jnp.where(there, p, FAR))
                high[a] = jnp.maximum(high[a], jnp.where(there, p, -FAR))
                at = a * pitch + g * SUB
                home[at : at + SUB, :] = jnp.where(there, p, -FAR) if a == 0 else p
                at = (3 + a) * pitch + g * SUB
                home[at : at + SUB, :] = block(home_ref, (3 + a) * slots, g) * F32(VELOCITY_SCALE)
            for a, value in enumerate(home_noise(block(home_fixed_ref, fixed_at, g), step)):
                at = (6 + a) * pitch + g * SUB
                home[at : at + SUB, :] = value
        home_low = [spread(jnp.min(v, axis=0, keepdims=True)) - REACH for v in low]
        home_high = [spread(jnp.max(v, axis=0, keepdims=True)) + REACH for v in high]
        for i, v in enumerate(home_low + home_high):
            home[box_at + i * SUB : box_at + (i + 1) * SUB, :] = v
    else:
        walls = [home[box_at + i * SUB : box_at + (i + 1) * SUB, :] for i in range(6)]
        home_low, home_high = walls[:3], walls[3:]
        home_there = [home[g * SUB : (g + 1) * SUB, :] > F32(-0.5 * FAR) for g in range(groups)]

    reach = {}
    for r, (source, offset, dz) in enumerate(rows):
        data, fixed = near_refs[source], fixed_refs[source]
        base = r * 7 * pitch
        turned = (lambda v: pltpu.roll(v, turn, 1)) if turning else (lambda v: v)
        count = turned(spread(fixed[offset[1] + fixed_at + slots : offset[1] + fixed_at + slots + 1, :]))
        reach_low = [jnp.full((SUB, lanes), FAR, F32) for _ in range(2)]
        reach_high = [jnp.full((SUB, lanes), -FAR, F32) for _ in range(2)]
        for g in range(groups):
            there = iota_f + F32(g * SUB) < count
            for c in range(7):
                ref, at = (fixed, offset[1]) if c == 6 else (data, offset[0])
                v = turned(block(ref, at + c * slots, g))
                if c == 0:
                    v = jnp.where(there, v, FAR)
                if c == 1 and side:
                    v = v + F32(EDGE) * across
                if c == 2 and dz:
                    v = v + F32(EDGE * dz)
                if c == 3 and turning:
                    v = v + shear
                if 3 <= c < 6:
                    v = v * F32(VELOCITY_SCALE)
                if c in (1, 2) and not own:
                    a = c - 1
                    reach_low[a] = jnp.minimum(reach_low[a], jnp.where(there, v, FAR))
                    reach_high[a] = jnp.maximum(reach_high[a], jnp.where(there, v, -FAR))
                near[base + c * pitch + g * SUB : base + c * pitch + (g + 1) * SUB, :] = v
        if not own:
            for a in range(2):
                least = jnp.min(reach_low[a], axis=0, keepdims=True)
                most = jnp.max(reach_high[a], axis=0, keepdims=True)
                least, most = spread(least), spread(most)
                least = jnp.minimum(least, jnp.minimum(pltpu.roll(least, 1, 1), pltpu.roll(least, lanes - 1, 1)))
                most = jnp.maximum(most, jnp.maximum(pltpu.roll(most, 1, 1), pltpu.roll(most, lanes - 1, 1)))
                reach[(r, a)] = (least - REACH, most + REACH)

    below = lax.broadcasted_iota(jnp.int32, (slots, slots), 0) >= lax.broadcasted_iota(
        jnp.int32, (slots, slots), 1
    )
    triangle = jnp.where(below, 1.0, 0.0).astype(jnp.bfloat16)

    def ranked(slot, marks):
        ones = jnp.concatenate([jnp.where(m, 1.0, 0.0) for m in marks], axis=0)
        running = jnp.dot(triangle, ones.astype(jnp.bfloat16), preferred_element_type=F32)
        upto[slot * slots : (slot + 1) * slots, :] = running
        for g in range(groups):
            rows_of = slice(g * SUB, (g + 1) * SUB)
            place = jnp.where(marks[g], running[rows_of, :] - 1.0, -1.0)
            rank[(slot * slots + g * SUB) : (slot * slots + (g + 1) * SUB), :] = place
        sizes[slot] = jnp.max(running[slots - 1 : slots, :]).astype(jnp.int32)

    for r, (source, offset, dz) in enumerate(rows):
        base = r * 7 * pitch
        for d, dx in enumerate((0, -1, 1)):
            if own and d < 2:
                continue
            marks = []
            for g in range(groups):
                pos = [
                    near[base + a * pitch + g * SUB : base + a * pitch + (g + 1) * SUB, :]
                    for a in range(3)
                ]
                if dx:
                    pos = [pltpu.roll(v, (-dx) % lanes, 1) for v in pos]
                    pos[0] = pos[0] + F32(EDGE * dx)
                mark = (pos[0] > home_low[0]) & (pos[0] < home_high[0])
                for a in (1, 2):
                    mark = mark & (pos[a] > home_low[a]) & (pos[a] < home_high[a])
                marks.append(mark)
            ranked(4 * r + d, marks)
        if not own:
            marks = []
            for g in range(groups):
                mark = home_there[g]
                for a in range(2):
                    p = home[(a + 1) * pitch + g * SUB : (a + 1) * pitch + (g + 1) * SUB, :]
                    mark = mark & (p > reach[(r, a)][0]) & (p < reach[(r, a)][1])
                marks.append(mark)
            ranked(4 * r + 3, marks)

    def choose(slot, k):
        at = slot * slots
        line = lambda row: upto[pl.ds(at + row, SUB, stride=0), :]
        ends = [line(g * SUB + SUB - 1) for g in range(groups)]
        middles = [line(g * SUB + SUB // 2 - 1) for g in range(groups)]
        counts = [upto[pl.ds(aligned(at + g * SUB), SUB), :] for g in range(groups)]
        result = []
        for i in range(2):
            target = iota_f + ((k * (2 * SUB)).astype(F32) + F32(i * SUB))
            beyond = [ends[g] <= target for g in range(groups - 1)]

            def chosen(values):
                v = values[0]
                for g in range(1, groups):
                    v = jnp.where(beyond[g - 1], values[g], v)
                return v

            first = chosen([jnp.full((SUB, lanes), g * SUB, jnp.int32) for g in range(groups)])
            place = jnp.where(chosen(middles) <= target, SUB // 2, 0)
            for width in (2, 1):
                probe = place + (width - 1)
                found = chosen([take_rows(v, probe) for v in counts])
                place = jnp.where(found <= target, place + width, place)
            result.append(jnp.where(ends[groups - 1] > target, first + place, -1))
        return result

    def gathered(ref, base, index):
        within = index & (SUB - 1)
        result = take_rows(ref[pl.ds(base, SUB), :], within)
        for g in range(1, groups):
            result = jnp.where(
                index >= g * SUB, take_rows(ref[pl.ds(base + g * SUB, SUB), :], within), result
            )
        return result

    def aligned(value):
        return pl.multiple_of(value, SUB)

    def run_pairs(count, where_home, blocks, start=0, react=False):
        def one(j, carry):
            carry = list(carry)
            n = [liste[pl.ds(c * capacity + start + j, SUB, stride=0), :] for c in range(9)]
            tot = [None] * 3
            for b in range(blocks):
                h = [where_home[c * pitch + b * SUB : c * pitch + (b + 1) * SUB, :] for c in range(9)]
                rx, ry, rz = h[0] - n[0], h[1] - n[1], h[2] - n[2]
                squared = jnp.maximum(rx * rx + ry * ry + rz * rz, FLOOR_SQUARED)
                u = jnp.maximum(lax.rsqrt(squared) - 1.0, 0.0)
                rv = rx * (h[3] - n[3]) + ry * (h[4] - n[4]) + rz * (h[5] - n[5])
                t = ((h[6] * n[6] + h[7] * n[7]) + (h[8] + n[8])) * F32(INVERSE)
                y = (t - jnp.floor(t)) + F32(SHIFT)
                magnitude = u * (y - u * rv)
                f = [magnitude * rx, magnitude * ry, magnitude * rz]
                for a in range(3):
                    carry[3 * b + a] = carry[3 * b + a] + f[a]
                    tot[a] = f[a] if tot[a] is None else tot[a] + f[a]
            if virial:
                for i, (a, b) in enumerate(COMPONENT_PAIRS):
                    carry[3 * blocks + i] = carry[3 * blocks + i] - n[a] * tot[b]
            if react:
                for a in range(3):
                    answer[pl.ds(a * slots + j, 1), :] = jnp.sum(tot[a], axis=0, keepdims=True)
            return tuple(carry)

        def several(i, carry):
            for k in range(UNROLL):
                carry = one(UNROLL * i + k, carry)
            return carry

        zero = jnp.zeros((SUB, lanes), F32)
        begin = (zero,) * (3 * blocks + (6 if virial else 0))
        done = lax.fori_loop(0, (count + UNROLL - 1) // UNROLL, several, begin)
        for b in range(blocks):
            for a in range(3):
                part[a * slots + b * SUB : a * slots + (b + 1) * SUB, :] = done[3 * b + a]
        if virial:
            for i, (a, b) in enumerate(COMPONENT_PAIRS):
                value = done[3 * blocks + i]
                for g in range(blocks):
                    value = value + (
                        where_home[a * pitch + g * SUB : a * pitch + (g + 1) * SUB, :] * done[3 * g + b]
                    )
                if react:
                    value = value + pltpu.roll(value, 1, 1)
                tally[i * SUB : (i + 1) * SUB, :] = tally[i * SUB : (i + 1) * SUB, :] + value

    for c in range(3):
        for g in range(groups):
            at = c * slots + g * SUB
            total[at : at + SUB, :] = (
                jnp.zeros((SUB, lanes), F32) if first else force_in[at : at + SUB, :]
            )
    if virial:
        for i in range(6):
            tally[i * SUB : (i + 1) * SUB, :] = (
                jnp.zeros((SUB, lanes), F32) if first else virial_in[i * SUB : (i + 1) * SUB, :]
            )

    def gather_near(at, index, dx):
        v = gathered(near, at, index)
        return pltpu.roll(v, (-dx) % lanes, 1) if dx else v

    def fill_near(base, slot, dx, filled, k):
        for i, index in enumerate(choose(slot, k)):
            valid = index >= 0
            if dx:
                index = pltpu.roll(index, dx % lanes, 1)
            values = [gather_near(base + c * pitch, index, dx) for c in range(7)]
            values[0] = jnp.where(valid, values[0] + F32(EDGE * dx), FAR)
            values = values[:6] + list(near_noise(values[6]))
            for c in range(9):
                at = c * capacity + filled + k * (2 * SUB) + i * SUB
                liste[pl.ds(at, SUB), :] = values[c]

    def fill_home(slot, k):
        for i, index in enumerate(choose(slot, k)):
            for c in range(9):
                v = gathered(home, c * pitch, index)
                if c == 0:
                    v = jnp.where(index >= 0, v, -FAR)
                pick[pl.ds(aligned(c * pitch + k * (2 * SUB) + i * SUB), SUB), :] = v

    def steps(size):
        return (size + 2 * SUB - 1) // (2 * SUB)

    def each(first, size, fill):
        def body(k, _):
            fill(k)
            return 0

        lax.fori_loop(first, steps(size), body, 0)

    def close(filled):
        liste[pl.ds(filled, SUB), :] = jnp.full((SUB, lanes), FAR, F32)
        for c in range(1, 9):
            liste[pl.ds(c * capacity + filled, SUB), :] = jnp.zeros((SUB, lanes), F32)

    def collect():
        for c in range(3):
            for g in range(groups):
                at = c * slots + g * SUB
                total[at : at + SUB, :] = total[at : at + SUB, :] + part[at : at + SUB, :]

    def own_row():
        for g in range(groups):
            values = [near[c * pitch + g * SUB : c * pitch + (g + 1) * SUB, :] for c in range(7)]
            values = values[:6] + list(near_noise(values[6]))
            for c in range(9):
                at = c * capacity + g * SUB
                liste[at : at + SUB, :] = values[c]
        size = sizes[2]
        each(0, size, functools.partial(fill_near, 0, 2, 1, slots))
        close(slots + size)
        run_pairs(slots, home, groups)
        collect()
        run_pairs(size, home, groups, start=slots, react=True)
        collect()

        def back(k, _):
            forces = [
                pltpu.roll(answer[pl.ds(aligned(c * slots + k * SUB), SUB), :], 1, 1) for c in range(3)
            ]
            for g in range(groups):
                place = rank[(2 * slots + g * SUB) : (2 * slots + (g + 1) * SUB), :]
                place = pltpu.roll(place, 1, 1).astype(jnp.int32)
                mine = (place >= k * SUB) & (place < (k + 1) * SUB)
                within = place & (SUB - 1)
                for c in range(3):
                    at = c * slots + g * SUB
                    v = take_rows(forces[c], within)
                    total[at : at + SUB, :] = total[at : at + SUB, :] - jnp.where(mine, v, 0.0)
            return 0

        lax.fori_loop(0, (size + SUB - 1) // SUB, back, 0)

    def direction(r, _):
        base = r * (7 * pitch)
        slot = 4 * r + 3
        needed = (sizes[slot] + SUB - 1) // SUB
        parts, filled, longest = [], jnp.int32(0), sizes[slot]
        for d, dx in enumerate((0, -1, 1)):
            size = sizes[4 * r + d]
            parts.append((size, functools.partial(fill_near, base, 4 * r + d, dx, filled)))
            filled = filled + size
            longest = jnp.maximum(longest, size)

        @pl.when(longest > 2 * SUB)
        def _():
            for size, fill in parts:
                each(1, size, fill)
            each(1, sizes[slot], functools.partial(fill_home, slot))

        for _, fill in parts:
            fill(jnp.int32(0))
        fill_home(slot, jnp.int32(0))
        close(filled)
        for blocks in range(1, groups + 1):
            pl.when(needed == blocks)(functools.partial(run_pairs, filled, pick, blocks))

        def back(k, _):
            for g in range(groups):
                place = rank[pl.ds(aligned(slot * slots + g * SUB), SUB), :].astype(jnp.int32)
                mine = (place >= k * SUB) & (place < (k + 1) * SUB)
                within = place & (SUB - 1)
                for c in range(3):
                    at = c * slots + g * SUB
                    v = take_rows(part[pl.ds(aligned(c * slots + k * SUB), SUB), :], within)
                    total[at : at + SUB, :] = total[at : at + SUB, :] + jnp.where(mine, v, 0.0)
            return 0

        lax.fori_loop(0, needed, back, 0)
        return 0

    if own:
        own_row()
    else:
        lax.fori_loop(0, len(rows), direction, 0)

    half = F32(0.5 * TIME_STEP)
    for c in range(3):
        for g in range(groups):
            at = c * slots + g * SUB
            f = total[at : at + SUB, :]
            if not last:
                force_out[at : at + SUB, :] = f
                continue
            f = f * F32(NOISE_UNIT)
            v = block(home_ref, (3 + c) * slots, g) + half * f
            if virial:
                force_out[at : at + SUB, :] = f
                velocity_out[at : at + SUB, :] = jnp.where(home_there[g], v, 0.0)
            else:
                v = v + half * f
                force_out[at : at + SUB, :] = block(home_ref, c * slots, g) + F32(TIME_STEP) * v
                force_out[3 * slots + at : 3 * slots + at + SUB, :] = v
    if virial:
        for i in range(6):
            v = tally[i * SUB : (i + 1) * SUB, :]
            if last:
                virial_out[i] = jnp.sum(v, axis=0, keepdims=True) * F32(
                    NOISE_UNIT * 0.5 / CELL_VOLUME
                )
            else:
                virial_out[i * SUB : (i + 1) * SUB, :] = v


def pairs(home, home_fixed, beads, nears, fixed, carried, rows, step, last, virial, slots, cost, side=0):
    lanes = home.shape[-1]
    own = len(rows) == 1
    first = carried is None
    operands = [home, home_fixed, *beads, *nears]
    if fixed is not None:
        operands += list(fixed)
    if not first:
        operands += list(carried)
    shape = lambda n: jax.ShapeDtypeStruct((n, lanes), F32)
    if last and virial:
        outs = (shape(3 * slots), shape(3 * slots), jax.ShapeDtypeStruct((6, 1, lanes), F32))
    elif virial:
        outs = (shape(3 * slots), shape(6 * SUB))
    elif last:
        outs = (shape(6 * slots),)
    else:
        outs = (shape(3 * slots),)
    pitch = slots + SUB
    if own:
        outs += (shape(9 * pitch + 6 * SUB),)
    vmem = pl.BlockSpec(memory_space=pltpu.VMEM)
    capacity = 3 * slots + 2 * SUB + 1
    count = len(rows)
    return pl.pallas_call(
        functools.partial(
            pair_kernel,
            slots=slots,
            lanes=lanes,
            sources=len(nears),
            rows=rows,
            own=own,
            step=step,
            first=first,
            last=last,
            virial=virial,
            has_fixed=fixed is not None,
            side=side,
        ),
        out_shape=outs,
        in_specs=[vmem] * len(operands),
        out_specs=tuple(vmem for _ in outs),
        scratch_shapes=[
            pltpu.VMEM((count * 7 * pitch, lanes), F32),
            pltpu.VMEM((4 * slots, lanes), F32),
            pltpu.VMEM((count * 4 * slots, lanes), F32),
            pltpu.VMEM((count * 4 * slots, lanes), F32),
            pltpu.VMEM((9 * pitch, lanes), F32),
            pltpu.VMEM((9 * capacity, lanes), F32),
            pltpu.VMEM((3 * slots, lanes), F32),
            pltpu.VMEM((3 * slots, lanes), F32),
            pltpu.VMEM((6 * SUB, lanes), F32),
            pltpu.SMEM((4 * count,), jnp.int32),
        ],
        compiler_params=pltpu.CompilerParams(vmem_limit_bytes=VMEM_LIMIT),
        cost_estimate=pl.CostEstimate(flops=cost, bytes_accessed=1, transcendentals=0),
        name=f"pairs_{side}_{step}",
    )(*operands)


def kick_kernel(*refs, slots, lanes):
    sources, out, held, done = refs[:6], refs[6], refs[7:13], refs[13]
    copies = [
        pltpu.make_async_copy(source, target, done.at[i])
        for i, (source, target) in enumerate(zip(sources, held))
    ]
    for copy in copies:
        copy.start()
    for copy in copies:
        copy.wait()
    position, velocity, force, seed, count, strain = held
    for c in range(3):
        for g in range(slots // SUB):
            at = c * slots + g * SUB
            rows = slice(at, at + SUB)
            v = velocity[rows, :] + F32(0.5 * TIME_STEP) * force[rows, :]
            out[rows, :] = position[rows, :] + F32(TIME_STEP) * v
            out[3 * slots + at : 3 * slots + at + SUB, :] = v
    out[6 * slots : 7 * slots, :] = seed[...].astype(F32)
    aside = jnp.broadcast_to(count[...], (SUB, lanes)).astype(F32)
    row = lax.broadcasted_iota(jnp.int32, (SUB, lanes), 0)
    for step in range(strain.shape[1]):
        aside = jnp.where(row == 1 + step, strain[:, step : step + 1].astype(F32), aside)
    out[7 * slots : 7 * slots + SUB, :] = aside


def ring(count, by):
    return [(i, (i + by) % count) for i in range(count)]


def swap(count, first):
    assert count % 2 == 0
    pairs_of = [((first + i) % count, (first + i + 1) % count) for i in range(0, count, 2)]
    return pairs_of + [(b, a) for a, b in pairs_of]


def shards(positions, velocities, forces_prev, seeds, counts, offsets):
    slots, depth, width, lanes = seeds.shape
    assert depth == 1 and width == 1
    gz, xy = lax.axis_size("gz"), lax.axis_size("xy")
    flat = lambda a: a.reshape(-1, lanes)
    tall = 7 * slots + SUB
    inputs = [flat(a) for a in (positions, velocities, forces_prev, seeds, counts)]
    inputs.append(offsets.reshape(1, -1))
    state = pl.pallas_call(
        functools.partial(kick_kernel, slots=slots, lanes=lanes),
        out_shape=jax.ShapeDtypeStruct((tall, lanes), F32),
        in_specs=[pl.BlockSpec(memory_space=pltpu.HBM)] * len(inputs),
        out_specs=pl.BlockSpec(memory_space=pltpu.VMEM),
        scratch_shapes=[pltpu.VMEM(a.shape, a.dtype) for a in inputs]
        + [pltpu.SemaphoreType.DMA((len(inputs),))],
        compiler_params=pltpu.CompilerParams(vmem_limit_bytes=KICK_LIMIT),
        name="kick",
    )(*inputs)
    home_fixed = state
    kept = None
    for step in range(2):
        final = step == 1
        high = state.shape[0]
        planes = [lax.ppermute(state, "gz", ring(gz, -1))]
        if gz > 2:
            planes.append(lax.ppermute(state, "gz", ring(gz, 1)))
        up, down = 0, len(planes) - 1
        call = functools.partial(
            pairs, state, home_fixed, step=step, virial=final, slots=slots
        )
        here = (0, 0)
        *carried, beads = call(
            [],
            [state],
            [home_fixed] if final else None,
            None,
            rows=((0, here, 0),),
            last=False,
            cost=100_000_000,
        )
        planes, carried, beads = lax.optimization_barrier((planes, carried, beads))
        stacked = jnp.concatenate([state, *planes], axis=0)
        far = lax.ppermute(stacked, "xy", swap(xy, 1))
        near = lax.ppermute(stacked, "xy", swap(xy, 0))
        arrived = (planes, [near], [far])
        if not final:
            kept = arrived
        carried = call(
            [beads],
            planes,
            kept[0] if final else None,
            carried,
            rows=((down, here, -1), (up, here, 1)),
            last=False,
            cost=100_000_000,
        )
        beside = tuple(
            (0, (place * high, place * tall), dz) for dz, place in ((0, 0), (-1, 1 + down), (1, 1 + up))
        )
        for side in (NEAR_SIDE, FAR_SIDE):
            carried = call(
                [beads],
                arrived[side],
                kept[side] if final else None,
                carried,
                rows=beside,
                last=side == FAR_SIDE,
                cost=100_000_000,
                side=side,
            )
        outs = carried
        if not final:
            state = outs[0]
    force, velocity, stress = outs
    return (
        force.reshape(positions.shape),
        velocity.reshape(positions.shape),
        stress.reshape(6, depth, width, lanes),
    )


def solution(mesh):
    beads = P(None, None, "gz", "xy", None)
    return jax.shard_map(
        shards,
        mesh=mesh,
        in_specs=(beads, beads, beads, P(None, "gz", "xy", None), P("gz", "xy", None), P()),
        out_specs=(beads, beads, P(None, "gz", "xy", None)),
        check_vma=False,
    )
```

```python
import functools
import math

import jax
import jax.numpy as jnp
from jax import lax
from jax.experimental import pallas as pl
from jax.experimental.pallas import tpu as pltpu
from jax.sharding import PartitionSpec as P

CONSERVATIVE = 25.0
FRICTION = 4.5
NOISE_LEVEL = 3.0
TIME_STEP = 0.04
SHEAR_SPEED = 1.0
CELL_VOLUME = 8.0
FLOOR_SQUARED = 0.0025
EDGE = 2.0
MODULUS = 65521
COMPONENT_PAIRS = [(0, 0), (1, 1), (2, 2), (0, 1), (0, 2), (1, 2)]

NOISE_UNIT = NOISE_LEVEL * math.sqrt(12.0) / math.sqrt(TIME_STEP)
SHIFT = CONSERVATIVE / NOISE_UNIT - 0.5 - 0.5 / MODULUS
VELOCITY_SCALE = FRICTION / NOISE_UNIT
INVERSE = 1.0 / MODULUS
FAR = 1.0e15
REACH = 1.001
SEED_MIDDLE = 8192
NEAR_SIDE, FAR_SIDE = 1, 2
F32 = jnp.float32
SUB = 8
UNROLL = 4
VMEM_LIMIT = 6 * 2**20
KICK_LIMIT = 67043328 - 160 * 1024


def take_rows(values, index):
    dims = lax.GatherDimensionNumbers(
        offset_dims=(),
        collapsed_slice_dims=(0,),
        start_index_map=(0,),
        operand_batching_dims=(1,),
        start_indices_batching_dims=(1,),
    )
    return lax.gather(
        values,
        index[..., None],
        dims,
        slice_sizes=(1, 1),
        mode=lax.GatherScatterMode.PROMISE_IN_BOUNDS,
    )


def centred(value):
    turns = jnp.round(value.astype(F32) * F32(INVERSE)).astype(jnp.int32)
    return (value - turns * MODULUS).astype(F32)


def home_noise(seed, step):
    a = seed.astype(jnp.int32) + (7919 * step + 1 + SEED_MIDDLE)
    return (
        centred(256 * a),
        centred(2 * a),
        centred(a * (a + 1)) + 0.5,
    )


def near_noise(seed):
    b = seed - SEED_MIDDLE
    high = jnp.floor((b + 64.0) * (1.0 / 128.0))
    low = b - 128.0 * high
    whole = b.astype(jnp.int32)
    return high, low, centred(whole * (whole + 1))


def pair_kernel(
    *refs, slots, lanes, sources, rows, own, step, first, last, virial, has_fixed, side
):
    refs = list(refs)
    take = lambda n: [refs.pop(0) for _ in range(n)]
    turning = side == FAR_SIDE
    home_ref, home_fixed_ref = take(2)
    home = None if own else take(1)[0]
    near_refs = take(sources)
    fixed_refs = take(sources) if has_fixed else near_refs
    force_in = None if first else take(1)[0]
    virial_in = take(1)[0] if (virial and not first) else None
    if last and virial:
        force_out, velocity_out, virial_out = take(3)
    elif virial:
        force_out, virial_out = take(2)
    else:
        (force_out,) = take(1)
    if own:
        (home,) = take(1)
    near, answer, rank, upto, pick, liste, part, total, tally, sizes = take(10)
    groups = slots // SUB
    pitch = slots + SUB
    capacity = liste.shape[0] // 9
    iota = lax.broadcasted_iota(jnp.int32, (SUB, lanes), 0)
    iota_f = iota.astype(F32)
    fixed_at = 6 * slots
    if side:
        index, count = lax.axis_index("xy"), lax.axis_size("xy")
        upper = (lax.rem(index, 2) == 0) == (side == NEAR_SIDE)
        across = jnp.where(upper, F32(1.0), F32(-1.0))
    if turning:
        wraps = jnp.where(upper, index == count - 1, index == 0)
        strain_at = fixed_at + slots + 1 + step
        amount = jnp.max(home_fixed_ref[strain_at : strain_at + 1, :]).astype(jnp.int32)
        turn = jnp.where(upper, amount, lax.rem(lanes - amount, lanes))
        turn = jnp.where(wraps, turn, 0)
        shear = jnp.where(wraps, across * F32(SHEAR_SPEED), F32(0.0))

    def block(ref, base, group):
        return ref[base + group * SUB : base + (group + 1) * SUB, :]

    def spread(row):
        return jnp.broadcast_to(row, (SUB, lanes))

    box_at = 9 * pitch
    if own:
        home_count = spread(home_fixed_ref[fixed_at + slots : fixed_at + slots + 1, :])
        low = [jnp.full((SUB, lanes), FAR, F32) for _ in range(3)]
        high = [jnp.full((SUB, lanes), -FAR, F32) for _ in range(3)]
        for g in range(groups):
            there = iota_f + F32(g * SUB) < home_count
            for a in range(3):
                p = block(home_ref, a * slots, g)
                low[a] = jnp.minimum(low[a], jnp.where(there, p, FAR))
                high[a] = jnp.maximum(high[a], jnp.where(there, p, -FAR))
                at = a * pitch + g * SUB
                home[at : at + SUB, :] = jnp.where(there, p, -FAR) if a == 0 else p
                at = (3 + a) * pitch + g * SUB
                home[at : at + SUB, :] = block(home_ref, (3 + a) * slots, g) * F32(VELOCITY_SCALE)
            for a, value in enumerate(home_noise(block(home_fixed_ref, fixed_at, g), step)):
                at = (6 + a) * pitch + g * SUB
                home[at : at + SUB, :] = value
        home_low = [spread(jnp.min(v, axis=0, keepdims=True)) - REACH for v in low]
        home_high = [spread(jnp.max(v, axis=0, keepdims=True)) + REACH for v in high]
        for i, v in enumerate(home_low + home_high):
            home[box_at + i * SUB : box_at + (i + 1) * SUB, :] = v
    else:
        walls = [home[box_at + i * SUB : box_at + (i + 1) * SUB, :] for i in range(6)]
        home_low, home_high = walls[:3], walls[3:]
        home_there = [home[g * SUB : (g + 1) * SUB, :] > F32(-0.5 * FAR) for g in range(groups)]

    reach = {}
    for r, (source, offset, dz) in enumerate(rows):
        data, fixed = near_refs[source], fixed_refs[source]
        base = r * 7 * pitch
        turned = (lambda v: pltpu.roll(v, turn, 1)) if turning else (lambda v: v)
        count = turned(spread(fixed[offset[1] + fixed_at + slots : offset[1] + fixed_at + slots + 1, :]))
        reach_low = [jnp.full((SUB, lanes), FAR, F32) for _ in range(2)]
        reach_high = [jnp.full((SUB, lanes), -FAR, F32) for _ in range(2)]
        for g in range(groups):
            there = iota_f + F32(g * SUB) < count
            for c in range(7):
                ref, at = (fixed, offset[1]) if c == 6 else (data, offset[0])
                v = turned(block(ref, at + c * slots, g))
                if c == 0:
                    v = jnp.where(there, v, FAR)
                if c == 1 and side:
                    v = v + F32(EDGE) * across
                if c == 2 and dz:
                    v = v + F32(EDGE * dz)
                if c == 3 and turning:
                    v = v + shear
                if 3 <= c < 6:
                    v = v * F32(VELOCITY_SCALE)
                if c in (1, 2) and not own:
                    a = c - 1
                    reach_low[a] = jnp.minimum(reach_low[a], jnp.where(there, v, FAR))
                    reach_high[a] = jnp.maximum(reach_high[a], jnp.where(there, v, -FAR))
                near[base + c * pitch + g * SUB : base + c * pitch + (g + 1) * SUB, :] = v
        if not own:
            for a in range(2):
                least = jnp.min(reach_low[a], axis=0, keepdims=True)
                most = jnp.max(reach_high[a], axis=0, keepdims=True)
                least, most = spread(least), spread(most)
                least = jnp.minimum(least, jnp.minimum(pltpu.roll(least, 1, 1), pltpu.roll(least, lanes - 1, 1)))
                most = jnp.maximum(most, jnp.maximum(pltpu.roll(most, 1, 1), pltpu.roll(most, lanes - 1, 1)))
                reach[(r, a)] = (least - REACH, most + REACH)

    below = lax.broadcasted_iota(jnp.int32, (slots, slots), 0) >= lax.broadcasted_iota(
        jnp.int32, (slots, slots), 1
    )
    triangle = jnp.where(below, 1.0, 0.0).astype(jnp.bfloat16)

    def ranked(slot, marks):
        ones = jnp.concatenate([jnp.where(m, 1.0, 0.0) for m in marks], axis=0)
        running = jnp.dot(triangle, ones.astype(jnp.bfloat16), preferred_element_type=F32)
        upto[slot * slots : (slot + 1) * slots, :] = running
        for g in range(groups):
            rows_of = slice(g * SUB, (g + 1) * SUB)
            place = jnp.where(marks[g], running[rows_of, :] - 1.0, -1.0)
            rank[(slot * slots + g * SUB) : (slot * slots + (g + 1) * SUB), :] = place
        sizes[slot] = jnp.max(running[slots - 1 : slots, :]).astype(jnp.int32)

    for r, (source, offset, dz) in enumerate(rows):
        base = r * 7 * pitch
        for d, dx in enumerate((0, -1, 1)):
            if own and d < 2:
                continue
            marks = []
            for g in range(groups):
                pos = [
                    near[base + a * pitch + g * SUB : base + a * pitch + (g + 1) * SUB, :]
                    for a in range(3)
                ]
                if dx:
                    pos = [pltpu.roll(v, (-dx) % lanes, 1) for v in pos]
                    pos[0] = pos[0] + F32(EDGE * dx)
                mark = (pos[0] > home_low[0]) & (pos[0] < home_high[0])
                for a in (1, 2):
                    mark = mark & (pos[a] > home_low[a]) & (pos[a] < home_high[a])
                marks.append(mark)
            ranked(4 * r + d, marks)
        if not own:
            marks = []
            for g in range(groups):
                mark = home_there[g]
                for a in range(2):
                    p = home[(a + 1) * pitch + g * SUB : (a + 1) * pitch + (g + 1) * SUB, :]
                    mark = mark & (p > reach[(r, a)][0]) & (p < reach[(r, a)][1])
                marks.append(mark)
            ranked(4 * r + 3, marks)

    def choose(slot, k):
        at = slot * slots
        line = lambda row: upto[pl.ds(at + row, SUB, stride=0), :]
        ends = [line(g * SUB + SUB - 1) for g in range(groups)]
        middles = [line(g * SUB + SUB // 2 - 1) for g in range(groups)]
        counts = [upto[pl.ds(aligned(at + g * SUB), SUB), :] for g in range(groups)]
        result = []
        for i in range(2):
            target = iota_f + ((k * (2 * SUB)).astype(F32) + F32(i * SUB))
            beyond = [ends[g] <= target for g in range(groups - 1)]

            def chosen(values):
                v = values[0]
                for g in range(1, groups):
                    v = jnp.where(beyond[g - 1], values[g], v)
                return v

            first = chosen([jnp.full((SUB, lanes), g * SUB, jnp.int32) for g in range(groups)])
            place = jnp.where(chosen(middles) <= target, SUB // 2, 0)
            for width in (2, 1):
                probe = place + (width - 1)
                found = chosen([take_rows(v, probe) for v in counts])
                place = jnp.where(found <= target, place + width, place)
            result.append(jnp.where(ends[groups - 1] > target, first + place, -1))
        return result

    def gathered(ref, base, index):
        within = index & (SUB - 1)
        result = take_rows(ref[pl.ds(base, SUB), :], within)
        for g in range(1, groups):
            result = jnp.where(
                index >= g * SUB, take_rows(ref[pl.ds(base + g * SUB, SUB), :], within), result
            )
        return result

    def aligned(value):
        return pl.multiple_of(value, SUB)

    def run_pairs(count, where_home, blocks, start=0, react=False):
        def one(j, carry):
            carry = list(carry)
            n = [liste[pl.ds(c * capacity + start + j, SUB, stride=0), :] for c in range(9)]
            tot = [None] * 3
            for b in range(blocks):
                h = [where_home[c * pitch + b * SUB : c * pitch + (b + 1) * SUB, :] for c in range(9)]
                rx, ry, rz = h[0] - n[0], h[1] - n[1], h[2] - n[2]
                squared = jnp.maximum(rx * rx + ry * ry + rz * rz, FLOOR_SQUARED)
                u = jnp.maximum(lax.rsqrt(squared) - 1.0, 0.0)
                rv = rx * (h[3] - n[3]) + ry * (h[4] - n[4]) + rz * (h[5] - n[5])
                t = ((h[6] * n[6] + h[7] * n[7]) + (h[8] + n[8])) * F32(INVERSE)
                y = (t - jnp.floor(t)) + F32(SHIFT)
                magnitude = u * (y - u * rv)
                f = [magnitude * rx, magnitude * ry, magnitude * rz]
                for a in range(3):
                    carry[3 * b + a] = carry[3 * b + a] + f[a]
                    tot[a] = f[a] if tot[a] is None else tot[a] + f[a]
            if virial:
                for i, (a, b) in enumerate(COMPONENT_PAIRS):
                    carry[3 * blocks + i] = carry[3 * blocks + i] - n[a] * tot[b]
            if react:
                for a in range(3):
                    answer[pl.ds(a * slots + j, 1), :] = jnp.sum(tot[a], axis=0, keepdims=True)
            return tuple(carry)

        def several(i, carry):
            for k in range(UNROLL):
                carry = one(UNROLL * i + k, carry)
            return carry

        zero = jnp.zeros((SUB, lanes), F32)
        begin = (zero,) * (3 * blocks + (6 if virial else 0))
        done = lax.fori_loop(0, (count + UNROLL - 1) // UNROLL, several, begin)
        for b in range(blocks):
            for a in range(3):
                part[a * slots + b * SUB : a * slots + (b + 1) * SUB, :] = done[3 * b + a]
        if virial:
            for i, (a, b) in enumerate(COMPONENT_PAIRS):
                value = done[3 * blocks + i]
                for g in range(blocks):
                    value = value + (
                        where_home[a * pitch + g * SUB : a * pitch + (g + 1) * SUB, :] * done[3 * g + b]
                    )
                if react:
                    value = value + pltpu.roll(value, 1, 1)
                tally[i * SUB : (i + 1) * SUB, :] = tally[i * SUB : (i + 1) * SUB, :] + value

    for c in range(3):
        for g in range(groups):
            at = c * slots + g * SUB
            total[at : at + SUB, :] = (
                jnp.zeros((SUB, lanes), F32) if first else force_in[at : at + SUB, :]
            )
    if virial:
        for i in range(6):
            tally[i * SUB : (i + 1) * SUB, :] = (
                jnp.zeros((SUB, lanes), F32) if first else virial_in[i * SUB : (i + 1) * SUB, :]
            )

    def gather_near(at, index, dx):
        v = gathered(near, at, index)
        return pltpu.roll(v, (-dx) % lanes, 1) if dx else v

    def fill_near(base, slot, dx, filled, k):
        for i, index in enumerate(choose(slot, k)):
            valid = index >= 0
            if dx:
                index = pltpu.roll(index, dx % lanes, 1)
            values = [gather_near(base + c * pitch, index, dx) for c in range(7)]
            values[0] = jnp.where(valid, values[0] + F32(EDGE * dx), FAR)
            values = values[:6] + list(near_noise(values[6]))
            for c in range(9):
                at = c * capacity + filled + k * (2 * SUB) + i * SUB
                liste[pl.ds(at, SUB), :] = values[c]

    def fill_home(slot, k):
        for i, index in enumerate(choose(slot, k)):
            for c in range(9):
                v = gathered(home, c * pitch, index)
                if c == 0:
                    v = jnp.where(index >= 0, v, -FAR)
                pick[pl.ds(aligned(c * pitch + k * (2 * SUB) + i * SUB), SUB), :] = v

    def steps(size):
        return (size + 2 * SUB - 1) // (2 * SUB)

    def each(first, size, fill):
        def body(k, _):
            fill(k)
            return 0

        lax.fori_loop(first, steps(size), body, 0)

    def close(filled):
        liste[pl.ds(filled, SUB), :] = jnp.full((SUB, lanes), FAR, F32)
        for c in range(1, 9):
            liste[pl.ds(c * capacity + filled, SUB), :] = jnp.zeros((SUB, lanes), F32)

    def collect():
        for c in range(3):
            for g in range(groups):
                at = c * slots + g * SUB
                total[at : at + SUB, :] = total[at : at + SUB, :] + part[at : at + SUB, :]

    def own_row():
        for g in range(groups):
            values = [near[c * pitch + g * SUB : c * pitch + (g + 1) * SUB, :] for c in range(7)]
            values = values[:6] + list(near_noise(values[6]))
            for c in range(9):
                at = c * capacity + g * SUB
                liste[at : at + SUB, :] = values[c]
        size = sizes[2]
        each(0, size, functools.partial(fill_near, 0, 2, 1, slots))
        close(slots + size)
        run_pairs(slots, home, groups)
        collect()
        run_pairs(size, home, groups, start=slots, react=True)
        collect()

        def back(k, _):
            forces = [
                pltpu.roll(answer[pl.ds(aligned(c * slots + k * SUB), SUB), :], 1, 1) for c in range(3)
            ]
            for g in range(groups):
                place = rank[(2 * slots + g * SUB) : (2 * slots + (g + 1) * SUB), :]
                place = pltpu.roll(place, 1, 1).astype(jnp.int32)
                mine = (place >= k * SUB) & (place < (k + 1) * SUB)
                within = place & (SUB - 1)
                for c in range(3):
                    at = c * slots + g * SUB
                    v = take_rows(forces[c], within)
                    total[at : at + SUB, :] = total[at : at + SUB, :] - jnp.where(mine, v, 0.0)
            return 0

        lax.fori_loop(0, (size + SUB - 1) // SUB, back, 0)

    def direction(r, _):
        base = r * (7 * pitch)
        slot = 4 * r + 3
        needed = (sizes[slot] + SUB - 1) // SUB
        parts, filled, longest = [], jnp.int32(0), sizes[slot]
        for d, dx in enumerate((0, -1, 1)):
            size = sizes[4 * r + d]
            parts.append((size, functools.partial(fill_near, base, 4 * r + d, dx, filled)))
            filled = filled + size
            longest = jnp.maximum(longest, size)

        @pl.when(longest > 2 * SUB)
        def _():
            for size, fill in parts:
                each(1, size, fill)
            each(1, sizes[slot], functools.partial(fill_home, slot))

        for _, fill in parts:
            fill(jnp.int32(0))
        fill_home(slot, jnp.int32(0))
        close(filled)
        for blocks in range(1, groups + 1):
            pl.when(needed == blocks)(functools.partial(run_pairs, filled, pick, blocks))

        def back(k, _):
            for g in range(groups):
                place = rank[pl.ds(aligned(slot * slots + g * SUB), SUB), :].astype(jnp.int32)
                mine = (place >= k * SUB) & (place < (k + 1) * SUB)
                within = place & (SUB - 1)
                for c in range(3):
                    at = c * slots + g * SUB
                    v = take_rows(part[pl.ds(aligned(c * slots + k * SUB), SUB), :], within)
                    total[at : at + SUB, :] = total[at : at + SUB, :] + jnp.where(mine, v, 0.0)
            return 0

        lax.fori_loop(0, needed, back, 0)
        return 0

    if own:
        own_row()
    else:
        for r in range(len(rows)):
            direction(jnp.int32(r), 0)

    half = F32(0.5 * TIME_STEP)
    for c in range(3):
        for g in range(groups):
            at = c * slots + g * SUB
            f = total[at : at + SUB, :]
            if not last:
                force_out[at : at + SUB, :] = f
                continue
            f = f * F32(NOISE_UNIT)
            v = block(home_ref, (3 + c) * slots, g) + half * f
            if virial:
                force_out[at : at + SUB, :] = f
                velocity_out[at : at + SUB, :] = jnp.where(home_there[g], v, 0.0)
            else:
                v = v + half * f
                force_out[at : at + SUB, :] = block(home_ref, c * slots, g) + F32(TIME_STEP) * v
                force_out[3 * slots + at : 3 * slots + at + SUB, :] = v
    if virial:
        for i in range(6):
            v = tally[i * SUB : (i + 1) * SUB, :]
            if last:
                virial_out[i] = jnp.sum(v, axis=0, keepdims=True) * F32(
                    NOISE_UNIT * 0.5 / CELL_VOLUME
                )
            else:
                virial_out[i * SUB : (i + 1) * SUB, :] = v


def pairs(home, home_fixed, beads, nears, fixed, carried, rows, step, last, virial, slots, cost, side=0):
    lanes = home.shape[-1]
    own = len(rows) == 1
    first = carried is None
    operands = [home, home_fixed, *beads, *nears]
    if fixed is not None:
        operands += list(fixed)
    if not first:
        operands += list(carried)
    shape = lambda n: jax.ShapeDtypeStruct((n, lanes), F32)
    if last and virial:
        outs = (shape(3 * slots), shape(3 * slots), jax.ShapeDtypeStruct((6, 1, lanes), F32))
    elif virial:
        outs = (shape(3 * slots), shape(6 * SUB))
    elif last:
        outs = (shape(6 * slots),)
    else:
        outs = (shape(3 * slots),)
    pitch = slots + SUB
    if own:
        outs += (shape(9 * pitch + 6 * SUB),)
    vmem = pl.BlockSpec(memory_space=pltpu.VMEM)
    capacity = 3 * slots + 2 * SUB + 1
    count = len(rows)
    return pl.pallas_call(
        functools.partial(
            pair_kernel,
            slots=slots,
            lanes=lanes,
            sources=len(nears),
            rows=rows,
            own=own,
            step=step,
            first=first,
            last=last,
            virial=virial,
            has_fixed=fixed is not None,
            side=side,
        ),
        out_shape=outs,
        in_specs=[vmem] * len(operands),
        out_specs=tuple(vmem for _ in outs),
        scratch_shapes=[
            pltpu.VMEM((count * 7 * pitch, lanes), F32),
            pltpu.VMEM((4 * slots, lanes), F32),
            pltpu.VMEM((count * 4 * slots, lanes), F32),
            pltpu.VMEM((count * 4 * slots, lanes), F32),
            pltpu.VMEM((9 * pitch, lanes), F32),
            pltpu.VMEM((9 * capacity, lanes), F32),
            pltpu.VMEM((3 * slots, lanes), F32),
            pltpu.VMEM((3 * slots, lanes), F32),
            pltpu.VMEM((6 * SUB, lanes), F32),
            pltpu.SMEM((4 * count,), jnp.int32),
        ],
        compiler_params=pltpu.CompilerParams(vmem_limit_bytes=VMEM_LIMIT),
        cost_estimate=pl.CostEstimate(flops=cost, bytes_accessed=1, transcendentals=0),
        name=f"pairs_{side}_{step}",
    )(*operands)


def kick_kernel(*refs, slots, lanes):
    sources, out, held, done = refs[:6], refs[6], refs[7:13], refs[13]
    copies = [
        pltpu.make_async_copy(source, target, done.at[i])
        for i, (source, target) in enumerate(zip(sources, held))
    ]
    for copy in copies:
        copy.start()
    for copy in copies:
        copy.wait()
    position, velocity, force, seed, count, strain = held
    for c in range(3):
        for g in range(slots // SUB):
            at = c * slots + g * SUB
            rows = slice(at, at + SUB)
            v = velocity[rows, :] + F32(0.5 * TIME_STEP) * force[rows, :]
            out[rows, :] = position[rows, :] + F32(TIME_STEP) * v
            out[3 * slots + at : 3 * slots + at + SUB, :] = v
    out[6 * slots : 7 * slots, :] = seed[...].astype(F32)
    aside = jnp.broadcast_to(count[...], (SUB, lanes)).astype(F32)
    row = lax.broadcasted_iota(jnp.int32, (SUB, lanes), 0)
    for step in range(strain.shape[1]):
        aside = jnp.where(row == 1 + step, strain[:, step : step + 1].astype(F32), aside)
    out[7 * slots : 7 * slots + SUB, :] = aside


def ring(count, by):
    return [(i, (i + by) % count) for i in range(count)]


def swap(count, first):
    assert count % 2 == 0
    pairs_of = [((first + i) % count, (first + i + 1) % count) for i in range(0, count, 2)]
    return pairs_of + [(b, a) for a, b in pairs_of]


def shards(positions, velocities, forces_prev, seeds, counts, offsets):
    slots, depth, width, lanes = seeds.shape
    assert depth == 1 and width == 1
    gz, xy = lax.axis_size("gz"), lax.axis_size("xy")
    flat = lambda a: a.reshape(-1, lanes)
    tall = 7 * slots + SUB
    inputs = [flat(a) for a in (positions, velocities, forces_prev, seeds, counts)]
    inputs.append(offsets.reshape(1, -1))
    state = pl.pallas_call(
        functools.partial(kick_kernel, slots=slots, lanes=lanes),
        out_shape=jax.ShapeDtypeStruct((tall, lanes), F32),
        in_specs=[pl.BlockSpec(memory_space=pltpu.HBM)] * len(inputs),
        out_specs=pl.BlockSpec(memory_space=pltpu.VMEM),
        scratch_shapes=[pltpu.VMEM(a.shape, a.dtype) for a in inputs]
        + [pltpu.SemaphoreType.DMA((len(inputs),))],
        compiler_params=pltpu.CompilerParams(vmem_limit_bytes=KICK_LIMIT),
        name="kick",
    )(*inputs)
    home_fixed = state
    kept = None
    for step in range(2):
        final = step == 1
        high = state.shape[0]
        planes = [lax.ppermute(state, "gz", ring(gz, -1))]
        if gz > 2:
            planes.append(lax.ppermute(state, "gz", ring(gz, 1)))
        up, down = 0, len(planes) - 1
        call = functools.partial(
            pairs, state, home_fixed, step=step, virial=final, slots=slots
        )
        here = (0, 0)
        *carried, beads = call(
            [],
            [state],
            [home_fixed] if final else None,
            None,
            rows=((0, here, 0),),
            last=False,
            cost=100_000_000,
        )
        planes, carried, beads = lax.optimization_barrier((planes, carried, beads))
        stacked = jnp.concatenate([state, *planes], axis=0)
        far = lax.ppermute(stacked, "xy", swap(xy, 1))
        near = lax.ppermute(stacked, "xy", swap(xy, 0))
        arrived = (planes, [near], [far])
        if not final:
            kept = arrived
        carried = call(
            [beads],
            planes,
            kept[0] if final else None,
            carried,
            rows=((down, here, -1), (up, here, 1)),
            last=False,
            cost=100_000_000,
        )
        beside = tuple(
            (0, (place * high, place * tall), dz) for dz, place in ((0, 0), (-1, 1 + down), (1, 1 + up))
        )
        for side in (NEAR_SIDE, FAR_SIDE):
            carried = call(
                [beads],
                arrived[side],
                kept[side] if final else None,
                carried,
                rows=beside,
                last=side == FAR_SIDE,
                cost=100_000_000,
                side=side,
            )
        outs = carried
        if not final:
            state = outs[0]
    force, velocity, stress = outs
    return (
        force.reshape(positions.shape),
        velocity.reshape(positions.shape),
        stress.reshape(6, depth, width, lanes),
    )


def solution(mesh):
    beads = P(None, None, "gz", "xy", None)
    return jax.shard_map(
        shards,
        mesh=mesh,
        in_specs=(beads, beads, beads, P(None, "gz", "xy", None), P("gz", "xy", None), P()),
        out_specs=(beads, beads, P(None, "gz", "xy", None)),
        check_vma=False,
    )
```

```python
import functools
import math

import jax
import jax.numpy as jnp
from jax import lax
from jax.experimental import pallas as pl
from jax.experimental.pallas import tpu as pltpu
from jax.sharding import PartitionSpec as P

CONSERVATIVE = 25.0
FRICTION = 4.5
NOISE_LEVEL = 3.0
TIME_STEP = 0.04
SHEAR_SPEED = 1.0
CELL_VOLUME = 8.0
FLOOR_SQUARED = 0.0025
EDGE = 2.0
MODULUS = 65521
COMPONENT_PAIRS = [(0, 0), (1, 1), (2, 2), (0, 1), (0, 2), (1, 2)]

NOISE_UNIT = NOISE_LEVEL * math.sqrt(12.0) / math.sqrt(TIME_STEP)
SHIFT = CONSERVATIVE / NOISE_UNIT - 0.5 - 0.5 / MODULUS
VELOCITY_SCALE = FRICTION / NOISE_UNIT
INVERSE = 1.0 / MODULUS
FAR = 1.0e15
REACH = 1.001
SEED_MIDDLE = 8192
NEAR_SIDE, FAR_SIDE = 1, 2
F32 = jnp.float32
SUB = 8
UNROLL = 4
VMEM_LIMIT = 6 * 2**20
KICK_LIMIT = 67043328 - 160 * 1024


def take_rows(values, index):
    dims = lax.GatherDimensionNumbers(
        offset_dims=(),
        collapsed_slice_dims=(0,),
        start_index_map=(0,),
        operand_batching_dims=(1,),
        start_indices_batching_dims=(1,),
    )
    return lax.gather(
        values,
        index[..., None],
        dims,
        slice_sizes=(1, 1),
        mode=lax.GatherScatterMode.PROMISE_IN_BOUNDS,
    )


def centred(value):
    turns = jnp.round(value.astype(F32) * F32(INVERSE)).astype(jnp.int32)
    return (value - turns * MODULUS).astype(F32)


def home_noise(seed, step):
    a = seed.astype(jnp.int32) + (7919 * step + 1 + SEED_MIDDLE)
    return (
        centred(256 * a),
        centred(2 * a),
        centred(a * (a + 1)) + 0.5,
    )


def near_noise(seed):
    b = seed - SEED_MIDDLE
    high = jnp.floor((b + 64.0) * (1.0 / 128.0))
    low = b - 128.0 * high
    whole = b.astype(jnp.int32)
    return high, low, centred(whole * (whole + 1))


def pair_kernel(
    *refs, slots, lanes, sources, rows, own, step, first, last, virial, has_fixed, side
):
    refs = list(refs)
    take = lambda n: [refs.pop(0) for _ in range(n)]
    turning = side == FAR_SIDE
    home_ref, home_fixed_ref = take(2)
    home = None if own else take(1)[0]
    near_refs = take(sources)
    fixed_refs = take(sources) if has_fixed else near_refs
    force_in = None if first else take(1)[0]
    virial_in = take(1)[0] if (virial and not first) else None
    if last and virial:
        force_out, velocity_out, virial_out = take(3)
    elif virial:
        force_out, virial_out = take(2)
    else:
        (force_out,) = take(1)
    if own:
        (home,) = take(1)
    near, answer, rank, upto, pick, liste, part, total, tally, sizes = take(10)
    groups = slots // SUB
    pitch = slots + SUB
    capacity = liste.shape[0] // 9
    iota = lax.broadcasted_iota(jnp.int32, (SUB, lanes), 0)
    iota_f = iota.astype(F32)
    fixed_at = 6 * slots
    if side:
        index, count = lax.axis_index("xy"), lax.axis_size("xy")
        upper = (lax.rem(index, 2) == 0) == (side == NEAR_SIDE)
        across = jnp.where(upper, F32(1.0), F32(-1.0))
    if turning:
        wraps = jnp.where(upper, index == count - 1, index == 0)
        strain_at = fixed_at + slots + 1 + step
        amount = jnp.max(home_fixed_ref[strain_at : strain_at + 1, :]).astype(jnp.int32)
        turn = jnp.where(upper, amount, lax.rem(lanes - amount, lanes))
        turn = jnp.where(wraps, turn, 0)
        shear = jnp.where(wraps, across * F32(SHEAR_SPEED), F32(0.0))

    def block(ref, base, group):
        return ref[base + group * SUB : base + (group + 1) * SUB, :]

    def spread(row):
        return jnp.broadcast_to(row, (SUB, lanes))

    box_at = 9 * pitch
    if own:
        home_count = spread(home_fixed_ref[fixed_at + slots : fixed_at + slots + 1, :])
        low = [jnp.full((SUB, lanes), FAR, F32) for _ in range(3)]
        high = [jnp.full((SUB, lanes), -FAR, F32) for _ in range(3)]
        for g in range(groups):
            there = iota_f + F32(g * SUB) < home_count
            for a in range(3):
                p = block(home_ref, a * slots, g)
                low[a] = jnp.minimum(low[a], jnp.where(there, p, FAR))
                high[a] = jnp.maximum(high[a], jnp.where(there, p, -FAR))
                at = a * pitch + g * SUB
                home[at : at + SUB, :] = jnp.where(there, p, -FAR) if a == 0 else p
                at = (3 + a) * pitch + g * SUB
                home[at : at + SUB, :] = block(home_ref, (3 + a) * slots, g) * F32(VELOCITY_SCALE)
            for a, value in enumerate(home_noise(block(home_fixed_ref, fixed_at, g), step)):
                at = (6 + a) * pitch + g * SUB
                home[at : at + SUB, :] = value
        home_low = [spread(jnp.min(v, axis=0, keepdims=True)) - REACH for v in low]
        home_high = [spread(jnp.max(v, axis=0, keepdims=True)) + REACH for v in high]
        for i, v in enumerate(home_low + home_high):
            home[box_at + i * SUB : box_at + (i + 1) * SUB, :] = v
    else:
        walls = [home[box_at + i * SUB : box_at + (i + 1) * SUB, :] for i in range(6)]
        home_low, home_high = walls[:3], walls[3:]
        home_there = [home[g * SUB : (g + 1) * SUB, :] > F32(-0.5 * FAR) for g in range(groups)]

    reach = {}
    for r, (source, offset, dz) in enumerate(rows):
        data, fixed = near_refs[source], fixed_refs[source]
        base = r * 7 * pitch
        turned = (lambda v: pltpu.roll(v, turn, 1)) if turning else (lambda v: v)
        count = turned(spread(fixed[offset[1] + fixed_at + slots : offset[1] + fixed_at + slots + 1, :]))
        reach_low = [jnp.full((SUB, lanes), FAR, F32) for _ in range(2)]
        reach_high = [jnp.full((SUB, lanes), -FAR, F32) for _ in range(2)]
        for g in range(groups):
            there = iota_f + F32(g * SUB) < count
            for c in range(7):
                ref, at = (fixed, offset[1]) if c == 6 else (data, offset[0])
                v = turned(block(ref, at + c * slots, g))
                if c == 0:
                    v = jnp.where(there, v, FAR)
                if c == 1 and side:
                    v = v + F32(EDGE) * across
                if c == 2 and dz:
                    v = v + F32(EDGE * dz)
                if c == 3 and turning:
                    v = v + shear
                if 3 <= c < 6:
                    v = v * F32(VELOCITY_SCALE)
                if c in (1, 2) and not own:
                    a = c - 1
                    reach_low[a] = jnp.minimum(reach_low[a], jnp.where(there, v, FAR))
                    reach_high[a] = jnp.maximum(reach_high[a], jnp.where(there, v, -FAR))
                near[base + c * pitch + g * SUB : base + c * pitch + (g + 1) * SUB, :] = v
        if not own:
            for a in range(2):
                least = jnp.min(reach_low[a], axis=0, keepdims=True)
                most = jnp.max(reach_high[a], axis=0, keepdims=True)
                least, most = spread(least), spread(most)
                least = jnp.minimum(least, jnp.minimum(pltpu.roll(least, 1, 1), pltpu.roll(least, lanes - 1, 1)))
                most = jnp.maximum(most, jnp.maximum(pltpu.roll(most, 1, 1), pltpu.roll(most, lanes - 1, 1)))
                reach[(r, a)] = (least - REACH, most + REACH)

    below = lax.broadcasted_iota(jnp.int32, (slots, slots), 0) >= lax.broadcasted_iota(
        jnp.int32, (slots, slots), 1
    )
    triangle = jnp.where(below, 1.0, 0.0).astype(jnp.bfloat16)

    def ranked(slot, marks):
        ones = jnp.concatenate([jnp.where(m, 1.0, 0.0) for m in marks], axis=0)
        running = jnp.dot(triangle, ones.astype(jnp.bfloat16), preferred_element_type=F32)
        upto[slot * slots : (slot + 1) * slots, :] = running
        for g in range(groups):
            rows_of = slice(g * SUB, (g + 1) * SUB)
            place = jnp.where(marks[g], running[rows_of, :] - 1.0, -1.0)
            rank[(slot * slots + g * SUB) : (slot * slots + (g + 1) * SUB), :] = place
        sizes[slot] = jnp.max(running[slots - 1 : slots, :]).astype(jnp.int32)

    for r, (source, offset, dz) in enumerate(rows):
        base = r * 7 * pitch
        for d, dx in enumerate((0, -1, 1)):
            if own and d < 2:
                continue
            marks = []
            for g in range(groups):
                pos = [
                    near[base + a * pitch + g * SUB : base + a * pitch + (g + 1) * SUB, :]
                    for a in range(3)
                ]
                if dx:
                    pos = [pltpu.roll(v, (-dx) % lanes, 1) for v in pos]
                    pos[0] = pos[0] + F32(EDGE * dx)
                mark = (pos[0] > home_low[0]) & (pos[0] < home_high[0])
                for a in (1, 2):
                    mark = mark & (pos[a] > home_low[a]) & (pos[a] < home_high[a])
                marks.append(mark)
            ranked(4 * r + d, marks)
        if not own:
            marks = []
            for g in range(groups):
                mark = home_there[g]
                for a in range(2):
                    p = home[(a + 1) * pitch + g * SUB : (a + 1) * pitch + (g + 1) * SUB, :]
                    mark = mark & (p > reach[(r, a)][0]) & (p < reach[(r, a)][1])
                marks.append(mark)
            ranked(4 * r + 3, marks)

    def choose(slot, k):
        at = slot * slots
        line = lambda row: upto[pl.ds(at + row, SUB, stride=0), :]
        ends = [line(g * SUB + SUB - 1) for g in range(groups)]
        middles = [line(g * SUB + SUB // 2 - 1) for g in range(groups)]
        counts = [upto[pl.ds(aligned(at + g * SUB), SUB), :] for g in range(groups)]
        result = []
        for i in range(2):
            target = iota_f + ((k * (2 * SUB)).astype(F32) + F32(i * SUB))
            beyond = [ends[g] <= target for g in range(groups - 1)]

            def chosen(values):
                v = values[0]
                for g in range(1, groups):
                    v = jnp.where(beyond[g - 1], values[g], v)
                return v

            first = chosen([jnp.full((SUB, lanes), g * SUB, jnp.int32) for g in range(groups)])
            place = jnp.where(chosen(middles) <= target, SUB // 2, 0)
            for width in (2, 1):
                probe = place + (width - 1)
                found = chosen([take_rows(v, probe) for v in counts])
                place = jnp.where(found <= target, place + width, place)
            result.append(jnp.where(ends[groups - 1] > target, first + place, -1))
        return result

    def gathered(ref, base, index):
        within = index & (SUB - 1)
        result = take_rows(ref[pl.ds(base, SUB), :], within)
        for g in range(1, groups):
            result = jnp.where(
                index >= g * SUB, take_rows(ref[pl.ds(base + g * SUB, SUB), :], within), result
            )
        return result

    def aligned(value):
        return pl.multiple_of(value, SUB)

    def run_pairs(count, where_home, blocks, start=0, react=False):
        def one(j, carry):
            carry = list(carry)
            n = [liste[pl.ds(c * capacity + start + j, SUB, stride=0), :] for c in range(9)]
            tot = [None] * 3
            for b in range(blocks):
                h = [where_home[c * pitch + b * SUB : c * pitch + (b + 1) * SUB, :] for c in range(9)]
                rx, ry, rz = h[0] - n[0], h[1] - n[1], h[2] - n[2]
                squared = jnp.maximum(rx * rx + ry * ry + rz * rz, FLOOR_SQUARED)
                u = jnp.maximum(lax.rsqrt(squared) - 1.0, 0.0)
                rv = rx * (h[3] - n[3]) + ry * (h[4] - n[4]) + rz * (h[5] - n[5])
                t = ((h[6] * n[6] + h[7] * n[7]) + (h[8] + n[8])) * F32(INVERSE)
                y = (t - jnp.floor(t)) + F32(SHIFT)
                magnitude = u * (y - u * rv)
                f = [magnitude * rx, magnitude * ry, magnitude * rz]
                for a in range(3):
                    carry[3 * b + a] = carry[3 * b + a] + f[a]
                    tot[a] = f[a] if tot[a] is None else tot[a] + f[a]
            if virial:
                for i, (a, b) in enumerate(COMPONENT_PAIRS):
                    carry[3 * blocks + i] = carry[3 * blocks + i] - n[a] * tot[b]
            if react:
                for a in range(3):
                    answer[pl.ds(a * slots + j, 1), :] = jnp.sum(tot[a], axis=0, keepdims=True)
            return tuple(carry)

        def several(i, carry):
            for k in range(UNROLL):
                carry = one(UNROLL * i + k, carry)
            return carry

        zero = jnp.zeros((SUB, lanes), F32)
        begin = (zero,) * (3 * blocks + (6 if virial else 0))
        done = lax.fori_loop(0, (count + UNROLL - 1) // UNROLL, several, begin)
        for b in range(blocks):
            for a in range(3):
                part[a * slots + b * SUB : a * slots + (b + 1) * SUB, :] = done[3 * b + a]
        if virial:
            for i, (a, b) in enumerate(COMPONENT_PAIRS):
                value = done[3 * blocks + i]
                for g in range(blocks):
                    value = value + (
                        where_home[a * pitch + g * SUB : a * pitch + (g + 1) * SUB, :] * done[3 * g + b]
                    )
                if react:
                    value = value + pltpu.roll(value, 1, 1)
                tally[i * SUB : (i + 1) * SUB, :] = tally[i * SUB : (i + 1) * SUB, :] + value

    for c in range(3):
        for g in range(groups):
            at = c * slots + g * SUB
            total[at : at + SUB, :] = (
                jnp.zeros((SUB, lanes), F32) if first else force_in[at : at + SUB, :]
            )
    if virial:
        for i in range(6):
            tally[i * SUB : (i + 1) * SUB, :] = (
                jnp.zeros((SUB, lanes), F32) if first else virial_in[i * SUB : (i + 1) * SUB, :]
            )

    def gather_near(at, index, dx):
        v = gathered(near, at, index)
        return pltpu.roll(v, (-dx) % lanes, 1) if dx else v

    def fill_near(base, slot, dx, filled, k):
        for i, index in enumerate(choose(slot, k)):
            valid = index >= 0
            if dx:
                index = pltpu.roll(index, dx % lanes, 1)
            values = [gather_near(base + c * pitch, index, dx) for c in range(7)]
            values[0] = jnp.where(valid, values[0] + F32(EDGE * dx), FAR)
            values = values[:6] + list(near_noise(values[6]))
            for c in range(9):
                at = c * capacity + filled + k * (2 * SUB) + i * SUB
                liste[pl.ds(at, SUB), :] = values[c]

    def fill_home(slot, k):
        for i, index in enumerate(choose(slot, k)):
            for c in range(9):
                v = gathered(home, c * pitch, index)
                if c == 0:
                    v = jnp.where(index >= 0, v, -FAR)
                pick[pl.ds(aligned(c * pitch + k * (2 * SUB) + i * SUB), SUB), :] = v

    def steps(size):
        return (size + 2 * SUB - 1) // (2 * SUB)

    def each(first, size, fill):
        for k in range(first, (groups + 1) // 2):
            pl.when(steps(size) > k)(functools.partial(fill, jnp.int32(k)))

    def close(filled):
        liste[pl.ds(filled, SUB), :] = jnp.full((SUB, lanes), FAR, F32)
        for c in range(1, 9):
            liste[pl.ds(c * capacity + filled, SUB), :] = jnp.zeros((SUB, lanes), F32)

    def collect():
        for c in range(3):
            for g in range(groups):
                at = c * slots + g * SUB
                total[at : at + SUB, :] = total[at : at + SUB, :] + part[at : at + SUB, :]

    def own_row():
        for g in range(groups):
            values = [near[c * pitch + g * SUB : c * pitch + (g + 1) * SUB, :] for c in range(7)]
            values = values[:6] + list(near_noise(values[6]))
            for c in range(9):
                at = c * capacity + g * SUB
                liste[at : at + SUB, :] = values[c]
        size = sizes[2]
        each(0, size, functools.partial(fill_near, 0, 2, 1, slots))
        close(slots + size)
        run_pairs(slots, home, groups)
        collect()
        run_pairs(size, home, groups, start=slots, react=True)
        collect()

        def back(k, _):
            forces = [
                pltpu.roll(answer[pl.ds(aligned(c * slots + k * SUB), SUB), :], 1, 1) for c in range(3)
            ]
            for g in range(groups):
                place = rank[(2 * slots + g * SUB) : (2 * slots + (g + 1) * SUB), :]
                place = pltpu.roll(place, 1, 1).astype(jnp.int32)
                mine = (place >= k * SUB) & (place < (k + 1) * SUB)
                within = place & (SUB - 1)
                for c in range(3):
                    at = c * slots + g * SUB
                    v = take_rows(forces[c], within)
                    total[at : at + SUB, :] = total[at : at + SUB, :] - jnp.where(mine, v, 0.0)
            return 0

        lax.fori_loop(0, (size + SUB - 1) // SUB, back, 0)

    def direction(r, _):
        base = r * (7 * pitch)
        slot = 4 * r + 3
        needed = (sizes[slot] + SUB - 1) // SUB
        parts, filled, longest = [], jnp.int32(0), sizes[slot]
        for d, dx in enumerate((0, -1, 1)):
            size = sizes[4 * r + d]
            parts.append((size, functools.partial(fill_near, base, 4 * r + d, dx, filled)))
            filled = filled + size
            longest = jnp.maximum(longest, size)

        @pl.when(longest > 2 * SUB)
        def _():
            for size, fill in parts:
                each(1, size, fill)
            each(1, sizes[slot], functools.partial(fill_home, slot))

        for _, fill in parts:
            fill(jnp.int32(0))
        fill_home(slot, jnp.int32(0))
        close(filled)
        for blocks in range(1, groups + 1):
            pl.when(needed == blocks)(functools.partial(run_pairs, filled, pick, blocks))

        def back(k, _):
            for g in range(groups):
                place = rank[pl.ds(aligned(slot * slots + g * SUB), SUB), :].astype(jnp.int32)
                mine = (place >= k * SUB) & (place < (k + 1) * SUB)
                within = place & (SUB - 1)
                for c in range(3):
                    at = c * slots + g * SUB
                    v = take_rows(part[pl.ds(aligned(c * slots + k * SUB), SUB), :], within)
                    total[at : at + SUB, :] = total[at : at + SUB, :] + jnp.where(mine, v, 0.0)
            return 0

        lax.fori_loop(0, needed, back, 0)
        return 0

    if own:
        own_row()
    else:
        for r in range(len(rows)):
            direction(jnp.int32(r), 0)

    half = F32(0.5 * TIME_STEP)
    for c in range(3):
        for g in range(groups):
            at = c * slots + g * SUB
            f = total[at : at + SUB, :]
            if not last:
                force_out[at : at + SUB, :] = f
                continue
            f = f * F32(NOISE_UNIT)
            v = block(home_ref, (3 + c) * slots, g) + half * f
            if virial:
                force_out[at : at + SUB, :] = f
                velocity_out[at : at + SUB, :] = jnp.where(home_there[g], v, 0.0)
            else:
                v = v + half * f
                force_out[at : at + SUB, :] = block(home_ref, c * slots, g) + F32(TIME_STEP) * v
                force_out[3 * slots + at : 3 * slots + at + SUB, :] = v
    if virial:
        for i in range(6):
            v = tally[i * SUB : (i + 1) * SUB, :]
            if last:
                virial_out[i] = jnp.sum(v, axis=0, keepdims=True) * F32(
                    NOISE_UNIT * 0.5 / CELL_VOLUME
                )
            else:
                virial_out[i * SUB : (i + 1) * SUB, :] = v


def pairs(home, home_fixed, beads, nears, fixed, carried, rows, step, last, virial, slots, cost, side=0):
    lanes = home.shape[-1]
    own = len(rows) == 1
    first = carried is None
    operands = [home, home_fixed, *beads, *nears]
    if fixed is not None:
        operands += list(fixed)
    if not first:
        operands += list(carried)
    shape = lambda n: jax.ShapeDtypeStruct((n, lanes), F32)
    if last and virial:
        outs = (shape(3 * slots), shape(3 * slots), jax.ShapeDtypeStruct((6, 1, lanes), F32))
    elif virial:
        outs = (shape(3 * slots), shape(6 * SUB))
    elif last:
        outs = (shape(6 * slots),)
    else:
        outs = (shape(3 * slots),)
    pitch = slots + SUB
    if own:
        outs += (shape(9 * pitch + 6 * SUB),)
    vmem = pl.BlockSpec(memory_space=pltpu.VMEM)
    capacity = 3 * slots + 2 * SUB + 1
    count = len(rows)
    return pl.pallas_call(
        functools.partial(
            pair_kernel,
            slots=slots,
            lanes=lanes,
            sources=len(nears),
            rows=rows,
            own=own,
            step=step,
            first=first,
            last=last,
            virial=virial,
            has_fixed=fixed is not None,
            side=side,
        ),
        out_shape=outs,
        in_specs=[vmem] * len(operands),
        out_specs=tuple(vmem for _ in outs),
        scratch_shapes=[
            pltpu.VMEM((count * 7 * pitch, lanes), F32),
            pltpu.VMEM((4 * slots, lanes), F32),
            pltpu.VMEM((count * 4 * slots, lanes), F32),
            pltpu.VMEM((count * 4 * slots, lanes), F32),
            pltpu.VMEM((9 * pitch, lanes), F32),
            pltpu.VMEM((9 * capacity, lanes), F32),
            pltpu.VMEM((3 * slots, lanes), F32),
            pltpu.VMEM((3 * slots, lanes), F32),
            pltpu.VMEM((6 * SUB, lanes), F32),
            pltpu.SMEM((4 * count,), jnp.int32),
        ],
        compiler_params=pltpu.CompilerParams(vmem_limit_bytes=VMEM_LIMIT),
        cost_estimate=pl.CostEstimate(flops=cost, bytes_accessed=1, transcendentals=0),
        name=f"pairs_{side}_{step}",
    )(*operands)


def kick_kernel(*refs, slots, lanes):
    sources, out, held, done = refs[:6], refs[6], refs[7:13], refs[13]
    copies = [
        pltpu.make_async_copy(source, target, done.at[i])
        for i, (source, target) in enumerate(zip(sources, held))
    ]
    for copy in copies:
        copy.start()
    for copy in copies:
        copy.wait()
    position, velocity, force, seed, count, strain = held
    for c in range(3):
        for g in range(slots // SUB):
            at = c * slots + g * SUB
            rows = slice(at, at + SUB)
            v = velocity[rows, :] + F32(0.5 * TIME_STEP) * force[rows, :]
            out[rows, :] = position[rows, :] + F32(TIME_STEP) * v
            out[3 * slots + at : 3 * slots + at + SUB, :] = v
    out[6 * slots : 7 * slots, :] = seed[...].astype(F32)
    aside = jnp.broadcast_to(count[...], (SUB, lanes)).astype(F32)
    row = lax.broadcasted_iota(jnp.int32, (SUB, lanes), 0)
    for step in range(strain.shape[1]):
        aside = jnp.where(row == 1 + step, strain[:, step : step + 1].astype(F32), aside)
    out[7 * slots : 7 * slots + SUB, :] = aside


def ring(count, by):
    return [(i, (i + by) % count) for i in range(count)]


def swap(count, first):
    assert count % 2 == 0
    pairs_of = [((first + i) % count, (first + i + 1) % count) for i in range(0, count, 2)]
    return pairs_of + [(b, a) for a, b in pairs_of]


def shards(positions, velocities, forces_prev, seeds, counts, offsets):
    slots, depth, width, lanes = seeds.shape
    assert depth == 1 and width == 1
    gz, xy = lax.axis_size("gz"), lax.axis_size("xy")
    flat = lambda a: a.reshape(-1, lanes)
    tall = 7 * slots + SUB
    inputs = [flat(a) for a in (positions, velocities, forces_prev, seeds, counts)]
    inputs.append(offsets.reshape(1, -1))
    state = pl.pallas_call(
        functools.partial(kick_kernel, slots=slots, lanes=lanes),
        out_shape=jax.ShapeDtypeStruct((tall, lanes), F32),
        in_specs=[pl.BlockSpec(memory_space=pltpu.HBM)] * len(inputs),
        out_specs=pl.BlockSpec(memory_space=pltpu.VMEM),
        scratch_shapes=[pltpu.VMEM(a.shape, a.dtype) for a in inputs]
        + [pltpu.SemaphoreType.DMA((len(inputs),))],
        compiler_params=pltpu.CompilerParams(vmem_limit_bytes=KICK_LIMIT),
        name="kick",
    )(*inputs)
    home_fixed = state
    kept = None
    for step in range(2):
        final = step == 1
        high = state.shape[0]
        planes = [lax.ppermute(state, "gz", ring(gz, -1))]
        if gz > 2:
            planes.append(lax.ppermute(state, "gz", ring(gz, 1)))
        up, down = 0, len(planes) - 1
        call = functools.partial(
            pairs, state, home_fixed, step=step, virial=final, slots=slots
        )
        here = (0, 0)
        *carried, beads = call(
            [],
            [state],
            [home_fixed] if final else None,
            None,
            rows=((0, here, 0),),
            last=False,
            cost=100_000_000,
        )
        planes, carried, beads = lax.optimization_barrier((planes, carried, beads))
        stacked = jnp.concatenate([state, *planes], axis=0)
        far = lax.ppermute(stacked, "xy", swap(xy, 1))
        near = lax.ppermute(stacked, "xy", swap(xy, 0))
        arrived = (planes, [near], [far])
        if not final:
            kept = arrived
        carried = call(
            [beads],
            planes,
            kept[0] if final else None,
            carried,
            rows=((down, here, -1), (up, here, 1)),
            last=False,
            cost=100_000_000,
        )
        beside = tuple(
            (0, (place * high, place * tall), dz) for dz, place in ((0, 0), (-1, 1 + down), (1, 1 + up))
        )
        for side in (NEAR_SIDE, FAR_SIDE):
            carried = call(
                [beads],
                arrived[side],
                kept[side] if final else None,
                carried,
                rows=beside,
                last=side == FAR_SIDE,
                cost=100_000_000,
                side=side,
            )
        outs = carried
        if not final:
            state = outs[0]
    force, velocity, stress = outs
    return (
        force.reshape(positions.shape),
        velocity.reshape(positions.shape),
        stress.reshape(6, depth, width, lanes),
    )


def solution(mesh):
    beads = P(None, None, "gz", "xy", None)
    return jax.shard_map(
        shards,
        mesh=mesh,
        in_specs=(beads, beads, beads, P(None, "gz", "xy", None), P("gz", "xy", None), P()),
        out_specs=(beads, beads, P(None, "gz", "xy", None)),
        check_vma=False,
    )
```
